128 devices in a mesh: tp: 16 (over z, y), dp: 8 (over x, core).
Axes of the slice: x: 4, y: 4, z: 4, core: 2. Of those that a mesh axis runs over, the one named last changes fastest.
Arguments:
- w_in: float32 [16, 384, 2688], P(None, None, 'tp')
- w_out: float32 [16, 1920, 384], P(None, 'tp')
- g_in: float32 [8, 16, 384, 2688], P('dp', None, None, 'tp')
- g_out: float32 [8, 16, 1920, 384], P('dp', None, 'tp')
- m_in: bfloat16 [16, 384, 2688], P(None, 'dp', 'tp')
- m_out: bfloat16 [16, 1920, 384], P(None, 'tp', 'dp')
- r_in: float32 [16, 384], P(None, 'dp')
- c_in: float32 [16, 2688], P(None, 'tp')
- r_out: float32 [16, 1920], P(None, 'tp')
- c_out: float32 [16, 384], P(None, 'dp')
- learn_rate: float32 [], replicated
- weight_decay: float32 [], replicated
- beta_two: float32 [], replicated
Outputs:
- output 1: float32 [16, 384, 2688], P(None, None, 'tp')
- output 2: float32 [16, 1920, 384], P(None, 'tp')
- output 3: bfloat16 [16, 384, 2688], P(None, 'dp', 'tp')
- output 4: bfloat16 [16, 1920, 384], P(None, 'tp', 'dp')
- output 5: float32 [16, 384], P(None, 'dp')
- output 6: float32 [16, 2688], P(None, 'tp')
- output 7: float32 [16, 1920], P(None, 'tp')
- output 8: float32 [16, 384], P(None, 'dp')
All inputs are finite; a program needn't handle non-finite values.
Results may differ from the reference program's by a relative error of at most 0.00121556.
Values sent between devices are 32-bit elements.
A program may use at most 1 GiB of HBM per device.

```python
import math
import jax
import jax.numpy as jnp

LAYERS = 16
D = 384
MLP = 1536
DP = 8

FIN = MLP + 3 * D
FOUT = MLP + D


def axis_scales(key, count):
    key_ramp, key_noise = jax.random.split(key)
    ramp_slope = jax.random.uniform(key_ramp, (LAYERS, 1), jnp.float32, 0.6, 1.0)
    ramp_vals = jnp.linspace(-1.0, 1.0, count, dtype=jnp.float32)[None, :]
    noise_vals = jax.random.normal(key_noise, (LAYERS, count), jnp.float32)
    return jnp.exp(ramp_slope * ramp_vals + 0.3 * noise_vals)


def draw_matrix(key, n_rows, n_cols):
    key_list = jax.random.split(key, 7)
    row_scale = axis_scales(key_list[0], n_rows)
    col_scale = axis_scales(key_list[1], n_cols)
    noise_rep = jax.random.normal(key_list[2], (DP, LAYERS, n_rows, n_cols), jnp.float32)
    grad_rep = noise_rep * (row_scale[:, :, None] * col_scale[:, None, :] / math.sqrt(DP))
    grad_sum = jnp.sum(grad_rep, axis=0)
    grad_sq = grad_sum * grad_sum
    row_noise = jax.random.normal(key_list[3], (LAYERS, n_rows), jnp.float32)
    col_noise = jax.random.normal(key_list[4], (LAYERS, n_cols), jnp.float32)
    row_old = 0.25 * jnp.mean(grad_sq, axis=2) * jnp.exp(0.5 * row_noise)
    col_old = 0.25 * jnp.mean(grad_sq, axis=1) * jnp.exp(0.5 * col_noise)
    weight = jax.random.normal(key_list[5], (LAYERS, n_rows, n_cols), jnp.float32) * n_rows ** -0.5
    moment = (0.1 * jax.random.normal(key_list[6], (LAYERS, n_rows, n_cols), jnp.float32)).astype(jnp.bfloat16)
    return weight, grad_rep, moment, row_old, col_old


def setup_inputs(seed: int = 0) -> dict:
    key_list = jax.random.split(jax.random.key(seed), 5)
    w_in, g_in, m_in, r_in, c_in = draw_matrix(key_list[0], D, FIN)
    w_out, g_out, m_out, r_out, c_out = draw_matrix(key_list[1], FOUT, D)
    learn_rate = jax.random.uniform(key_list[2], (), jnp.float32, 0.25, 0.75) * D ** -0.5
    weight_decay = jax.random.uniform(key_list[3], (), jnp.float32, 0.15, 0.45) * D ** 0.5
    beta_two = jax.random.uniform(key_list[4], (), jnp.float32, 0.8, 0.9)
    return dict(w_in=w_in, w_out=w_out, g_in=g_in, g_out=g_out, m_in=m_in, m_out=m_out, r_in=r_in, c_in=c_in, r_out=r_out, c_out=c_out, learn_rate=learn_rate, weight_decay=weight_decay, beta_two=beta_two)


def adafactor_matrix(weight, grad_rep, moment, row_old, col_old, learn_rate, weight_decay, beta_two):
    grad_sum = jnp.sum(grad_rep, axis=0)
    grad_sq = grad_sum * grad_sum + 1e-30
    row_new = beta_two * row_old + (1.0 - beta_two) * jnp.mean(grad_sq, axis=2)
    col_new = beta_two * col_old + (1.0 - beta_two) * jnp.mean(grad_sq, axis=1)
    row_avg = jnp.mean(row_new, axis=1)
    second = row_new[:, :, None] * col_new[:, None, :] / row_avg[:, None, None]
    update = grad_sum / jnp.sqrt(second)
    rms_val = jnp.sqrt(jnp.mean(update * update, axis=(1, 2)))
    update = update / jnp.maximum(1.0, rms_val)[:, None, None]
    mom_new = (0.9 * moment.astype(jnp.float32) + 0.1 * update).astype(jnp.bfloat16)
    w_new = weight - learn_rate * mom_new.astype(jnp.float32) - learn_rate * weight_decay * weight
    return w_new, mom_new, row_new, col_new


def reference(w_in, w_out, g_in, g_out, m_in, m_out, r_in, c_in, r_out, c_out, learn_rate, weight_decay, beta_two):
    in_result = adafactor_matrix(w_in, g_in, m_in, r_in, c_in, learn_rate, weight_decay, beta_two)
    out_result = adafactor_matrix(w_out, g_out, m_out, r_out, c_out, learn_rate, weight_decay, beta_two)
    return (in_result[0], out_result[0], in_result[1], out_result[1], in_result[2], in_result[3], out_result[2], out_result[3])
```

```python
import jax
import jax.numpy as jnp
from jax import lax
from jax.experimental import pallas as pl
from jax.experimental.pallas import tpu as pltpu
from jax.sharding import PartitionSpec as P

F32, BF16 = jnp.float32, jnp.bfloat16
MESH = pl.DeviceIdType.MESH
RING = 4
L, D = 16, 384
KI, NO = 168, 120
LC, LG, NG = 8, 4, 2
Q, LN, B48, B96 = 72, 128, 48, 96
CH, HEAD, MID = 3 * Q, KI - 2 * Q, 256
NI, KIN, NOUT, KO = 384.0, 2688.0, 1920.0, 384.0
KINDS = RV, LY, LZ, SY, SZ, SX = range(6)
OB, OC = 2, 4


def roll(val, shift):
    return pltpu.roll(val, shift % LN, 1)


def lane_of(shape):
    return lax.broadcasted_iota(jnp.int32, shape, 1)


def row_of(shape):
    return lax.broadcasted_iota(jnp.int32, shape, 0)


def colsum(val):
    return jnp.sum(val, axis=0, keepdims=True)


def rowsum(val):
    return jnp.sum(val, axis=1, keepdims=True)


def pick(cond, val):
    return jnp.where(cond, val, 0.0)


def first(num):
    return pl.ds(0, num)


def block(i):
    return pl.ds(Q * i, Q)


def tile_cols(t):
    return pl.ds(LN * t, LN)


def last_quarter(parts):
    lane = lane_of(parts[0].shape)
    tail = jnp.where(lane < 64, roll(parts[1], 64), roll(parts[2], B96))
    return jnp.where(lane < 32, roll(parts[0], 32), tail)


def join_quarters(quarters, keep):
    return [jnp.where(keep, quarters[i], roll(quarters[3], B96 - 32 * i)) for i in range(3)]


def kernel(rate_ref, wd_ref, beta_ref, w_in, w_out, g_in, g_out, m_in, m_out, r_in, c_in, r_out, c_out,
           wn_in, wn_out, mn_in, mn_out, rn_in, cn_in, rn_out, cn_out,
           gbuf, pbuf, pack, via, rin, fin, mall, mraw_in, mraw_out, msend, mt, mpack, tall,
           rvacc, lvacc, lraw, craw, oraw, pads, lvold, rvold, lvnew, rvnew, box_rv, box_ly, box_lz, box_sy, box_sz, box_sx,
           gl_sem, gs_sem, gr_sem, ml_sem, ms_sem, mr_sem, s_sem, via_sem, rin_sem, ags_sem, agr_sem,
           shs_sem, shr_sem, sts_sem, str_sem, vs_sem, vr_sem, ol_sem, os_sem, or_sem, wl_sem):
    tp, dp = lax.axis_index('tp'), lax.axis_index('dp')
    z, y, x, c = tp // RING, tp % RING, dp // 2, dp % 2
    other = 1 - c
    base, pbase = c * LC, other * LC

    def at_x(xx):
        return {'dp': (xx % RING) * 2 + c}

    def at_y(yy):
        return {'tp': z * RING + yy % RING}

    def at_z(zz):
        return {'tp': (zz % RING) * RING + y}

    partner = {'dp': x * 2 + other}

    def local(src, dst, sem):
        return pltpu.make_async_copy(src, dst, sem)

    def remote(src, dst, send_sem, recv_sem, device):
        return pltpu.make_async_remote_copy(src_ref=src, dst_ref=dst, send_sem=send_sem, recv_sem=recv_sem,
                                            device_id=device, device_id_type=MESH)

    barrier = pltpu.get_barrier_semaphore()
    peers = [partner]
    for k in range(1, RING):
        peers += [at_x(x + k), at_y(y + k), at_z(z + k)]
    for peer in peers:
        pl.semaphore_signal(barrier, inc=1, device_id=peer, device_id_type=MESH)

    def own(l, i):
        src, dst = ((g_in, first(KI)), (g_out, pl.ds(KI, NO)))[i]
        return local(src.at[base + l], gbuf.at[l, dst], gl_sem.at[l, i])

    def swap(l, i):
        src, dst = ((g_in, first(KI)), (g_out, pl.ds(KI, NO)))[i]
        return remote(src.at[pbase + l], pbuf.at[l, dst], gs_sem.at[l, i], gr_sem.at[l, i], partner)

    my_rows, its_rows = pl.ds(base, LC), pl.ds(pbase, LC)
    loads = [local(m_in, mraw_in, ml_sem.at[0]), local(m_out, mraw_out, ml_sem.at[1]),
             local(r_in.at[my_rows], lraw.at[0, c], ol_sem.at[0]), local(c_out.at[my_rows], lraw.at[1, c], ol_sem.at[1]),
             local(c_in.at[my_rows], craw, ol_sem.at[2]), local(r_out.at[my_rows], oraw, ol_sem.at[3])]
    w_loads = [local(w_in, wn_in, wl_sem.at[0]), local(w_out, wn_out, wl_sem.at[1])]

    def lane_swap(m, core):
        return remote((r_in, c_out)[m].at[its_rows], lraw.at[m, core], os_sem.at[m], or_sem.at[m], partner)

    def start_loads(l, carry):
        own(l, 0).start()
        own(l, 1).start()
        return carry

    lax.fori_loop(0, LC, start_loads, 0)
    for copy in loads:
        copy.start()
    pl.semaphore_wait(barrier, len(peers))
    for l in range(OB):
        swap(l, 0).start()
        swap(l, 1).start()
    lane_swap(0, c).start()
    lane_swap(1, c).start()
    rvacc[...] = jnp.zeros_like(rvacc)
    lvacc[...] = jnp.zeros_like(lvacc)

    lane, lane8, row8, row16 = lane_of((Q, LN)), lane_of((8, LN)), row_of((8, LN)), row_of((16, LN))
    m96, k96 = lane < B96, lane8 < B96
    head = row_of((Q, LN)) < HEAD
    only_x, only_yz = row16 >= 12, (row16 >= 8) & (row16 < 12)

    def way(l):
        return 1 - 2 * (l % 2)

    def ahead(l):
        return (x + way(l) + RING) % RING

    def behind(l):
        return (x - way(l) + RING) % RING

    across = (x + 2) % RING

    def step1(l):
        return remote(pack.at[l, across], via.at[l], s_sem.at[l, 0], via_sem.at[l], at_x(ahead(l)))

    def step2(l):
        return remote(pack.at[l, ahead(l)], rin.at[l, 0], s_sem.at[l, 1], rin_sem.at[l, 0], at_x(ahead(l)))

    def step3(l):
        return remote(pack.at[l, behind(l)], rin.at[l, 1], s_sem.at[l, 2], rin_sem.at[l, 1], at_x(behind(l)))

    def m_rows(core):
        return pl.ds(pl.multiple_of(core * B48, 16), B48)

    def moment_swap(l, core):
        return remote(msend.at[l], mt.at[l, m_rows(core)], ms_sem.at[l], mr_sem.at[l], partner)

    def stage_a(l):
        for i in range(2):
            own(l, i).wait()
            swap(l, i).wait_recv()

        def tile(t, q):
            return gbuf[l, block(q), tile_cols(t)] + pbuf[l, block(q), tile_cols(t)]

        def chunk(d, q):
            if d == 0:
                return tile(0, q)
            if d == 1:
                return roll(jnp.where(m96, tile(1, q), tile(0, q)), 32)
            if d == 2:
                return roll(jnp.where(lane < 64, tile(2, q), tile(1, q)), 64)
            return roll(tile(2, q), B96)

        for d in range(RING):
            for i, val in enumerate(join_quarters([chunk(d, q) for q in range(4)], m96)):
                pack[l, d, block(i), :] = val
        step1(l).start()
        step3(l).start()

    def stage_n(l):
        msend[l, :, first(KI)] = mraw_in[pbase + l].astype(F32)
        msend[l, :, pl.ds(MID, NO)] = mraw_out[pbase + l].astype(F32)
        moment_swap(l, c).start()
        mt[l, m_rows(c), first(KI)] = mraw_in[base + l].astype(F32)
        mt[l, m_rows(c), pl.ds(MID, NO)] = mraw_out[base + l].astype(F32)

    def stage_b(l):
        step1(l).wait_recv()
        to = ahead(l)
        pack[l, to] = pack[l, to] + via[l]
        step2(l).start()

    def stage_c(l):
        step2(l).wait_recv()
        step3(l).wait_recv()
        sq = []
        for i in range(3):
            grad = pack[l, x, block(i), :] + rin[l, 0, block(i), :] + rin[l, 1, block(i), :]
            fin[l, block(i), :] = grad
            sq.append(grad * grad + 1e-30)
        g, lg = l // LG, l % LG
        sums = [rowsum(pick(m96, val)) for val in sq]
        sums.append(rowsum(jnp.where(m96, 0.0, sq[0] + sq[1] + sq[2])))
        acc = rvacc[g, first(Q), :]
        for q in range(4):
            acc = jnp.where(lane == LG * q + lg, sums[q], acc)
        rvacc[g, first(Q), :] = acc
        top = colsum(pick(head, sq[2]))
        low = colsum(jnp.where(head, 0.0, sq[2]))
        cols = [colsum(sq[0]), colsum(sq[1])]
        wide = [jnp.broadcast_to(val, (8, LN)) for val in (cols[0], cols[1], top + low)]
        in_sum = pick(k96, cols[0] + cols[1] + top)
        out_sum = pick(k96, low + last_quarter(wide))
        both = jnp.where(row8 == lg, in_sum, lvacc[g])
        lvacc[g] = jnp.where(row8 == LG + lg, out_sum, both)

    def stage_m(l):
        moment_swap(l, other).wait_recv()
        val = mt[l].T
        third = jnp.concatenate([val[2 * Q:KI], val[MID:MID + B48]], axis=0)
        quarters = [val[:Q], val[Q:2 * Q], third, val[MID + B48:MID + NO]]
        for i, part in enumerate(join_quarters(quarters, m96)):
            mpack[l, block(i), :] = part

    boxes = {RV: (box_rv, x, at_x), LY: (box_ly, y, at_y), LZ: (box_lz, z, at_z),
             SX: (box_sx, x, at_x), SY: (box_sy, y, at_y), SZ: (box_sz, z, at_z)}

    def box_copy(kind, g, k, slot):
        box, me, place = boxes[kind]
        return remote(box.at[g, slot], box.at[g, slot], sts_sem.at[g, kind, k - 1], str_sem.at[g, kind, slot], place(me + k))

    def post(kind, g, val):
        box, me, place = boxes[kind]
        box[g, me] = val
        for k in range(1, RING):
            box_copy(kind, g, k, me).start()

    def collect(kind, g):
        box, me, place = boxes[kind]
        for k in range(1, RING):
            box_copy(kind, g, k, (me + k) % RING).wait_recv()
        return ((box[g, 0] + box[g, 1]) + box[g, 2]) + box[g, 3]

    def sums_send(g):
        post(LY, g, lvacc[g])
        post(RV, g, rvacc[g].T[:16])

    def sums_mid(g):
        post(LZ, g, collect(LY, g))

    beta = beta_ref[0]

    def old_vectors():
        for copy in loads[2:]:
            copy.wait()
        for m in range(2):
            lane_swap(m, other).wait_recv()
            for core in range(2):
                pads[m, core, :, first(B48)] = lraw[m, core]
        pads[2, 0, :, first(KI - LN)] = craw[:, pl.ds(LN, KI - LN)]
        pads[2, 1, :, first(NO)] = oraw[...]
        low, high, rest = craw[:, first(LN)], pads[2, 0], pads[2, 1]
        lanes = [jnp.where(lane8 < B48, pads[m, 0], roll(pads[m, 1], B48)) for m in range(2)]
        rows = [low, jnp.where(lane8 < LN - Q, roll(low, -Q), roll(high, -Q)),
                jnp.where(lane8 < HEAD, roll(high, -16), roll(rest, HEAD)), roll(rest, -B48)]
        for g in range(NG):
            part = slice(LG * g, LG * g + LG)
            lvold[g] = jnp.concatenate([val[part] for val in lanes], axis=0)
            rvold[g] = jnp.concatenate([val[part] for val in rows], axis=0)

    def vec_swap(g, half, i):
        ref = (lvnew, rvnew)[i]
        return remote(ref.at[half, g], ref.at[half, g], vs_sem.at[g, i], vr_sem.at[g, i], partner)

    def moments(g):
        lv_mean = collect(LZ, g) / jnp.where(row8 < LG, KIN, NOUT)
        lv_new = beta * lvold[g] + (1.0 - beta) * lv_mean
        lvnew[c, g] = lv_new
        rv_new = beta * rvold[g] + (1.0 - beta) * (collect(RV, g) / NI)
        rvnew[c, g] = rv_new
        for i in range(2):
            vec_swap(g, c, i).start()
        scale_l = 1.0 / jnp.sqrt(jnp.where(k96, lv_new, 1.0))
        scale_r = 1.0 / jnp.sqrt(jnp.where(lane_of((16, LN)) < Q, rv_new, 1.0))
        wide = jnp.concatenate([scale_r, jnp.ones((LN - 16, LN), F32)], axis=0).T
        tots = jnp.zeros((16, LN), F32)
        lane1 = lane_of((1, LN))
        for lg in range(LG):
            l = g * LG + lg
            rs = [jnp.broadcast_to(wide[:Q, LG * q + lg:LG * q + lg + 1], (Q, LN)) for q in range(4)]
            sc_in = scale_l[lg:lg + 1, :]
            sc_out = jnp.broadcast_to(scale_l[LG + lg:LG + lg + 1, :], (8, LN))
            parts = []
            for i in range(3):
                body = jnp.where(head, sc_in, sc_out[:1]) if i == 2 else sc_in
                lanes = jnp.where(m96, body, roll(sc_out, B96 - 32 * i)[:1])
                u0 = fin[l, block(i), :] * jnp.where(m96, rs[i], rs[3]) * lanes
                fin[l, block(i), :] = u0
                parts.append(u0 * u0)
            inner = pick(m96, parts[0] + parts[1] + pick(head, parts[2]))
            outer = jnp.where(m96, jnp.where(head, 0.0, parts[2]), parts[0] + parts[1] + parts[2])
            v_in = pick(lane1 < B96, lv_new[lg:lg + 1, :])
            v_out = pick((lane1 >= HEAD) & (lane1 < Q), rv_new[8 + lg:9 + lg, :]) + pick(lane1 < Q, rv_new[12 + lg:13 + lg, :])
            for k, val in enumerate((colsum(inner), colsum(outer), v_in, v_out)):
                tots = jnp.where(row16 == LG * k + lg, val, tots)
        post(SY, g, tots)

    def totals_y(g):
        post(SZ, g, jnp.where(only_yz, box_sy[g, y], collect(SY, g)))

    def totals_z(g):
        post(SX, g, jnp.where(only_yz, box_sz[g, z], collect(SZ, g)))

    def factors(g):
        tot = rowsum(jnp.where(only_x, box_sx[g, x], collect(SX, g)))
        isin = row_of((8, 1)) < LG
        mean_r = tot[8:] / jnp.where(isin, NI, NOUT)
        rms = jnp.sqrt(mean_r * tot[:8] / jnp.where(isin, NI * KIN, NOUT * KO))
        return jnp.sqrt(mean_r) / jnp.maximum(1.0, rms)

    def update(l, lg, fac):
        f_in, f_out = fac[lg:lg + 1, :], fac[LG + lg:LG + lg + 1, :]
        for i in range(3):
            upd = fin[l, block(i), :] * jnp.where((m96 & head) if i == 2 else m96, f_in, f_out)
            new = 0.9 * mpack[l, block(i), :] + 0.1 * upd
            mall[base + l, x, block(i), :] = new.astype(BF16).astype(F32)

    def gather(l, k):
        slot = x if k < 2 else behind(l)
        ref = mall.at[base + l, slot]
        return remote(ref, ref, ags_sem.at[l, k], agr_sem.at[l, k], at_x(behind(l) if k == 1 else ahead(l)))

    def arrival(l, k):
        ref = mall.at[base + l, (behind(l), ahead(l), across)[k]]
        return remote(ref, ref, ags_sem.at[l, k], agr_sem.at[l, k], at_x(ahead(l)))

    def share(l, k, start):
        ref = mall.at[start + l, (behind(l), ahead(l), across, x)[k]]
        return remote(ref, ref, shs_sem.at[l, k], shr_sem.at[l, k], partner)

    def send_pair(l):
        gather(l, 0).start()
        gather(l + 1, 0).start()
        gather(l, 1).start()
        gather(l + 1, 1).start()
        share(l, 3, base).start()
        share(l + 1, 3, base).start()

    def forward_pair(l):
        for k in (l, l + 1):
            arrival(k, 0).wait_recv()
            gather(k, 2).start()
            share(k, 0, base).start()

    def settle_pair(l):
        for k in (l, l + 1):
            for i in (1, 2):
                arrival(k, i).wait_recv()
                share(k, i, base).start()

    rate = rate_ref[0]
    decay = rate * wd_ref[0]

    def unpack(at):
        for q in range(4):
            if q < 3:
                chunk = [mall[at, d, block(q), :] for d in range(RING)]
            else:
                chunk = [last_quarter([mall[at, d, block(i), :] for i in range(3)]) for d in range(RING)]
            r1, r2, r3 = roll(chunk[1], B96), roll(chunk[2], 64), roll(chunk[3], 32)
            mom = (jnp.where(m96, chunk[0], r1), jnp.where(lane < 64, r1, r2), jnp.where(lane < 32, r2, r3))
            spots = (((wn_in, 0, 0, Q),), ((wn_in, Q, 0, Q),), ((wn_in, 2 * Q, 0, HEAD), (wn_out, 0, HEAD, B48)), ((wn_out, B48, 0, Q),))[q]
            for t in range(3):
                for ref, dst, src, num in spots:
                    rows = pl.ds(dst, num)
                    w = ref[at, rows, tile_cols(t)]
                    ref[at, rows, tile_cols(t)] = w - rate * mom[t][src:src + num] - decay * w
        parts = [mall[at, x, block(i), :] for i in range(3)]
        parts.append(last_quarter(parts))
        spots = ((0, 0, Q),), ((Q, 0, Q),), ((2 * Q, 0, HEAD), (MID, HEAD, B48)), ((MID + B48, 0, Q),)
        for val, places in zip(parts, spots):
            val = jnp.where(c == 0, val, roll(val, -B48))
            for dst, src, num in places:
                tall[pl.ds(dst, num), :] = val[src:src + num]
        turned = [tall[tile_cols(t), :].T[:B48] for t in range(3)]
        mn_in[at, :, first(LN)] = turned[0].astype(BF16)
        mn_in[at, :, pl.ds(LN, KI - LN)] = turned[1][:, :KI - LN].astype(BF16)
        mn_out[at] = turned[2][:, :NO].astype(BF16)

    def unpack_pair(l, start):
        lax.fori_loop(start + l, start + l + 2, lambda at, carry: (unpack(at), carry)[1], 0)

    def take_pair(l):
        for k in (l, l + 1):
            for i in range(4):
                share(k, i, pbase).wait_recv()
        unpack_pair(l, pbase)

    def new_vectors():
        lane4 = lane_of((LG, LN))
        for half in range(2):
            for g in range(NG):
                rows = pl.ds(LC * half + LG * g, LG)
                both, val = lvnew[half, g], rvnew[half, g]
                both = jnp.where(c == 0, both, roll(both, -B48))
                rn_in[rows, :] = both[:LG, :B48]
                cn_out[rows, :] = both[LG:, :B48]
                two, three = roll(val, Q)[LG:8], val[8:12]
                cn_in[rows, first(LN)] = jnp.where(lane4 < Q, val[:LG], two)
                cn_in[rows, pl.ds(LN, KI - LN)] = jnp.where(lane4 < 16, two, roll(val, 16)[8:12])[:, :KI - LN]
                rn_out[rows, :] = jnp.where(lane4 < B48, roll(val, -HEAD)[8:12], roll(val, B48)[12:])[:, :NO]

    def stage(it, carry):
        @pl.when(it < LC)
        def _():
            stage_a(it)

        @pl.when(it < LC - OB)
        def _():
            swap(it + OB, 0).start()
            swap(it + OB, 1).start()

        @pl.when(it == 0)
        def _():
            loads[0].wait()
            loads[1].wait()

        @pl.when((it >= OB) & (it < LC + OB))
        def _():
            stage_b(it - OB)

        @pl.when(it < LC)
        def _():
            stage_n(it)

        @pl.when(it >= OC)
        def _():
            stage_c(it - OC)
            stage_m(it - OC)

        @pl.when(it == OC)
        def _():
            w_loads[0].start()
            w_loads[1].start()
            old_vectors()

        @pl.when(it == OC + 3)
        def _():
            sums_send(0)

        @pl.when(it == OC + 4)
        def _():
            sums_mid(0)

        @pl.when(it == OC + 5)
        def _():
            moments(0)

        @pl.when(it == OC + 6)
        def _():
            totals_y(0)

        @pl.when(it == OC + 7)
        def _():
            totals_z(0)

        return carry

    lax.fori_loop(0, LC + OC, stage, 0)
    sums_send(1)
    fac = factors(0)
    for lg in range(LG):
        update(lg, lg, fac)
        if lg == 1:
            send_pair(0)
    sums_mid(1)
    forward_pair(0)
    send_pair(2)
    moments(1)
    totals_y(1)
    forward_pair(2)
    totals_z(1)
    settle_pair(0)
    settle_pair(2)
    w_loads[0].wait()
    w_loads[1].wait()
    unpack_pair(0, base)
    fac = factors(1)
    for lg in range(LG):
        update(LG + lg, lg, fac)
        if lg == 1:
            send_pair(4)
    unpack_pair(2, base)
    take_pair(0)
    forward_pair(4)
    send_pair(6)
    take_pair(2)
    for g in range(NG):
        for i in range(2):
            vec_swap(g, other, i).wait_recv()
    new_vectors()
    settle_pair(4)
    unpack_pair(4, base)
    forward_pair(6)
    take_pair(4)
    settle_pair(6)
    unpack_pair(6, base)
    take_pair(6)

    def drain(l, carry):
        for i in range(2):
            swap(l, i).wait_send()
        moment_swap(l, c).wait_send()
        for step in (step1, step2, step3):
            step(l).wait_send()
        for k in range(3):
            gather(l, k).wait_send()
        for k in range(4):
            share(l, k, base).wait_send()
        return carry

    lax.fori_loop(0, LC, drain, 0)
    for m in range(2):
        lane_swap(m, c).wait_send()
    for g in range(NG):
        for kind in KINDS:
            for k in range(1, RING):
                box_copy(kind, g, k, boxes[kind][1]).wait_send()
        for i in range(2):
            vec_swap(g, c, i).wait_send()


def update_call(scalars, arrays):
    hbm, smem = pl.BlockSpec(memory_space=pltpu.HBM), pl.BlockSpec(memory_space=pltpu.SMEM)
    dma, vmem = pltpu.SemaphoreType.DMA, pltpu.VMEM

    def lanes(*lead):
        return vmem(lead + (LN,), F32)

    scratch = [
        vmem((LC, KI + NO, D), F32), vmem((LC, KI + NO, D), F32), lanes(LC, RING, CH), lanes(LC, CH), lanes(LC, 2, CH), lanes(LC, CH),
        lanes(L, RING, CH), vmem((L, B48, KI), BF16), vmem((L, B48, NO), BF16), vmem((LC, B48, D), F32), vmem((LC, LN, D), F32),
        lanes(LC, CH), lanes(D), lanes(NG, LN), lanes(NG, 8),
        vmem((2, 2, LC, B48), F32), vmem((LC, KI), F32), vmem((LC, NO), F32), lanes(3, 2, LC),
        lanes(NG, 8), lanes(NG, 16), lanes(2, NG, 8), lanes(2, NG, 16),
        lanes(NG, RING, 16), lanes(NG, RING, 8), lanes(NG, RING, 8), lanes(NG, RING, 16), lanes(NG, RING, 16), lanes(NG, RING, 16),
        dma((LC, 2)), dma((LC, 2)), dma((LC, 2)), dma((2,)), dma((LC,)), dma((LC,)), dma((LC, 3)), dma((LC,)), dma((LC, 2)),
        dma((LC, 3)), dma((LC, 3)), dma((LC, 4)), dma((LC, 4)), dma((NG, len(KINDS), 3)), dma((NG, len(KINDS), RING)),
        dma((NG, 2)), dma((NG, 2)), dma((4,)), dma((2,)), dma((2,)), dma((2,)),
    ]
    outs = [((L, KI, D), F32), ((L, NO, D), F32), ((L, B48, KI), BF16), ((L, B48, NO), BF16),
            ((L, B48), F32), ((L, KI), F32), ((L, NO), F32), ((L, B48), F32)]
    return pl.pallas_call(
        kernel,
        out_shape=[vmem(*out) for out in outs],
        in_specs=[smem] * len(scalars) + [hbm] * len(arrays),
        out_specs=[pl.BlockSpec(memory_space=vmem)] * len(outs),
        scratch_shapes=scratch,
        compiler_params=pltpu.CompilerParams(collective_id=0, has_side_effects=True, vmem_limit_bytes=36 * 2**20),
        name='adafactor',
    )(*[val.reshape(1) for val in scalars], *[pltpu.with_memory_space_constraint(val, pltpu.HBM) for val in arrays])


def solution(mesh):
    def turn(val):
        return val.swapaxes(1, 2)

    def body(w_in, w_out, g_in, g_out, m_in, m_out, r_in, c_in, r_out, c_out, learn_rate, weight_decay, beta_two):
        out = update_call((learn_rate, weight_decay, beta_two),
                          (turn(w_in), w_out, turn(g_in[0]), g_out[0], m_in, turn(m_out), r_in, c_in, r_out, c_out))
        return (turn(out[0]), out[1], out[2], turn(out[3])) + tuple(out[4:])

    cols, rows, own = P(None, None, 'tp'), P(None, 'tp', None), P(None, 'dp')
    outs = (cols, rows, P(None, 'dp', 'tp'), P(None, 'tp', 'dp'), own, P(None, 'tp'), P(None, 'tp'), own)
    in_specs = (cols, rows, P('dp', *cols), P('dp', *rows)) + outs[2:] + (P(), P(), P())
    return jax.shard_map(body, mesh=mesh, in_specs=in_specs, out_specs=outs, check_vma=False)
```

```python
import jax
import jax.numpy as jnp
from jax import lax
from jax.experimental import pallas as pl
from jax.experimental.pallas import tpu as pltpu
from jax.sharding import PartitionSpec as P

F32, BF16 = jnp.float32, jnp.bfloat16
MESH = pl.DeviceIdType.MESH
RING = 4
L, D = 16, 384
KI, NO = 168, 120
LC, LG, NG = 8, 2, 4
Q, LN, B48, B96 = 72, 128, 48, 96
CH, HEAD, MID = 3 * Q, KI - 2 * Q, 256
NI, KIN, NOUT, KO = 384.0, 2688.0, 1920.0, 384.0
KINDS = RV, LY, LZ, SY, SZ, SX = range(6)
AHEAD = 2


def roll(val, shift):
    return pltpu.roll(val, shift % LN, 1)


def lane_of(shape):
    return lax.broadcasted_iota(jnp.int32, shape, 1)


def row_of(shape):
    return lax.broadcasted_iota(jnp.int32, shape, 0)


def colsum(val):
    return jnp.sum(val, axis=0, keepdims=True)


def rowsum(val):
    return jnp.sum(val, axis=1, keepdims=True)


def pick(cond, val):
    return jnp.where(cond, val, 0.0)


def first(num):
    return pl.ds(0, num)


def block(i):
    return pl.ds(Q * i, Q)


def tile_cols(t):
    return pl.ds(LN * t, LN)


def last_quarter(parts):
    lane = lane_of(parts[0].shape)
    tail = jnp.where(lane < 64, roll(parts[1], 64), roll(parts[2], B96))
    return jnp.where(lane < 32, roll(parts[0], 32), tail)


def join_quarters(quarters, keep):
    return [jnp.where(keep, quarters[i], roll(quarters[3], B96 - 32 * i)) for i in range(3)]


def kernel(rate_ref, wd_ref, beta_ref, w_in, w_out, g_in, g_out, m_in, m_out, r_in, c_in, r_out, c_out,
           wn_in, wn_out, mn_in, mn_out, rn_in, cn_in, rn_out, cn_out,
           gbuf, pbuf, pack, via, rin, fin, mall, mraw_in, mraw_out, msend, mt, mpack, tall,
           rvacc, lvacc, lraw, craw, oraw, pads, lvold, rvold, lvnew, rvnew, box_rv, box_ly, box_lz, box_sy, box_sz, box_sx,
           gl_sem, gs_sem, gr_sem, ml_sem, ms_sem, mr_sem, s_sem, via_sem, rin_sem, ags_sem, agr_sem,
           shs_sem, shr_sem, sts_sem, str_sem, vs_sem, vr_sem, ol_sem, os_sem, or_sem, wl_sem):
    tp, dp = lax.axis_index('tp'), lax.axis_index('dp')
    z, y, x, c = tp // RING, tp % RING, dp // 2, dp % 2
    other = 1 - c
    base, pbase = c * LC, other * LC

    def at_x(xx):
        return {'dp': (xx % RING) * 2 + c}

    def at_y(yy):
        return {'tp': z * RING + yy % RING}

    def at_z(zz):
        return {'tp': (zz % RING) * RING + y}

    partner = {'dp': x * 2 + other}

    def local(src, dst, sem):
        return pltpu.make_async_copy(src, dst, sem)

    def remote(src, dst, send_sem, recv_sem, device):
        return pltpu.make_async_remote_copy(src_ref=src, dst_ref=dst, send_sem=send_sem, recv_sem=recv_sem,
                                            device_id=device, device_id_type=MESH)

    barrier = pltpu.get_barrier_semaphore()
    peers = [partner]
    for k in range(1, RING):
        peers += [at_x(x + k), at_y(y + k), at_z(z + k)]
    for peer in peers:
        pl.semaphore_signal(barrier, inc=1, device_id=peer, device_id_type=MESH)

    def own(l, i):
        src, dst = ((g_in, first(KI)), (g_out, pl.ds(KI, NO)))[i]
        return local(src.at[base + l], gbuf.at[l, dst], gl_sem.at[l, i])

    def swap(l, i):
        src, dst = ((g_in, first(KI)), (g_out, pl.ds(KI, NO)))[i]
        return remote(src.at[pbase + l], pbuf.at[l, dst], gs_sem.at[l, i], gr_sem.at[l, i], partner)

    my_rows, its_rows = pl.ds(base, LC), pl.ds(pbase, LC)
    loads = [local(m_in, mraw_in, ml_sem.at[0]), local(m_out, mraw_out, ml_sem.at[1]),
             local(r_in.at[my_rows], lraw.at[0, c], ol_sem.at[0]), local(c_out.at[my_rows], lraw.at[1, c], ol_sem.at[1]),
             local(c_in.at[my_rows], craw, ol_sem.at[2]), local(r_out.at[my_rows], oraw, ol_sem.at[3])]
    w_loads = [local(w_in, wn_in, wl_sem.at[0]), local(w_out, wn_out, wl_sem.at[1])]

    def lane_swap(m, core):
        return remote((r_in, c_out)[m].at[its_rows], lraw.at[m, core], os_sem.at[m], or_sem.at[m], partner)

    def start_loads(l, carry):
        own(l, 0).start()
        own(l, 1).start()
        return carry

    lax.fori_loop(0, LC, start_loads, 0)
    for copy in loads:
        copy.start()
    pl.semaphore_wait(barrier, len(peers))
    for l in range(AHEAD * LG):
        swap(l, 0).start()
        swap(l, 1).start()
    lane_swap(0, c).start()
    lane_swap(1, c).start()
    rvacc[...] = jnp.zeros_like(rvacc)
    lvacc[...] = jnp.zeros_like(lvacc)

    lane, lane8, row8 = lane_of((Q, LN)), lane_of((8, LN)), row_of((8, LN))
    m96, k96 = lane < B96, lane8 < B96
    head = row_of((Q, LN)) < HEAD
    no_x, only_x = row8 >= 3 * LG, (row8 >= 2 * LG) & (row8 < 3 * LG)

    def way(l):
        return 1 - 2 * (l % 2)

    def ahead(l):
        return (x + way(l) + RING) % RING

    def behind(l):
        return (x - way(l) + RING) % RING

    across = (x + 2) % RING

    def step1(l):
        return remote(pack.at[l, across], via.at[l], s_sem.at[l, 0], via_sem.at[l], at_x(ahead(l)))

    def step2(l):
        return remote(pack.at[l, ahead(l)], rin.at[l, 0], s_sem.at[l, 1], rin_sem.at[l, 0], at_x(ahead(l)))

    def step3(l):
        return remote(pack.at[l, behind(l)], rin.at[l, 1], s_sem.at[l, 2], rin_sem.at[l, 1], at_x(behind(l)))

    def m_rows(core):
        return pl.ds(pl.multiple_of(core * B48, 16), B48)

    def moment_swap(l, core):
        return remote(msend.at[l], mt.at[l, m_rows(core)], ms_sem.at[l], mr_sem.at[l], partner)

    def stage_a(l):
        for i in range(2):
            own(l, i).wait()
            swap(l, i).wait_recv()

        def tile(t, q):
            return gbuf[l, block(q), tile_cols(t)] + pbuf[l, block(q), tile_cols(t)]

        def chunk(d, q):
            if d == 0:
                return tile(0, q)
            if d == 1:
                return roll(jnp.where(m96, tile(1, q), tile(0, q)), 32)
            if d == 2:
                return roll(jnp.where(lane < 64, tile(2, q), tile(1, q)), 64)
            return roll(tile(2, q), B96)

        for d in range(RING):
            for i, val in enumerate(join_quarters([chunk(d, q) for q in range(4)], m96)):
                pack[l, d, block(i), :] = val
        step1(l).start()
        step3(l).start()

    def stage_n(l):
        msend[l, :, first(KI)] = mraw_in[pbase + l].astype(F32)
        msend[l, :, pl.ds(MID, NO)] = mraw_out[pbase + l].astype(F32)
        moment_swap(l, c).start()
        mt[l, m_rows(c), first(KI)] = mraw_in[base + l].astype(F32)
        mt[l, m_rows(c), pl.ds(MID, NO)] = mraw_out[base + l].astype(F32)

    def stage_b(l):
        step1(l).wait_recv()
        to = ahead(l)
        pack[l, to] = pack[l, to] + via[l]
        step2(l).start()

    def stage_c(l):
        step2(l).wait_recv()
        step3(l).wait_recv()
        sq = []
        for i in range(3):
            grad = pack[l, x, block(i), :] + rin[l, 0, block(i), :] + rin[l, 1, block(i), :]
            fin[l, block(i), :] = grad
            sq.append(grad * grad + 1e-30)
        g, lg = l // LG, l % LG
        sums = [rowsum(pick(m96, val)) for val in sq]
        sums.append(rowsum(jnp.where(m96, 0.0, sq[0] + sq[1] + sq[2])))
        acc = rvacc[g, first(Q), :]
        for q in range(4):
            acc = jnp.where(lane == LG * q + lg, sums[q], acc)
        rvacc[g, first(Q), :] = acc
        top = colsum(pick(head, sq[2]))
        low = colsum(jnp.where(head, 0.0, sq[2]))
        cols = [colsum(sq[0]), colsum(sq[1])]
        wide = [jnp.broadcast_to(val, (8, LN)) for val in (cols[0], cols[1], top + low)]
        in_sum = pick(k96, cols[0] + cols[1] + top)
        out_sum = pick(k96, low + last_quarter(wide))
        both = jnp.where(row8 == lg, in_sum, lvacc[g])
        lvacc[g] = jnp.where(row8 == LG + lg, out_sum, both)

    def stage_m(l):
        moment_swap(l, other).wait_recv()
        val = mt[l].T
        third = jnp.concatenate([val[2 * Q:KI], val[MID:MID + B48]], axis=0)
        quarters = [val[:Q], val[Q:2 * Q], third, val[MID + B48:MID + NO]]
        for i, part in enumerate(join_quarters(quarters, m96)):
            mpack[l, block(i), :] = part

    boxes = {RV: (box_rv, x, at_x), LY: (box_ly, y, at_y), LZ: (box_lz, z, at_z),
             SX: (box_sx, x, at_x), SY: (box_sy, y, at_y), SZ: (box_sz, z, at_z)}

    def box_copy(kind, g, k, slot):
        box, me, place = boxes[kind]
        return remote(box.at[g, slot], box.at[g, slot], sts_sem.at[g, kind, k - 1], str_sem.at[g, kind, slot], place(me + k))

    def post(kind, g, val):
        box, me, place = boxes[kind]
        box[g, me] = val
        for k in range(1, RING):
            box_copy(kind, g, k, me).start()

    def collect(kind, g):
        box, me, place = boxes[kind]
        for k in range(1, RING):
            box_copy(kind, g, k, (me + k) % RING).wait_recv()
        return ((box[g, 0] + box[g, 1]) + box[g, 2]) + box[g, 3]

    def sums_send(g):
        post(LY, g, lvacc[g])
        post(RV, g, rvacc[g].T[:8])

    def sums_mid(g):
        post(LZ, g, collect(LY, g))

    beta = beta_ref[0]

    def old_vectors():
        for copy in loads[2:]:
            copy.wait()
        for m in range(2):
            lane_swap(m, other).wait_recv()
            for core in range(2):
                pads[m, core, :, first(B48)] = lraw[m, core]
        pads[2, 0, :, first(KI - LN)] = craw[:, pl.ds(LN, KI - LN)]
        pads[2, 1, :, first(NO)] = oraw[...]
        low, high, rest = craw[:, first(LN)], pads[2, 0], pads[2, 1]
        lanes = [jnp.where(lane8 < B48, pads[m, 0], roll(pads[m, 1], B48)) for m in range(2)]
        rows = [low, jnp.where(lane8 < LN - Q, roll(low, -Q), roll(high, -Q)),
                jnp.where(lane8 < HEAD, roll(high, -16), roll(rest, HEAD)), roll(rest, -B48)]
        for g in range(NG):
            part = slice(LG * g, LG * g + LG)
            lvold[g] = jnp.concatenate([val[part] for val in lanes + lanes], axis=0)
            rvold[g] = jnp.concatenate([val[part] for val in rows], axis=0)

    def vec_swap(g, half, i):
        ref = (lvnew, rvnew)[i]
        return remote(ref.at[half, g], ref.at[half, g], vs_sem.at[g, i], vr_sem.at[g, i], partner)

    def moments(g):
        lv_mean = collect(LZ, g) / jnp.where(row8 < LG, KIN, NOUT)
        lv_new = beta * lvold[g] + (1.0 - beta) * lv_mean
        lvnew[c, g] = lv_new
        rv_new = beta * rvold[g] + (1.0 - beta) * (collect(RV, g) / NI)
        rvnew[c, g] = rv_new
        for i in range(2):
            vec_swap(g, c, i).start()
        scale_l = 1.0 / jnp.sqrt(jnp.where(k96, lv_new, 1.0))
        scale_r = 1.0 / jnp.sqrt(jnp.where(lane8 < Q, rv_new, 1.0))
        wide = jnp.concatenate([scale_r, jnp.ones((LN - 8, LN), F32)], axis=0).T
        tots = jnp.zeros((8, LN), F32)
        lane1 = lane_of((1, LN))
        for lg in range(LG):
            l = g * LG + lg
            rs = [jnp.broadcast_to(wide[:Q, LG * q + lg:LG * q + lg + 1], (Q, LN)) for q in range(4)]
            sc_in = scale_l[lg:lg + 1, :]
            sc_out = jnp.broadcast_to(scale_l[LG + lg:LG + lg + 1, :], (8, LN))
            parts = []
            for i in range(3):
                body = jnp.where(head, sc_in, sc_out[:1]) if i == 2 else sc_in
                lanes = jnp.where(m96, body, roll(sc_out, B96 - 32 * i)[:1])
                u0 = fin[l, block(i), :] * jnp.where(m96, rs[i], rs[3]) * lanes
                fin[l, block(i), :] = u0
                parts.append(u0 * u0)
            inner = pick(m96, parts[0] + parts[1] + pick(head, parts[2]))
            outer = jnp.where(m96, jnp.where(head, 0.0, parts[2]), parts[0] + parts[1] + parts[2])
            v_in = pick(lane1 < B96, lv_new[lg:lg + 1, :])
            v_out = pick((lane1 >= HEAD) & (lane1 < Q), rv_new[2 * LG + lg:2 * LG + lg + 1, :]) + pick(lane1 < Q, rv_new[3 * LG + lg:3 * LG + lg + 1, :])
            for k, val in enumerate((colsum(inner), colsum(outer), v_in, v_out)):
                tots = jnp.where(row8 == LG * k + lg, val, tots)
        post(SY, g, tots)

    def totals_y(g):
        post(SZ, g, jnp.where(only_x, box_sy[g, y], collect(SY, g)))

    def totals_z(g):
        post(SX, g, jnp.where(only_x, box_sz[g, z], collect(SZ, g)))

    def factors(g):
        tot = rowsum(jnp.where(no_x, box_sx[g, x], collect(SX, g)))
        isin = row_of((2 * LG, 1)) < LG
        mean_r = tot[2 * LG:] / jnp.where(isin, NI, NOUT)
        rms = jnp.sqrt(mean_r * tot[:2 * LG] / jnp.where(isin, NI * KIN, NOUT * KO))
        return jnp.sqrt(mean_r) / jnp.maximum(1.0, rms)

    def update(l, lg, fac):
        f_in, f_out = fac[lg:lg + 1, :], fac[LG + lg:LG + lg + 1, :]
        for i in range(3):
            upd = fin[l, block(i), :] * jnp.where((m96 & head) if i == 2 else m96, f_in, f_out)
            new = 0.9 * mpack[l, block(i), :] + 0.1 * upd
            mall[base + l, x, block(i), :] = new.astype(BF16).astype(F32)

    def gather(l, k):
        slot = x if k < 2 else behind(l)
        ref = mall.at[base + l, slot]
        return remote(ref, ref, ags_sem.at[l, k], agr_sem.at[l, k], at_x(behind(l) if k == 1 else ahead(l)))

    def arrival(l, k):
        ref = mall.at[base + l, (behind(l), ahead(l), across)[k]]
        return remote(ref, ref, ags_sem.at[l, k], agr_sem.at[l, k], at_x(ahead(l)))

    def share(l, k, start):
        ref = mall.at[start + l, (behind(l), ahead(l), across, x)[k]]
        return remote(ref, ref, shs_sem.at[l, k], shr_sem.at[l, k], partner)

    def send_pair(l):
        gather(l, 0).start()
        gather(l + 1, 0).start()
        gather(l, 1).start()
        gather(l + 1, 1).start()
        share(l, 3, base).start()
        share(l + 1, 3, base).start()

    def forward_pair(l):
        for k in (l, l + 1):
            arrival(k, 0).wait_recv()
            gather(k, 2).start()
            share(k, 0, base).start()

    def settle_pair(l):
        for k in (l, l + 1):
            for i in (1, 2):
                arrival(k, i).wait_recv()
                share(k, i, base).start()

    rate = rate_ref[0]
    decay = rate * wd_ref[0]

    def unpack(at):
        for q in range(4):
            if q < 3:
                chunk = [mall[at, d, block(q), :] for d in range(RING)]
            else:
                chunk = [last_quarter([mall[at, d, block(i), :] for i in range(3)]) for d in range(RING)]
            r1, r2, r3 = roll(chunk[1], B96), roll(chunk[2], 64), roll(chunk[3], 32)
            mom = (jnp.where(m96, chunk[0], r1), jnp.where(lane < 64, r1, r2), jnp.where(lane < 32, r2, r3))
            spots = (((wn_in, 0, 0, Q),), ((wn_in, Q, 0, Q),), ((wn_in, 2 * Q, 0, HEAD), (wn_out, 0, HEAD, B48)), ((wn_out, B48, 0, Q),))[q]
            for t in range(3):
                for ref, dst, src, num in spots:
                    rows = pl.ds(dst, num)
                    w = ref[at, rows, tile_cols(t)]
                    ref[at, rows, tile_cols(t)] = w - rate * mom[t][src:src + num] - decay * w
        parts = [mall[at, x, block(i), :] for i in range(3)]
        parts.append(last_quarter(parts))
        spots = ((0, 0, Q),), ((Q, 0, Q),), ((2 * Q, 0, HEAD), (MID, HEAD, B48)), ((MID + B48, 0, Q),)
        for val, places in zip(parts, spots):
            val = jnp.where(c == 0, val, roll(val, -B48))
            for dst, src, num in places:
                tall[pl.ds(dst, num), :] = val[src:src + num]
        turned = [tall[tile_cols(t), :].T[:B48] for t in range(3)]
        mn_in[at, :, first(LN)] = turned[0].astype(BF16)
        mn_in[at, :, pl.ds(LN, KI - LN)] = turned[1][:, :KI - LN].astype(BF16)
        mn_out[at] = turned[2][:, :NO].astype(BF16)

    def unpack_pair(l, start):
        lax.fori_loop(start + l, start + l + 2, lambda at, carry: (unpack(at), carry)[1], 0)

    def take_pair(l):
        for k in (l, l + 1):
            for i in range(4):
                share(k, i, pbase).wait_recv()
        unpack_pair(l, pbase)

    def new_vectors():
        lane4 = lane_of((LG, LN))
        for half in range(2):
            for g in range(NG):
                rows = pl.ds(LC * half + LG * g, LG)
                both, val = lvnew[half, g], rvnew[half, g]
                both = jnp.where(c == 0, both, roll(both, -B48))
                rn_in[rows, :] = both[:LG, :B48]
                cn_out[rows, :] = both[LG:2 * LG, :B48]
                two = roll(val, Q)[LG:2 * LG]
                cn_in[rows, first(LN)] = jnp.where(lane4 < Q, val[:LG], two)
                cn_in[rows, pl.ds(LN, KI - LN)] = jnp.where(lane4 < 16, two, roll(val, 16)[2 * LG:3 * LG])[:, :KI - LN]
                rn_out[rows, :] = jnp.where(lane4 < B48, roll(val, -HEAD)[2 * LG:3 * LG], roll(val, B48)[3 * LG:])[:, :NO]

    def both(step, g):
        for lg in range(LG):
            step(LG * g + lg)

    def swap_start(l):
        swap(l, 0).start()
        swap(l, 1).start()

    def stage(it, carry):
        @pl.when(it < NG)
        def _():
            both(stage_a, it)

        @pl.when(it < NG - AHEAD)
        def _():
            both(swap_start, it + AHEAD)

        @pl.when(it == 0)
        def _():
            loads[0].wait()
            loads[1].wait()

        @pl.when((it >= 1) & (it <= NG))
        def _():
            both(stage_b, it - 1)

        @pl.when(it == 4)
        def _():
            totals_y(0)

        @pl.when((it == 3) | (it == 4))
        def _():
            sums_mid(it - 3)

        @pl.when(it < NG)
        def _():
            both(stage_n, it)

        @pl.when(it == 2)
        def _():
            w_loads[0].start()
            w_loads[1].start()
            old_vectors()

        @pl.when(it >= 2)
        def _():
            both(stage_c, it - 2)
            sums_send(it - 2)
            both(stage_m, it - 2)

        @pl.when(it == 4)
        def _():
            totals_z(0)

        @pl.when((it == 3) | (it == 4))
        def _():
            moments(it - 3)

        return carry

    lax.fori_loop(0, NG + 2, stage, 0)

    def update_pair(g):
        fac = factors(g)
        for lg in range(LG):
            update(LG * g + lg, lg, fac)

    update_pair(0)
    send_pair(0)
    totals_y(1)
    sums_mid(2)
    totals_z(1)
    moments(2)
    sums_mid(3)
    forward_pair(0)
    update_pair(1)
    send_pair(2)
    totals_y(2)
    moments(3)
    totals_z(2)
    totals_y(3)
    settle_pair(0)
    forward_pair(2)
    w_loads[0].wait()
    w_loads[1].wait()
    unpack_pair(0, base)
    totals_z(3)
    update_pair(2)
    send_pair(4)
    take_pair(0)
    settle_pair(2)
    update_pair(3)
    forward_pair(4)
    send_pair(6)
    unpack_pair(2, base)
    take_pair(2)
    for g in range(NG):
        for i in range(2):
            vec_swap(g, other, i).wait_recv()
    new_vectors()
    settle_pair(4)
    unpack_pair(4, base)
    forward_pair(6)
    take_pair(4)
    settle_pair(6)
    unpack_pair(6, base)
    take_pair(6)

    def drain(l, carry):
        for i in range(2):
            swap(l, i).wait_send()
        moment_swap(l, c).wait_send()
        for step in (step1, step2, step3):
            step(l).wait_send()
        for k in range(3):
            gather(l, k).wait_send()
        for k in range(4):
            share(l, k, base).wait_send()
        return carry

    lax.fori_loop(0, LC, drain, 0)
    for m in range(2):
        lane_swap(m, c).wait_send()
    for g in range(NG):
        for kind in KINDS:
            for k in range(1, RING):
                box_copy(kind, g, k, boxes[kind][1]).wait_send()
        for i in range(2):
            vec_swap(g, c, i).wait_send()


def update_call(scalars, arrays):
    hbm, smem = pl.BlockSpec(memory_space=pltpu.HBM), pl.BlockSpec(memory_space=pltpu.SMEM)
    dma, vmem = pltpu.SemaphoreType.DMA, pltpu.VMEM

    def lanes(*lead):
        return vmem(lead + (LN,), F32)

    scratch = [
        vmem((LC, KI + NO, D), F32), vmem((LC, KI + NO, D), F32), lanes(LC, RING, CH), lanes(LC, CH), lanes(LC, 2, CH), lanes(LC, CH),
        lanes(L, RING, CH), vmem((L, B48, KI), BF16), vmem((L, B48, NO), BF16), vmem((LC, B48, D), F32), vmem((LC, LN, D), F32),
        lanes(LC, CH), lanes(D), lanes(NG, LN), lanes(NG, 8),
        vmem((2, 2, LC, B48), F32), vmem((LC, KI), F32), vmem((LC, NO), F32), lanes(3, 2, LC),
        lanes(NG, 8), lanes(NG, 8), lanes(2, NG, 8), lanes(2, NG, 8),
        *[lanes(NG, RING, 8)] * len(KINDS),
        dma((LC, 2)), dma((LC, 2)), dma((LC, 2)), dma((2,)), dma((LC,)), dma((LC,)), dma((LC, 3)), dma((LC,)), dma((LC, 2)),
        dma((LC, 3)), dma((LC, 3)), dma((LC, 4)), dma((LC, 4)), dma((NG, len(KINDS), 3)), dma((NG, len(KINDS), RING)),
        dma((NG, 2)), dma((NG, 2)), dma((4,)), dma((2,)), dma((2,)), dma((2,)),
    ]
    outs = [((L, KI, D), F32), ((L, NO, D), F32), ((L, B48, KI), BF16), ((L, B48, NO), BF16),
            ((L, B48), F32), ((L, KI), F32), ((L, NO), F32), ((L, B48), F32)]
    return pl.pallas_call(
        kernel,
        out_shape=[vmem(*out) for out in outs],
        in_specs=[smem] * len(scalars) + [hbm] * len(arrays),
        out_specs=[pl.BlockSpec(memory_space=vmem)] * len(outs),
        scratch_shapes=scratch,
        compiler_params=pltpu.CompilerParams(collective_id=0, has_side_effects=True, vmem_limit_bytes=36 * 2**20),
        name='adafactor',
    )(*[val.reshape(1) for val in scalars], *[pltpu.with_memory_space_constraint(val, pltpu.HBM) for val in arrays])


def store_kernel(*refs):
    num = len(refs) // 2
    copies = [pltpu.make_async_copy(src, dst, refs[-1].at[i]) for i, (src, dst) in enumerate(zip(refs[:num], refs[num:-1]))]
    for copy in copies:
        copy.start()
    for copy in copies:
        copy.wait()


def store_call(vals):
    anyspace = pl.BlockSpec(memory_space=pl.ANY)
    return pl.pallas_call(
        store_kernel,
        out_shape=[jax.ShapeDtypeStruct(val.shape, val.dtype) for val in vals],
        in_specs=[anyspace] * len(vals),
        out_specs=[anyspace] * len(vals),
        scratch_shapes=[pltpu.SemaphoreType.DMA((len(vals),))],
        compiler_params=pltpu.CompilerParams(vmem_limit_bytes=2**20),
        name='store',
    )(*[pltpu.with_memory_space_constraint(val, pltpu.VMEM) for val in vals])


def solution(mesh):
    def turn(val):
        return val.swapaxes(1, 2)

    def body(w_in, w_out, g_in, g_out, m_in, m_out, r_in, c_in, r_out, c_out, learn_rate, weight_decay, beta_two):
        out = store_call(update_call((learn_rate, weight_decay, beta_two),
                          (turn(w_in), w_out, turn(g_in[0]), g_out[0], m_in, turn(m_out), r_in, c_in, r_out, c_out)))
        return (turn(out[0]), out[1], out[2], turn(out[3])) + tuple(out[4:])

    cols, rows, own = P(None, None, 'tp'), P(None, 'tp', None), P(None, 'dp')
    outs = (cols, rows, P(None, 'dp', 'tp'), P(None, 'tp', 'dp'), own, P(None, 'tp'), P(None, 'tp'), own)
    in_specs = (cols, rows, P('dp', *cols), P('dp', *rows)) + outs[2:] + (P(), P(), P())
    return jax.shard_map(body, mesh=mesh, in_specs=in_specs, out_specs=outs, check_vma=False)
```

```python
import jax
import jax.numpy as jnp
from jax import lax
from jax.experimental import pallas as pl
from jax.experimental.pallas import tpu as pltpu
from jax.sharding import PartitionSpec as P

F32, BF16 = jnp.float32, jnp.bfloat16
MESH = pl.DeviceIdType.MESH
RING = 4
L, D = 16, 384
KI, NO = 168, 120
LC, LG, NG = 8, 2, 4
Q, LN, B48, B96 = 72, 128, 48, 96
CH, HEAD, MID = 3 * Q, KI - 2 * Q, 256
NI, KIN, NOUT, KO = 384.0, 2688.0, 1920.0, 384.0
KINDS = RV, SX, LT, ST = range(4)
TP = RING * RING


def roll(val, shift):
    return pltpu.roll(val, shift % LN, 1)


def lane_of(shape):
    return lax.broadcasted_iota(jnp.int32, shape, 1)


def row_of(shape):
    return lax.broadcasted_iota(jnp.int32, shape, 0)


def colsum(val):
    return jnp.sum(val, axis=0, keepdims=True)


def rowsum(val):
    return jnp.sum(val, axis=1, keepdims=True)


def pick(cond, val):
    return jnp.where(cond, val, 0.0)


def first(num):
    return pl.ds(0, num)


def block(i):
    return pl.ds(Q * i, Q)


def tile_cols(t):
    return pl.ds(LN * t, LN)


def last_quarter(parts):
    lane = lane_of(parts[0].shape)
    tail = jnp.where(lane < 64, roll(parts[1], 64), roll(parts[2], B96))
    return jnp.where(lane < 32, roll(parts[0], 32), tail)


def join_quarters(quarters, keep):
    return [jnp.where(keep, quarters[i], roll(quarters[3], B96 - 32 * i)) for i in range(3)]


def kernel(rate_ref, wd_ref, beta_ref, w_in, w_out, g_in, g_out, m_in, m_out, r_in, c_in, r_out, c_out,
           wn_in, wn_out, mn_in, mn_out, rn_in, cn_in, rn_out, cn_out,
           gbuf, pbuf, pack, via, rin, fin, mall, mraw_in, mraw_out, msend, mt, mpack, tall,
           rvacc, lvacc, lraw, craw, oraw, pads, lvold, rvold, lvnew, rvnew, box_rv, box_sx, box_lt, box_st,
           gl_sem, gs_sem, gr_sem, ml_sem, ms_sem, mr_sem, s_sem, via_sem, rin_sem, ags_sem, agr_sem,
           shs_sem, shr_sem, sts_sem, str_sem, vs_sem, vr_sem, ol_sem, os_sem, wl_sem, ready):
    tp, dp = lax.axis_index('tp'), lax.axis_index('dp')
    z, y, x, c = tp // RING, tp % RING, dp // 2, dp % 2
    other = 1 - c
    base, pbase = c * LC, other * LC

    def at_x(xx):
        return {'dp': (xx % RING) * 2 + c}

    def at_y(yy):
        return {'tp': z * RING + yy % RING}

    def at_z(zz):
        return {'tp': (zz % RING) * RING + y}

    partner = {'dp': x * 2 + other}

    def local(src, dst, sem):
        return pltpu.make_async_copy(src, dst, sem)

    def remote(src, dst, send_sem, recv_sem, device):
        return pltpu.make_async_remote_copy(src_ref=src, dst_ref=dst, send_sem=send_sem, recv_sem=recv_sem,
                                            device_id=device, device_id_type=MESH)

    barrier = pltpu.get_barrier_semaphore()
    peers = [partner]
    for k in range(1, RING):
        peers += [at_x(x + k), at_y(y + k), at_z(z + k)]
    for peer in peers:
        pl.semaphore_signal(barrier, inc=1, device_id=peer, device_id_type=MESH)

    def own(l, i):
        src, dst = ((g_in, first(KI)), (g_out, pl.ds(KI, NO)))[i]
        return local(src.at[base + l], gbuf.at[l, dst], gl_sem.at[l // LG])

    def swap(l, i):
        src, dst = ((g_in, first(KI)), (g_out, pl.ds(KI, NO)))[i]
        return remote(src.at[pbase + l], pbuf.at[l, dst], gs_sem.at[0], gr_sem.at[l // LG], partner)

    my_rows, its_rows = pl.ds(base, LC), pl.ds(pbase, LC)
    loads = [local(m_in, mraw_in, ml_sem.at[0]), local(m_out, mraw_out, ml_sem.at[1]),
             local(r_in.at[my_rows], lraw.at[0, c], ol_sem.at[0]), local(c_out.at[my_rows], lraw.at[1, c], ol_sem.at[1]),
             local(c_in.at[my_rows], craw, ol_sem.at[2]), local(r_out.at[my_rows], oraw, ol_sem.at[3])]
    w_loads = [local(w_in, wn_in, wl_sem.at[0]), local(w_out, wn_out, wl_sem.at[1])]

    def lane_swap(m, core):
        return remote((r_in, c_out)[m].at[its_rows], lraw.at[m, core], os_sem.at[0], os_sem.at[1], partner)

    def start_loads(l, carry):
        own(l, 0).start()
        own(l, 1).start()
        return carry

    lax.fori_loop(0, LC, start_loads, 0)
    for copy in loads:
        copy.start()
    pl.semaphore_wait(barrier, len(peers))
    for k in range(1, RING):
        pl.semaphore_signal(ready, inc=1, device_id=at_y(y + k), device_id_type=MESH)
    for l in range(LG):
        swap(l, 0).start()
        swap(l, 1).start()
    lane_swap(0, c).start()
    lane_swap(1, c).start()
    rvacc[...] = jnp.zeros_like(rvacc)
    lvacc[...] = jnp.zeros_like(lvacc)

    lane, lane8, row8 = lane_of((Q, LN)), lane_of((8, LN)), row_of((8, LN))
    m96, k96 = lane < B96, lane8 < B96
    head = row_of((Q, LN)) < HEAD
    no_x, only_x = row8 >= 3 * LG, (row8 >= 2 * LG) & (row8 < 3 * LG)

    def way(l):
        return 1 - 2 * (l % 2)

    def ahead(l):
        return (x + way(l) + RING) % RING

    def behind(l):
        return (x - way(l) + RING) % RING

    across = (x + 2) % RING

    def step1(l):
        return remote(pack.at[l, across], via.at[l], s_sem.at[0], via_sem.at[l], at_x(ahead(l)))

    def step2(l):
        return remote(pack.at[l, ahead(l)], rin.at[l, 0], s_sem.at[0], rin_sem.at[l], at_x(ahead(l)))

    def step3(l):
        return remote(pack.at[l, behind(l)], rin.at[l, 1], s_sem.at[0], rin_sem.at[l], at_x(behind(l)))

    def m_rows(core):
        return pl.ds(pl.multiple_of(core * B48, 16), B48)

    def moment_swap(l, core):
        return remote(msend.at[l], mt.at[l, m_rows(core)], ms_sem.at[0], mr_sem.at[l // LG], partner)

    def stage_a(l):
        def tile(t, q):
            return gbuf[l, block(q), tile_cols(t)] + pbuf[l, block(q), tile_cols(t)]

        def chunk(d, q):
            if d == 0:
                return tile(0, q)
            if d == 1:
                return roll(jnp.where(m96, tile(1, q), tile(0, q)), 32)
            if d == 2:
                return roll(jnp.where(lane < 64, tile(2, q), tile(1, q)), 64)
            return roll(tile(2, q), B96)

        for d in range(RING):
            for i, val in enumerate(join_quarters([chunk(d, q) for q in range(4)], m96)):
                pack[l, d, block(i), :] = val

    def stage_n(l):
        msend[l, :, first(KI)] = mraw_in[pbase + l].astype(F32)
        msend[l, :, pl.ds(MID, NO)] = mraw_out[pbase + l].astype(F32)
        moment_swap(l, c).start()
        mt[l, m_rows(c), first(KI)] = mraw_in[base + l].astype(F32)
        mt[l, m_rows(c), pl.ds(MID, NO)] = mraw_out[base + l].astype(F32)

    def stage_b(l):
        step1(l).wait_recv()
        to = ahead(l)
        pack[l, to] = pack[l, to] + via[l]
        step2(l).start()

    def stage_c(l):
        remote(rin.at[l], rin.at[l], s_sem.at[0], rin_sem.at[l], partner).wait_recv()
        sq = []
        for i in range(3):
            grad = pack[l, x, block(i), :] + rin[l, 0, block(i), :] + rin[l, 1, block(i), :]
            fin[l, block(i), :] = grad
            sq.append(grad * grad + 1e-30)
        g, lg = l // LG, l % LG
        sums = [rowsum(pick(m96, val)) for val in sq]
        sums.append(rowsum(jnp.where(m96, 0.0, sq[0] + sq[1] + sq[2])))
        acc = rvacc[g, first(Q), :]
        for q in range(4):
            acc = jnp.where(lane == LG * q + lg, sums[q], acc)
        rvacc[g, first(Q), :] = acc
        top = colsum(pick(head, sq[2]))
        low = colsum(jnp.where(head, 0.0, sq[2]))
        cols = [colsum(sq[0]), colsum(sq[1])]
        wide = [jnp.broadcast_to(val, (8, LN)) for val in (cols[0], cols[1], top + low)]
        in_sum = pick(k96, cols[0] + cols[1] + top)
        out_sum = pick(k96, low + last_quarter(wide))
        both = jnp.where(row8 == lg, in_sum, lvacc[g])
        lvacc[g] = jnp.where(row8 == LG + lg, out_sum, both)

    def stage_m(l):
        val = mt[l].T
        third = jnp.concatenate([val[2 * Q:KI], val[MID:MID + B48]], axis=0)
        quarters = [val[:Q], val[Q:2 * Q], third, val[MID + B48:MID + NO]]
        for i, part in enumerate(join_quarters(quarters, m96)):
            mpack[l, block(i), :] = part

    boxes = {RV: (box_rv, x, RING), SX: (box_sx, x, RING), LT: (box_lt, tp, TP), ST: (box_st, tp, TP)}

    def post(kind, g, val):
        box, me, num = boxes[kind]
        box[g, me] = val

        def send(k, carry):
            device = at_x(me + k) if num == RING else {'tp': (me + k) % TP}
            remote(box.at[g, me], box.at[g, me], sts_sem.at[0], str_sem.at[g, kind], device).start()
            return carry

        lax.fori_loop(1, num, send, 0)

    def collect(kind, g):
        box, me, num = boxes[kind]
        rest = box.at[g, first(num - 1)]
        remote(rest, rest, sts_sem.at[0], str_sem.at[g, kind], partner).wait_recv()
        val = box[g, 0]
        for k in range(1, num):
            val = val + box[g, k]
        return val

    def sums_send(g):
        post(LT, g, lvacc[g])
        post(RV, g, rvacc[g].T[:8])

    beta = beta_ref[0]

    def old_vectors():
        for copy in loads[2:]:
            copy.wait()
        remote(lraw.at[0], lraw.at[0], os_sem.at[0], os_sem.at[1], partner).wait_recv()
        for m in range(2):
            for core in range(2):
                pads[m, core, :, first(B48)] = lraw[m, core]
        pads[2, 0, :, first(KI - LN)] = craw[:, pl.ds(LN, KI - LN)]
        pads[2, 1, :, first(NO)] = oraw[...]
        low, high, rest = craw[:, first(LN)], pads[2, 0], pads[2, 1]
        lanes = [jnp.where(lane8 < B48, pads[m, 0], roll(pads[m, 1], B48)) for m in range(2)]
        rows = [low, jnp.where(lane8 < LN - Q, roll(low, -Q), roll(high, -Q)),
                jnp.where(lane8 < HEAD, roll(high, -16), roll(rest, HEAD)), roll(rest, -B48)]
        for g in range(NG):
            part = slice(LG * g, LG * g + LG)
            lvold[g] = jnp.concatenate([val[part] for val in lanes + lanes], axis=0)
            rvold[g] = jnp.concatenate([val[part] for val in rows], axis=0)

    def vec_swap(g, half, i):
        ref = (lvnew, rvnew)[i]
        return remote(ref.at[half, g], ref.at[half, g], vs_sem.at[0], vr_sem.at[i], partner)

    def moments(g):
        lv_mean = collect(LT, g) / jnp.where(row8 < LG, KIN, NOUT)
        lv_new = beta * lvold[g] + (1.0 - beta) * lv_mean
        lvnew[c, g] = lv_new
        rv_new = beta * rvold[g] + (1.0 - beta) * (collect(RV, g) / NI)
        rvnew[c, g] = rv_new
        for i in range(2):
            vec_swap(g, c, i).start()
        scale_l = 1.0 / jnp.sqrt(jnp.where(k96, lv_new, 1.0))
        scale_r = 1.0 / jnp.sqrt(jnp.where(lane8 < Q, rv_new, 1.0))
        wide = jnp.concatenate([scale_r, jnp.ones((LN - 8, LN), F32)], axis=0).T
        tots = jnp.zeros((8, LN), F32)
        lane1 = lane_of((1, LN))
        for lg in range(LG):
            l = g * LG + lg
            rs = [jnp.broadcast_to(wide[:Q, LG * q + lg:LG * q + lg + 1], (Q, LN)) for q in range(4)]
            sc_in = scale_l[lg:lg + 1, :]
            sc_out = jnp.broadcast_to(scale_l[LG + lg:LG + lg + 1, :], (8, LN))
            parts = []
            for i in range(3):
                body = jnp.where(head, sc_in, sc_out[:1]) if i == 2 else sc_in
                lanes = jnp.where(m96, body, roll(sc_out, B96 - 32 * i)[:1])
                u0 = fin[l, block(i), :] * jnp.where(m96, rs[i], rs[3]) * lanes
                fin[l, block(i), :] = u0
                parts.append(u0 * u0)
            inner = pick(m96, parts[0] + parts[1] + pick(head, parts[2]))
            outer = jnp.where(m96, jnp.where(head, 0.0, parts[2]), parts[0] + parts[1] + parts[2])
            v_in = pick(lane1 < B96, lv_new[lg:lg + 1, :])
            v_out = pick((lane1 >= HEAD) & (lane1 < Q), rv_new[2 * LG + lg:2 * LG + lg + 1, :]) + pick(lane1 < Q, rv_new[3 * LG + lg:3 * LG + lg + 1, :])
            for k, val in enumerate((colsum(inner), colsum(outer), v_in, v_out)):
                tots = jnp.where(row8 == LG * k + lg, val, tots)
        post(ST, g, tots)

    def totals(g):
        post(SX, g, jnp.where(only_x, box_st[g, tp], collect(ST, g)))

    def factors(g):
        tot = rowsum(jnp.where(no_x, box_sx[g, x], collect(SX, g)))
        isin = row_of((2 * LG, 1)) < LG
        mean_r = tot[2 * LG:] / jnp.where(isin, NI, NOUT)
        rms = jnp.sqrt(mean_r * tot[:2 * LG] / jnp.where(isin, NI * KIN, NOUT * KO))
        return jnp.sqrt(mean_r) / jnp.maximum(1.0, rms)

    def update(l, lg, fac):
        f_in, f_out = fac[lg:lg + 1, :], fac[LG + lg:LG + lg + 1, :]
        for i in range(3):
            upd = fin[l, block(i), :] * jnp.where((m96 & head) if i == 2 else m96, f_in, f_out)
            new = 0.9 * mpack[l, block(i), :] + 0.1 * upd
            mall[base + l, x, block(i), :] = new.astype(BF16).astype(F32)

    def gather(l, k):
        slot = x if k < 2 else behind(l)
        ref = mall.at[base + l, slot]
        return remote(ref, ref, ags_sem.at[0], agr_sem.at[l, min(k, 1)], at_x(behind(l) if k == 1 else ahead(l)))

    def share(l, k, start):
        ref = mall.at[start + l, (behind(l), ahead(l), across, x)[k]]
        return remote(ref, ref, shs_sem.at[0], shr_sem.at[l], partner)

    def send_pair(l):
        gather(l, 0).start()
        gather(l + 1, 0).start()

    def send_back(l):
        gather(l, 1).start()
        gather(l + 1, 1).start()
        share(l, 3, base).start()
        share(l + 1, 3, base).start()

    def forward_pair(l):
        for k in (l, l + 1):
            gather(k, 0).wait_recv()
            gather(k, 2).start()
            share(k, 0, base).start()

    def settle_pair(l):
        for k in (l, l + 1):
            two = mall.at[base + k, first(2)]
            remote(two, two, ags_sem.at[0], agr_sem.at[k, 1], partner).wait_recv()
            for i in (1, 2):
                share(k, i, base).start()

    rate = rate_ref[0]
    decay = rate * wd_ref[0]

    def unpack(at):
        for q in range(4):
            if q < 3:
                chunk = [mall[at, d, block(q), :] for d in range(RING)]
            else:
                chunk = [last_quarter([mall[at, d, block(i), :] for i in range(3)]) for d in range(RING)]
            r1, r2, r3 = roll(chunk[1], B96), roll(chunk[2], 64), roll(chunk[3], 32)
            mom = (jnp.where(m96, chunk[0], r1), jnp.where(lane < 64, r1, r2), jnp.where(lane < 32, r2, r3))
            spots = (((wn_in, 0, 0, Q),), ((wn_in, Q, 0, Q),), ((wn_in, 2 * Q, 0, HEAD), (wn_out, 0, HEAD, B48)), ((wn_out, B48, 0, Q),))[q]
            for t in range(3):
                for ref, dst, src, num in spots:
                    rows = pl.ds(dst, num)
                    w = ref[at, rows, tile_cols(t)]
                    ref[at, rows, tile_cols(t)] = w - rate * mom[t][src:src + num] - decay * w
        parts = [mall[at, x, block(i), :] for i in range(3)]
        parts.append(last_quarter(parts))
        spots = ((0, 0, Q),), ((Q, 0, Q),), ((2 * Q, 0, HEAD), (MID, HEAD, B48)), ((MID + B48, 0, Q),)
        for val, places in zip(parts, spots):
            val = jnp.where(c == 0, val, roll(val, -B48))
            for dst, src, num in places:
                tall[pl.ds(dst, num), :] = val[src:src + num]
        turned = [tall[tile_cols(t), :].T[:B48] for t in range(3)]
        mn_in[at, :, first(LN)] = turned[0].astype(BF16)
        mn_in[at, :, pl.ds(LN, KI - LN)] = turned[1][:, :KI - LN].astype(BF16)
        mn_out[at] = turned[2][:, :NO].astype(BF16)

    def unpack_pair(l, start):
        lax.fori_loop(start + l, start + l + 2, lambda at, carry: (unpack(at), carry)[1], 0)

    def take_pair(l):
        for k in (l, l + 1):
            four = mall.at[pbase + k]
            remote(four, four, shs_sem.at[0], shr_sem.at[k], partner).wait_recv()
        unpack_pair(l, pbase)

    def new_vectors():
        lane4 = lane_of((LG, LN))
        for half in range(2):
            for g in range(NG):
                rows = pl.ds(LC * half + LG * g, LG)
                both, val = lvnew[half, g], rvnew[half, g]
                both = jnp.where(c == 0, both, roll(both, -B48))
                rn_in[rows, :] = both[:LG, :B48]
                cn_out[rows, :] = both[LG:2 * LG, :B48]
                two = roll(val, Q)[LG:2 * LG]
                cn_in[rows, first(LN)] = jnp.where(lane4 < Q, val[:LG], two)
                cn_in[rows, pl.ds(LN, KI - LN)] = jnp.where(lane4 < 16, two, roll(val, 16)[2 * LG:3 * LG])[:, :KI - LN]
                rn_out[rows, :] = jnp.where(lane4 < B48, roll(val, -HEAD)[2 * LG:3 * LG], roll(val, B48)[3 * LG:])[:, :NO]

    def both(step, g):
        lax.fori_loop(LG * g, LG * g + LG, lambda l, carry: (step(l), carry)[1], 0)

    def swap_start(l):
        swap(l, 0).start()
        swap(l, 1).start()

    def pack_pair(g):
        two = pl.ds(LG * g, LG)
        local(gbuf.at[two], gbuf.at[two], gl_sem.at[g]).wait()
        remote(pbuf.at[two], pbuf.at[two], gs_sem.at[0], gr_sem.at[g], partner).wait_recv()
        if g + 1 < NG:
            both(swap_start, g + 1)
        both(stage_a, g)
        both(lambda l: step1(l).start(), g)

    def rest_pair(g):
        both(lambda l: step3(l).start(), g)
        if g == 0:
            loads[0].wait()
            loads[1].wait()
        both(stage_n, g)

    def relay_pair(g):
        both(stage_b, g)

    def sum_pair(g):
        both(stage_c, g)
        sums_send(g)

    def moment_pair(g):
        two = msend.at[pl.ds(LG * g, LG)]
        remote(two, two, ms_sem.at[0], mr_sem.at[g], partner).wait_recv()
        both(stage_m, g)

    def update_pair(g):
        fac = factors(g)
        for lg in range(LG):
            update(LG * g + lg, lg, fac)

    pack_pair(0)
    rest_pair(0)
    pack_pair(1)
    w_loads[0].start()
    w_loads[1].start()
    old_vectors()
    pl.semaphore_wait(ready, RING - 1)
    relay_pair(0)
    rest_pair(1)
    pack_pair(2)
    sum_pair(0)
    relay_pair(1)
    rest_pair(2)
    moment_pair(0)
    pack_pair(3)
    moments(0)
    sum_pair(1)
    relay_pair(2)
    rest_pair(3)
    moment_pair(1)
    totals(0)
    relay_pair(3)
    moments(1)
    sum_pair(2)
    moment_pair(2)
    update_pair(0)
    send_pair(0)
    totals(1)
    send_back(0)
    sum_pair(3)
    moment_pair(3)
    moments(2)
    forward_pair(0)
    update_pair(1)
    send_pair(2)
    moments(3)
    totals(2)
    send_back(2)
    settle_pair(0)
    w_loads[0].wait()
    w_loads[1].wait()
    unpack_pair(0, base)
    forward_pair(2)
    totals(3)
    update_pair(2)
    send_pair(4)
    send_back(4)
    take_pair(0)
    settle_pair(2)
    update_pair(3)
    send_pair(6)
    forward_pair(4)
    send_back(6)
    unpack_pair(2, base)
    take_pair(2)
    for i, ref in enumerate((lvnew, rvnew)):
        remote(ref.at[other], ref.at[other], vs_sem.at[0], vr_sem.at[i], partner).wait_recv()
    new_vectors()
    forward_pair(6)
    settle_pair(4)
    unpack_pair(4, base)
    take_pair(4)
    settle_pair(6)
    unpack_pair(6, base)
    take_pair(6)
    for ref, sem in ((pbuf, gs_sem), (msend, ms_sem), (mall.at[first(6)], s_sem), (mall.at[first(6)], ags_sem), (mall.at[first(8)], shs_sem),
                     (lraw.at[0], os_sem), (mt.at[first(3)], sts_sem), (lvnew, vs_sem)):
        remote(ref, ref, sem.at[0], os_sem.at[1], partner).wait_send()


def update_call(scalars, arrays):
    hbm, smem = pl.BlockSpec(memory_space=pltpu.HBM), pl.BlockSpec(memory_space=pltpu.SMEM)
    dma, vmem = pltpu.SemaphoreType.DMA, pltpu.VMEM

    def lanes(*lead):
        return vmem(lead + (LN,), F32)

    scratch = [
        vmem((LC, KI + NO, D), F32), vmem((LC, KI + NO, D), F32), lanes(LC, RING, CH), lanes(LC, CH), lanes(LC, 2, CH), lanes(LC, CH),
        lanes(L, RING, CH), vmem((L, B48, KI), BF16), vmem((L, B48, NO), BF16), vmem((LC, B48, D), F32), vmem((LC, LN, D), F32),
        lanes(LC, CH), lanes(D), lanes(NG, LN), lanes(NG, 8),
        vmem((2, 2, LC, B48), F32), vmem((LC, KI), F32), vmem((LC, NO), F32), lanes(3, 2, LC),
        lanes(NG, 8), lanes(NG, 8), lanes(2, NG, 8), lanes(2, NG, 8),
        lanes(NG, RING, 8), lanes(NG, RING, 8), lanes(NG, TP, 8), lanes(NG, TP, 8),
        dma((NG,)), dma((1,)), dma((NG,)), dma((2,)), dma((1,)), dma((NG,)), dma((1,)), dma((LC,)), dma((LC,)), dma((1,)), dma((LC, 2)),
        dma((1,)), dma((LC,)), dma((1,)), dma((NG, len(KINDS))), dma((1,)), dma((2,)), dma((4,)), dma((2,)), dma((2,)), pltpu.SemaphoreType.REGULAR,
    ]
    outs = [((L, KI, D), F32), ((L, NO, D), F32), ((L, B48, KI), BF16), ((L, B48, NO), BF16),
            ((L, B48), F32), ((L, KI), F32), ((L, NO), F32), ((L, B48), F32)]
    return pl.pallas_call(
        kernel,
        out_shape=[vmem(*out) for out in outs],
        in_specs=[smem] * len(scalars) + [hbm] * len(arrays),
        out_specs=[pl.BlockSpec(memory_space=vmem)] * len(outs),
        scratch_shapes=scratch,
        compiler_params=pltpu.CompilerParams(collective_id=0, has_side_effects=True, vmem_limit_bytes=36 * 2**20),
        name='adafactor',
    )(*[val.reshape(1) for val in scalars], *[pltpu.with_memory_space_constraint(val, pltpu.HBM) for val in arrays])


def store_kernel(*refs):
    num = len(refs) // 2
    copies = [pltpu.make_async_copy(src, dst, refs[-1].at[i]) for i, (src, dst) in enumerate(zip(refs[:num], refs[num:-1]))]
    for copy in copies:
        copy.start()
    for copy in copies:
        copy.wait()


def store_call(vals):
    anyspace = pl.BlockSpec(memory_space=pl.ANY)
    return pl.pallas_call(
        store_kernel,
        out_shape=[jax.ShapeDtypeStruct(val.shape, val.dtype) for val in vals],
        in_specs=[anyspace] * len(vals),
        out_specs=[anyspace] * len(vals),
        scratch_shapes=[pltpu.SemaphoreType.DMA((len(vals),))],
        compiler_params=pltpu.CompilerParams(vmem_limit_bytes=2**20),
        name='store',
    )(*[pltpu.with_memory_space_constraint(val, pltpu.VMEM) for val in vals])


def solution(mesh):
    def turn(val):
        return val.swapaxes(1, 2)

    def body(w_in, w_out, g_in, g_out, m_in, m_out, r_in, c_in, r_out, c_out, learn_rate, weight_decay, beta_two):
        out = store_call(update_call((learn_rate, weight_decay, beta_two),
                          (turn(w_in), w_out, turn(g_in[0]), g_out[0], m_in, turn(m_out), r_in, c_in, r_out, c_out)))
        return (turn(out[0]), out[1], out[2], turn(out[3])) + tuple(out[4:])

    cols, rows, own = P(None, None, 'tp'), P(None, 'tp', None), P(None, 'dp')
    outs = (cols, rows, P(None, 'dp', 'tp'), P(None, 'tp', 'dp'), own, P(None, 'tp'), P(None, 'tp'), own)
    in_specs = (cols, rows, P('dp', *cols), P('dp', *rows)) + outs[2:] + (P(), P(), P())
    return jax.shard_map(body, mesh=mesh, in_specs=in_specs, out_specs=outs, check_vma=False)
```

```python
import jax
import jax.numpy as jnp
from jax import lax
from jax.experimental import pallas as pl
from jax.experimental.pallas import tpu as pltpu
from jax.sharding import PartitionSpec as P

F32, BF16 = jnp.float32, jnp.bfloat16
MESH = pl.DeviceIdType.MESH
RING = 4
L, D = 16, 384
KI, NO = 168, 120
LC, LG, NG = 8, 2, 4
Q, LN, B48, B96 = 72, 128, 48, 96
CH, HEAD, MID, HALF = 3 * Q, KI - 2 * Q, 256, 104
NI, KIN, NOUT, KO = 384.0, 2688.0, 1920.0, 384.0
KINDS = RV, SX, LT, ST = range(4)
TP = RING * RING


def roll(val, shift):
    return pltpu.roll(val, shift % LN, 1)


def lane_of(shape):
    return lax.broadcasted_iota(jnp.int32, shape, 1)


def row_of(shape):
    return lax.broadcasted_iota(jnp.int32, shape, 0)


def colsum(val):
    return jnp.sum(val, axis=0, keepdims=True)


def rowsum(val):
    return jnp.sum(val, axis=1, keepdims=True)


def pick(cond, val):
    return jnp.where(cond, val, 0.0)


def first(num):
    return pl.ds(0, num)


def block(i):
    return pl.ds(Q * i, Q)


def tile_cols(t):
    return pl.ds(LN * t, LN)


def last_quarter(parts):
    lane = lane_of(parts[0].shape)
    tail = jnp.where(lane < 64, roll(parts[1], 64), roll(parts[2], B96))
    return jnp.where(lane < 32, roll(parts[0], 32), tail)


def join_quarters(quarters, keep):
    return [jnp.where(keep, quarters[i], roll(quarters[3], B96 - 32 * i)) for i in range(3)]


def kernel(rate_ref, wd_ref, beta_ref, w_in, w_out, g_in, g_out, m_in, m_out, r_in, c_in, r_out, c_out,
           wn_in, wn_out, mn_in, mn_out, rn_in, cn_in, rn_out, cn_out,
           gbuf, pbuf, gsend, pack, via, rin, fin, mall, mraw_in, mraw_out, msend, mt, mpack, tall,
           rvacc, lvacc, lraw, craw, oraw, pads, lvold, rvold, lvnew, rvnew, box_rv, box_sx, box_lt, box_st,
           gl_sem, gp_sem, gs_sem, gr_sem, ml_sem, ms_sem, mr_sem, s_sem, via_sem, rin_sem, ags_sem, agr_sem,
           shs_sem, shr_sem, sts_sem, str_sem, vs_sem, vr_sem, ol_sem, os_sem, wl_sem, ready):
    tp, dp = lax.axis_index('tp'), lax.axis_index('dp')
    z, y, x, c = tp // RING, tp % RING, dp // 2, dp % 2
    other = 1 - c
    base, pbase = c * LC, other * LC

    def at_x(xx):
        return {'dp': (xx % RING) * 2 + c}

    def at_y(yy):
        return {'tp': z * RING + yy % RING}

    def at_z(zz):
        return {'tp': (zz % RING) * RING + y}

    partner = {'dp': x * 2 + other}

    def local(src, dst, sem):
        return pltpu.make_async_copy(src, dst, sem)

    def remote(src, dst, send_sem, recv_sem, device):
        return pltpu.make_async_remote_copy(src_ref=src, dst_ref=dst, send_sem=send_sem, recv_sem=recv_sem,
                                            device_id=device, device_id_type=MESH)

    barrier = pltpu.get_barrier_semaphore()
    peers = [partner]
    for k in range(1, RING):
        peers += [at_x(x + k), at_y(y + k), at_z(z + k)]
    for peer in peers:
        pl.semaphore_signal(barrier, inc=1, device_id=peer, device_id_type=MESH)

    def own(l, i):
        src, dst = ((g_in, first(KI)), (g_out, pl.ds(KI, NO)))[i]
        return local(src.at[base + l], gbuf.at[l, dst], gl_sem.at[NG + l] if isinstance(l, int) else gl_sem.at[l // LG])

    def others(l, i):
        src, dst = ((g_in, first(KI)), (g_out, pl.ds(KI, NO)))[i]
        return local(src.at[pbase + l], gsend.at[l, dst], gp_sem.at[l])

    def swap_first(l):
        return remote(gsend.at[l], pbuf.at[l], gs_sem.at[0], gr_sem.at[NG + l], partner)

    def swap(l, i):
        src, dst = ((g_in, first(KI)), (g_out, pl.ds(KI, NO)))[i]
        return remote(src.at[pbase + l], pbuf.at[l, dst], gs_sem.at[0], gr_sem.at[l // LG], partner)

    my_rows, its_rows = pl.ds(base, LC), pl.ds(pbase, LC)
    loads = [local(m_in, mraw_in, ml_sem.at[0]), local(m_out, mraw_out, ml_sem.at[1]),
             local(r_in.at[my_rows], lraw.at[0, c], ol_sem.at[0]), local(c_out.at[my_rows], lraw.at[1, c], ol_sem.at[1]),
             local(c_in.at[my_rows], craw, ol_sem.at[2]), local(r_out.at[my_rows], oraw, ol_sem.at[3])]
    w_loads = [local(w_in, wn_in, wl_sem.at[0]), local(w_out, wn_out, wl_sem.at[1])]

    def lane_swap(m, core):
        return remote((r_in, c_out)[m].at[its_rows], lraw.at[m, core], os_sem.at[0], os_sem.at[1], partner)

    def start_loads(l, carry):
        own(l, 0).start()
        own(l, 1).start()
        return carry

    for l in range(LG):
        for i in range(2):
            others(l, i).start()
            own(l, i).start()
    lax.fori_loop(LG, LC, start_loads, 0)
    for copy in loads:
        copy.start()
    pl.semaphore_wait(barrier, len(peers))
    for k in range(1, RING):
        pl.semaphore_signal(ready, inc=1, device_id=at_y(y + k), device_id_type=MESH)
    for l in range(LG):
        local(gsend.at[l], gsend.at[l], gp_sem.at[l]).wait()
        swap_first(l).start()
    lane_swap(0, c).start()
    lane_swap(1, c).start()
    rvacc[...] = jnp.zeros_like(rvacc)
    lvacc[...] = jnp.zeros_like(lvacc)

    lane, lane8, row8 = lane_of((Q, LN)), lane_of((8, LN)), row_of((8, LN))
    m96, k96 = lane < B96, lane8 < B96
    head = row_of((Q, LN)) < HEAD
    no_x, only_x = row8 >= 3 * LG, (row8 >= 2 * LG) & (row8 < 3 * LG)

    def way(l):
        return 1 - 2 * (l % 2)

    def ahead(l):
        return (x + way(l) + RING) % RING

    def behind(l):
        return (x - way(l) + RING) % RING

    across = (x + 2) % RING

    def step1(l):
        return remote(pack.at[l, across], via.at[l], s_sem.at[0], via_sem.at[l], at_x(ahead(l)))

    def step2(l):
        return remote(pack.at[l, ahead(l)], rin.at[l, 0], s_sem.at[0], rin_sem.at[l // LG], at_x(ahead(l)))

    def step3(l):
        return remote(pack.at[l, behind(l)], rin.at[l, 1], s_sem.at[0], rin_sem.at[l // LG], at_x(behind(l)))

    def m_rows(core):
        return pl.ds(pl.multiple_of(core * B48, 16), B48)

    def moment_swap(l, core):
        return remote(msend.at[l], mt.at[l, m_rows(core)], ms_sem.at[0], mr_sem.at[l // LG], partner)

    def stage_a(l):
        def tile(t, q):
            return gbuf[l, block(q), tile_cols(t)] + pbuf[l, block(q), tile_cols(t)]

        def chunk(d, q):
            if d == 0:
                return tile(0, q)
            if d == 1:
                return roll(jnp.where(m96, tile(1, q), tile(0, q)), 32)
            if d == 2:
                return roll(jnp.where(lane < 64, tile(2, q), tile(1, q)), 64)
            return roll(tile(2, q), B96)

        for d in range(RING):
            for i, val in enumerate(join_quarters([chunk(d, q) for q in range(4)], m96)):
                pack[l, d, block(i), :] = val

    def stage_n(l):
        msend[l, :, first(KI)] = mraw_in[pbase + l].astype(F32)
        msend[l, :, pl.ds(MID, NO)] = mraw_out[pbase + l].astype(F32)
        moment_swap(l, c).start()
        mt[l, m_rows(c), first(KI)] = mraw_in[base + l].astype(F32)
        mt[l, m_rows(c), pl.ds(MID, NO)] = mraw_out[base + l].astype(F32)

    def stage_b(l):
        step1(l).wait_recv()
        to = ahead(l)
        pack[l, to] = pack[l, to] + via[l]
        step2(l).start()

    def stage_c(l):
        sq = []
        for i in range(3):
            grad = pack[l, x, block(i), :] + rin[l, 0, block(i), :] + rin[l, 1, block(i), :]
            fin[l, block(i), :] = grad
            sq.append(grad * grad + 1e-30)
        g, lg = l // LG, l % LG
        sums = [rowsum(pick(m96, val)) for val in sq]
        sums.append(rowsum(jnp.where(m96, 0.0, sq[0] + sq[1] + sq[2])))
        acc = rvacc[g, first(Q), :]
        for q in range(4):
            acc = jnp.where(lane == LG * q + lg, sums[q], acc)
        rvacc[g, first(Q), :] = acc
        top = colsum(pick(head, sq[2]))
        low = colsum(jnp.where(head, 0.0, sq[2]))
        cols = [colsum(sq[0]), colsum(sq[1])]
        wide = [jnp.broadcast_to(val, (8, LN)) for val in (cols[0], cols[1], top + low)]
        in_sum = pick(k96, cols[0] + cols[1] + top)
        out_sum = pick(k96, low + last_quarter(wide))
        both = jnp.where(row8 == lg, in_sum, lvacc[g])
        lvacc[g] = jnp.where(row8 == LG + lg, out_sum, both)

    def stage_m(l):
        val = mt[l].T
        third = jnp.concatenate([val[2 * Q:KI], val[MID:MID + B48]], axis=0)
        quarters = [val[:Q], val[Q:2 * Q], third, val[MID + B48:MID + NO]]
        for i, part in enumerate(join_quarters(quarters, m96)):
            mpack[l, block(i), :] = part

    boxes = {RV: (box_rv, x, RING), SX: (box_sx, x, RING), LT: (box_lt, tp, TP), ST: (box_st, tp, TP)}

    def post(kind, g, val):
        box, me, num = boxes[kind]
        box[g, me] = val

        def send(k, carry):
            device = at_x(me + k) if num == RING else {'tp': (me + k) % TP}
            remote(box.at[g, me], box.at[g, me], sts_sem.at[0], str_sem.at[g, kind], device).start()
            return carry

        lax.fori_loop(1, num, send, 0)

    def collect(kind, g):
        box, me, num = boxes[kind]
        rest = box.at[g, first(num - 1)]
        remote(rest, rest, sts_sem.at[0], str_sem.at[g, kind], partner).wait_recv()
        val = box[g, 0]
        for k in range(1, num):
            val = val + box[g, k]
        return val

    def sums_send(g):
        post(LT, g, lvacc[g])
        post(RV, g, rvacc[g].T[:8])

    beta = beta_ref[0]

    def old_vectors():
        for copy in loads[2:]:
            copy.wait()
        remote(lraw.at[0], lraw.at[0], os_sem.at[0], os_sem.at[1], partner).wait_recv()
        for m in range(2):
            for core in range(2):
                pads[m, core, :, first(B48)] = lraw[m, core]
        pads[2, 0, :, first(KI - LN)] = craw[:, pl.ds(LN, KI - LN)]
        pads[2, 1, :, first(NO)] = oraw[...]
        low, high, rest = craw[:, first(LN)], pads[2, 0], pads[2, 1]
        lanes = [jnp.where(lane8 < B48, pads[m, 0], roll(pads[m, 1], B48)) for m in range(2)]
        rows = [low, jnp.where(lane8 < LN - Q, roll(low, -Q), roll(high, -Q)),
                jnp.where(lane8 < HEAD, roll(high, -16), roll(rest, HEAD)), roll(rest, -B48)]
        for g in range(NG):
            part = slice(LG * g, LG * g + LG)
            lvold[g] = jnp.concatenate([val[part] for val in lanes + lanes], axis=0)
            rvold[g] = jnp.concatenate([val[part] for val in rows], axis=0)

    def vec_swap(g, half, i):
        ref = (lvnew, rvnew)[i]
        return remote(ref.at[half, g], ref.at[half, g], vs_sem.at[0], vr_sem.at[i], partner)

    def moments(g):
        lv_mean = collect(LT, g) / jnp.where(row8 < LG, KIN, NOUT)
        lv_new = beta * lvold[g] + (1.0 - beta) * lv_mean
        lvnew[c, g] = lv_new
        rv_new = beta * rvold[g] + (1.0 - beta) * (collect(RV, g) / NI)
        rvnew[c, g] = rv_new
        for i in range(2):
            vec_swap(g, c, i).start()
        scale_l = 1.0 / jnp.sqrt(jnp.where(k96, lv_new, 1.0))
        scale_r = 1.0 / jnp.sqrt(jnp.where(lane8 < Q, rv_new, 1.0))
        wide = jnp.concatenate([scale_r, jnp.ones((LN - 8, LN), F32)], axis=0).T
        tots = jnp.zeros((8, LN), F32)
        lane1 = lane_of((1, LN))
        for lg in range(LG):
            l = g * LG + lg
            rs = [jnp.broadcast_to(wide[:Q, LG * q + lg:LG * q + lg + 1], (Q, LN)) for q in range(4)]
            sc_in = scale_l[lg:lg + 1, :]
            sc_out = jnp.broadcast_to(scale_l[LG + lg:LG + lg + 1, :], (8, LN))
            parts = []
            for i in range(3):
                body = jnp.where(head, sc_in, sc_out[:1]) if i == 2 else sc_in
                lanes = jnp.where(m96, body, roll(sc_out, B96 - 32 * i)[:1])
                u0 = fin[l, block(i), :] * jnp.where(m96, rs[i], rs[3]) * lanes
                fin[l, block(i), :] = u0
                parts.append(u0 * u0)
            inner = pick(m96, parts[0] + parts[1] + pick(head, parts[2]))
            outer = jnp.where(m96, jnp.where(head, 0.0, parts[2]), parts[0] + parts[1] + parts[2])
            v_in = pick(lane1 < B96, lv_new[lg:lg + 1, :])
            v_out = pick((lane1 >= HEAD) & (lane1 < Q), rv_new[2 * LG + lg:2 * LG + lg + 1, :]) + pick(lane1 < Q, rv_new[3 * LG + lg:3 * LG + lg + 1, :])
            for k, val in enumerate((colsum(inner), colsum(outer), v_in, v_out)):
                tots = jnp.where(row8 == LG * k + lg, val, tots)
        post(ST, g, tots)

    def totals(g):
        post(SX, g, jnp.where(only_x, box_st[g, tp], collect(ST, g)))

    def factors(g):
        tot = rowsum(jnp.where(no_x, box_sx[g, x], collect(SX, g)))
        isin = row_of((2 * LG, 1)) < LG
        mean_r = tot[2 * LG:] / jnp.where(isin, NI, NOUT)
        rms = jnp.sqrt(mean_r * tot[:2 * LG] / jnp.where(isin, NI * KIN, NOUT * KO))
        return jnp.sqrt(mean_r) / jnp.maximum(1.0, rms)

    def update(l, lg, fac):
        f_in, f_out = fac[lg:lg + 1, :], fac[LG + lg:LG + lg + 1, :]
        for i in range(3):
            upd = fin[l, block(i), :] * jnp.where((m96 & head) if i == 2 else m96, f_in, f_out)
            new = 0.9 * mpack[l, block(i), :] + 0.1 * upd
            mall[base + l, x, block(i), :] = new.astype(BF16).astype(F32)

    def arrived(l, k):
        return l if k == 0 else LC + NG if k == 1 and l >= LC - LG else LC + l // LG

    def gather(l, k):
        slot = x if k < 2 else behind(l)
        ref = mall.at[base + l, slot]
        return remote(ref, ref, ags_sem.at[0], agr_sem.at[arrived(l, k)], at_x(behind(l) if k == 1 else ahead(l)))

    def share(l, k, start):
        ref = mall.at[start + l, (behind(l), ahead(l), across, x)[k]]
        return remote(ref, ref, shs_sem.at[0], shr_sem.at[NG if k == 3 and l >= LC - LG else l // LG], partner)

    def send_pair(l):
        gather(l, 0).start()
        gather(l + 1, 0).start()

    def send_back(l):
        gather(l, 1).start()
        gather(l + 1, 1).start()
        share(l, 3, base).start()
        share(l + 1, 3, base).start()

    def forward_pair(l):
        for k in (l, l + 1):
            gather(k, 0).wait_recv()
            gather(k, 2).start()
            share(k, 0, base).start()

    def half(ref, h):
        return ref.at[(first(HALF), pl.ds(HALF, CH - HALF))[h]]

    def gather_half(l, h, slot):
        ref = half(mall.at[base + l, slot], h)
        return remote(ref, ref, ags_sem.at[0], agr_sem.at[l if h == 0 else LC + NG + 1 + l], at_x(ahead(l)))

    def send_first():
        for h in range(2):
            for l in range(LG):
                gather_half(l, h, x).start()

    def forward_first():
        for h in range(2):
            for l in range(LG):
                gather_half(l, h, behind(l)).wait_recv()
                ref = half(mall.at[base + l, behind(l)], h)
                remote(ref, ref, ags_sem.at[0], agr_sem.at[arrived(l, 2)], at_x(ahead(l))).start()
        share(0, 0, base).start()
        share(1, 0, base).start()

    def settle_pair(l):
        four = mall.at[base + l]
        remote(four, four, ags_sem.at[0], agr_sem.at[LC + l // LG], partner).wait_recv()
        for k in (l, l + 1):
            for i in (1, 2):
                share(k, i, base).start()

    def settle_last(k):
        l = LC - LG
        two = mall.at[base + l, first(LG)]
        remote(two, two, ags_sem.at[0], agr_sem.at[arrived(l, k)], partner).wait_recv()
        share(l, k, base).start()
        share(l + 1, k, base).start()

    rate = rate_ref[0]
    decay = rate * wd_ref[0]

    def unpack(at):
        for q in range(4):
            if q < 3:
                chunk = [mall[at, d, block(q), :] for d in range(RING)]
            else:
                chunk = [last_quarter([mall[at, d, block(i), :] for i in range(3)]) for d in range(RING)]
            r1, r2, r3 = roll(chunk[1], B96), roll(chunk[2], 64), roll(chunk[3], 32)
            mom = (jnp.where(m96, chunk[0], r1), jnp.where(lane < 64, r1, r2), jnp.where(lane < 32, r2, r3))
            spots = (((wn_in, 0, 0, Q),), ((wn_in, Q, 0, Q),), ((wn_in, 2 * Q, 0, HEAD), (wn_out, 0, HEAD, B48)), ((wn_out, B48, 0, Q),))[q]
            for t in range(3):
                for ref, dst, src, num in spots:
                    rows = pl.ds(dst, num)
                    w = ref[at, rows, tile_cols(t)]
                    ref[at, rows, tile_cols(t)] = w - rate * mom[t][src:src + num] - decay * w

    def turn_moment(at):
        parts = [mall[at, x, block(i), :] for i in range(3)]
        parts.append(last_quarter(parts))
        spots = ((0, 0, Q),), ((Q, 0, Q),), ((2 * Q, 0, HEAD), (MID, HEAD, B48)), ((MID + B48, 0, Q),)
        for val, places in zip(parts, spots):
            val = jnp.where(c == 0, val, roll(val, -B48))
            for dst, src, num in places:
                tall[pl.ds(dst, num), :] = val[src:src + num]
        turned = [tall[tile_cols(t), :].T[:B48] for t in range(3)]
        mn_in[at, :, first(LN)] = turned[0].astype(BF16)
        mn_in[at, :, pl.ds(LN, KI - LN)] = turned[1][:, :KI - LN].astype(BF16)
        mn_out[at] = turned[2][:, :NO].astype(BF16)

    def each(step, l, start):
        lax.fori_loop(start + l, start + l + LG, lambda at, carry: (step(at), carry)[1], 0)

    def unpack_pair(l, start):
        each(unpack, l, start)
        if l < LC - LG:
            each(turn_moment, l, start)

    def turn_last():
        l = LC - LG
        each(turn_moment, l, base)
        two = mall.at[base, first(LG)]
        remote(two, two, shs_sem.at[0], shr_sem.at[NG], partner).wait_recv()
        each(turn_moment, l, pbase)

    def take_pair(l):
        two = mall.at[pl.ds(pbase + l, LG)] if l < LC - LG else mall.at[pl.ds(pbase + l, LG), first(3)]
        remote(two, two, shs_sem.at[0], shr_sem.at[l // LG], partner).wait_recv()
        unpack_pair(l, pbase)

    def new_vectors():
        lane4 = lane_of((LG, LN))
        for half in range(2):
            for g in range(NG):
                rows = pl.ds(LC * half + LG * g, LG)
                both, val = lvnew[half, g], rvnew[half, g]
                both = jnp.where(c == 0, both, roll(both, -B48))
                rn_in[rows, :] = both[:LG, :B48]
                cn_out[rows, :] = both[LG:2 * LG, :B48]
                two = roll(val, Q)[LG:2 * LG]
                cn_in[rows, first(LN)] = jnp.where(lane4 < Q, val[:LG], two)
                cn_in[rows, pl.ds(LN, KI - LN)] = jnp.where(lane4 < 16, two, roll(val, 16)[2 * LG:3 * LG])[:, :KI - LN]
                rn_out[rows, :] = jnp.where(lane4 < B48, roll(val, -HEAD)[2 * LG:3 * LG], roll(val, B48)[3 * LG:])[:, :NO]

    def both(step, g):
        lax.fori_loop(LG * g, LG * g + LG, lambda l, carry: (step(l), carry)[1], 0)

    def swap_start(l):
        swap(l, 0).start()
        swap(l, 1).start()

    def pack_first():
        for l in range(LG):
            local(gbuf.at[l], gbuf.at[l], gl_sem.at[NG + l]).wait()
            swap_first(l).wait_recv()
            stage_a(l)
            step1(l).start()
            if l == 0:
                both(swap_start, 1)
        both(lambda l: step3(l).start(), 0)

    def pack_pair(g):
        two = pl.ds(LG * g, LG)
        local(gbuf.at[two], gbuf.at[two], gl_sem.at[g]).wait()
        remote(pbuf.at[two], pbuf.at[two], gs_sem.at[0], gr_sem.at[g], partner).wait_recv()
        if g + 1 < NG:
            both(swap_start, g + 1)
        both(stage_a, g)
        both(lambda l: step1(l).start(), g)

    def direct_pair(g):
        both(lambda l: step3(l).start(), g)

    def cast_pair(g):
        if g == 0:
            loads[0].wait()
            loads[1].wait()
        both(stage_n, g)

    def relay_pair(g):
        both(stage_b, g)

    def sum_pair(g):
        two = rin.at[pl.ds(LG * g, LG)]
        remote(two, two, s_sem.at[0], rin_sem.at[g], partner).wait_recv()
        both(stage_c, g)
        sums_send(g)

    def moment_pair(g):
        two = msend.at[pl.ds(LG * g, LG)]
        remote(two, two, ms_sem.at[0], mr_sem.at[g], partner).wait_recv()
        both(stage_m, g)

    def update_pair(g):
        fac = factors(g)
        for lg in range(LG):
            update(LG * g + lg, lg, fac)

    pack_first()
    cast_pair(0)
    pack_pair(1)
    w_loads[0].start()
    w_loads[1].start()
    old_vectors()
    pl.semaphore_wait(ready, RING - 1)
    relay_pair(0)
    direct_pair(1)
    cast_pair(1)
    pack_pair(2)
    sum_pair(0)
    relay_pair(1)
    direct_pair(2)
    cast_pair(2)
    moment_pair(0)
    pack_pair(3)
    moments(0)
    sum_pair(1)
    relay_pair(2)
    cast_pair(3)
    moment_pair(1)
    totals(0)
    direct_pair(3)
    relay_pair(3)
    moments(1)
    sum_pair(2)
    moment_pair(2)
    update_pair(0)
    send_first()
    totals(1)
    send_back(0)
    sum_pair(3)
    moment_pair(3)
    moments(2)
    forward_first()
    update_pair(1)
    send_pair(2)
    moments(3)
    totals(2)
    send_back(2)
    forward_pair(2)
    settle_pair(0)
    totals(3)
    update_pair(2)
    send_pair(4)
    send_back(4)
    w_loads[0].wait()
    w_loads[1].wait()
    unpack_pair(0, base)
    take_pair(0)
    settle_pair(2)
    update_pair(3)
    send_pair(6)
    forward_pair(4)
    send_back(6)
    unpack_pair(2, base)
    take_pair(2)
    for i, ref in enumerate((lvnew, rvnew)):
        remote(ref.at[other], ref.at[other], vs_sem.at[0], vr_sem.at[i], partner).wait_recv()
    new_vectors()
    turn_last()
    forward_pair(6)
    settle_pair(4)
    unpack_pair(4, base)
    settle_last(1)
    take_pair(4)
    settle_last(2)
    unpack_pair(6, base)
    take_pair(6)
    for ref, sem in ((pbuf, gs_sem), (msend, ms_sem), (mall.at[first(6)], s_sem), (mall.at[first(6)], ags_sem), (mall.at[first(8)], shs_sem),
                     (lraw.at[0], os_sem), (mt.at[first(3)], sts_sem), (lvnew, vs_sem)):
        remote(ref, ref, sem.at[0], os_sem.at[1], partner).wait_send()


def update_call(scalars, arrays):
    hbm, smem = pl.BlockSpec(memory_space=pltpu.HBM), pl.BlockSpec(memory_space=pltpu.SMEM)
    dma, vmem = pltpu.SemaphoreType.DMA, pltpu.VMEM

    def lanes(*lead):
        return vmem(lead + (LN,), F32)

    scratch = [
        vmem((LC, KI + NO, D), F32), vmem((LC, KI + NO, D), F32), vmem((LG, KI + NO, D), F32), lanes(LC, RING, CH), lanes(LC, CH), lanes(LC, 2, CH), lanes(LC, CH),
        lanes(L, RING, CH), vmem((L, B48, KI), BF16), vmem((L, B48, NO), BF16), vmem((LC, B48, D), F32), vmem((LC, LN, D), F32),
        lanes(LC, CH), lanes(D), lanes(NG, LN), lanes(NG, 8),
        vmem((2, 2, LC, B48), F32), vmem((LC, KI), F32), vmem((LC, NO), F32), lanes(3, 2, LC),
        lanes(NG, 8), lanes(NG, 8), lanes(2, NG, 8), lanes(2, NG, 8),
        lanes(NG, RING, 8), lanes(NG, RING, 8), lanes(NG, TP, 8), lanes(NG, TP, 8),
        dma((NG + LG,)), dma((LG,)), dma((1,)), dma((NG + LG,)), dma((2,)), dma((1,)), dma((NG,)), dma((1,)), dma((LC,)), dma((NG,)),
        dma((1,)), dma((LC + NG + 1 + LG,)), dma((1,)), dma((NG + 1,)), dma((1,)), dma((NG, len(KINDS))), dma((1,)), dma((2,)), dma((4,)),
        dma((2,)), dma((2,)), pltpu.SemaphoreType.REGULAR,
    ]
    outs = [((L, KI, D), F32), ((L, NO, D), F32), ((L, B48, KI), BF16), ((L, B48, NO), BF16),
            ((L, B48), F32), ((L, KI), F32), ((L, NO), F32), ((L, B48), F32)]
    return pl.pallas_call(
        kernel,
        out_shape=[vmem(*out) for out in outs],
        in_specs=[smem] * len(scalars) + [hbm] * len(arrays),
        out_specs=[pl.BlockSpec(memory_space=vmem)] * len(outs),
        scratch_shapes=scratch,
        compiler_params=pltpu.CompilerParams(collective_id=0, has_side_effects=True, vmem_limit_bytes=36 * 2**20),
        name='adafactor',
    )(*[val.reshape(1) for val in scalars], *[pltpu.with_memory_space_constraint(val, pltpu.HBM) for val in arrays])


def store_kernel(*refs):
    num = len(refs) // 2
    copies = [pltpu.make_async_copy(src, dst, refs[-1].at[i]) for i, (src, dst) in enumerate(zip(refs[:num], refs[num:-1]))]
    for copy in copies:
        copy.start()
    for copy in copies:
        copy.wait()


def store_call(vals):
    anyspace = pl.BlockSpec(memory_space=pl.ANY)
    return pl.pallas_call(
        store_kernel,
        out_shape=[jax.ShapeDtypeStruct(val.shape, val.dtype) for val in vals],
        in_specs=[anyspace] * len(vals),
        out_specs=[anyspace] * len(vals),
        scratch_shapes=[pltpu.SemaphoreType.DMA((len(vals),))],
        compiler_params=pltpu.CompilerParams(vmem_limit_bytes=2**20),
        name='store',
    )(*[pltpu.with_memory_space_constraint(val, pltpu.VMEM) for val in vals])


def solution(mesh):
    def turn(val):
        return val.swapaxes(1, 2)

    def body(w_in, w_out, g_in, g_out, m_in, m_out, r_in, c_in, r_out, c_out, learn_rate, weight_decay, beta_two):
        out = store_call(update_call((learn_rate, weight_decay, beta_two),
                          (turn(w_in), w_out, turn(g_in[0]), g_out[0], m_in, turn(m_out), r_in, c_in, r_out, c_out)))
        return (turn(out[0]), out[1], out[2], turn(out[3])) + tuple(out[4:])

    cols, rows, own = P(None, None, 'tp'), P(None, 'tp', None), P(None, 'dp')
    outs = (cols, rows, P(None, 'dp', 'tp'), P(None, 'tp', 'dp'), own, P(None, 'tp'), P(None, 'tp'), own)
    in_specs = (cols, rows, P('dp', *cols), P('dp', *rows)) + outs[2:] + (P(), P(), P())
    return jax.shard_map(body, mesh=mesh, in_specs=in_specs, out_specs=outs, check_vma=False)
```

```python
import jax
import jax.numpy as jnp
from jax import lax
from jax.experimental import pallas as pl
from jax.experimental.pallas import tpu as pltpu
from jax.sharding import PartitionSpec as P

F32, BF16 = jnp.float32, jnp.bfloat16
MESH = pl.DeviceIdType.MESH
RING = 4
L, D = 16, 384
KI, NO = 168, 120
LC, LG, NG = 8, 2, 4
Q, LN, B48, B96 = 72, 128, 48, 96
CH, HEAD, MID, HALF = 3 * Q, KI - 2 * Q, 256, 104
NI, KIN, NOUT, KO = 384.0, 2688.0, 1920.0, 384.0
KINDS = RV, SX, LT, ST = range(4)
TP = RING * RING


def roll(val, shift):
    return pltpu.roll(val, shift % LN, 1)


def lane_of(shape):
    return lax.broadcasted_iota(jnp.int32, shape, 1)


def row_of(shape):
    return lax.broadcasted_iota(jnp.int32, shape, 0)


def colsum(val):
    return jnp.sum(val, axis=0, keepdims=True)


def rowsum(val):
    return jnp.sum(val, axis=1, keepdims=True)


def pick(cond, val):
    return jnp.where(cond, val, 0.0)


def first(num):
    return pl.ds(0, num)


def block(i):
    return pl.ds(Q * i, Q)


def tile_cols(t):
    return pl.ds(LN * t, LN)


def last_quarter(parts):
    lane = lane_of(parts[0].shape)
    tail = jnp.where(lane < 64, roll(parts[1], 64), roll(parts[2], B96))
    return jnp.where(lane < 32, roll(parts[0], 32), tail)


def join_quarters(quarters, keep):
    return [jnp.where(keep, quarters[i], roll(quarters[3], B96 - 32 * i)) for i in range(3)]


def kernel(rate_ref, wd_ref, beta_ref, w_in, w_out, g_in, g_out, m_in, m_out, r_in, c_in, r_out, c_out,
           wn_in, wn_out, mn_in, mn_out, rn_in, cn_in, rn_out, cn_out,
           gbuf, pbuf, gsend, pack, via, rin, fin, mall, mraw_in, mraw_out, msend, mt, mpack, tall,
           rvacc, lvacc, lraw, craw, oraw, pads, lvold, rvold, lvnew, rvnew, box_rv, box_sx, box_lt, box_st,
           gl_sem, gp_sem, gs_sem, gr_sem, ml_sem, ms_sem, mr_sem, s_sem, via_sem, rin_sem, ags_sem, agr_sem,
           shs_sem, shr_sem, sts_sem, str_sem, vs_sem, vr_sem, ol_sem, os_sem, wl_sem, ready):
    tp, dp = lax.axis_index('tp'), lax.axis_index('dp')
    z, y, x, c = tp // RING, tp % RING, dp // 2, dp % 2
    other = 1 - c
    base, pbase = c * LC, other * LC

    def at_x(xx):
        return {'dp': (xx % RING) * 2 + c}

    def at_y(yy):
        return {'tp': z * RING + yy % RING}

    def at_z(zz):
        return {'tp': (zz % RING) * RING + y}

    partner = {'dp': x * 2 + other}

    def local(src, dst, sem):
        return pltpu.make_async_copy(src, dst, sem)

    def remote(src, dst, send_sem, recv_sem, device):
        return pltpu.make_async_remote_copy(src_ref=src, dst_ref=dst, send_sem=send_sem, recv_sem=recv_sem,
                                            device_id=device, device_id_type=MESH)

    barrier = pltpu.get_barrier_semaphore()
    peers = [partner]
    for k in range(1, RING):
        peers += [at_x(x + k), at_y(y + k), at_z(z + k)]
    for peer in peers:
        pl.semaphore_signal(barrier, inc=1, device_id=peer, device_id_type=MESH)

    def own(l, i):
        src, dst = ((g_in, first(KI)), (g_out, pl.ds(KI, NO)))[i]
        return local(src.at[base + l], gbuf.at[l, dst], gl_sem.at[NG + l] if isinstance(l, int) else gl_sem.at[l // LG])

    def others(l, i):
        src, dst = ((g_in, first(KI)), (g_out, pl.ds(KI, NO)))[i]
        return local(src.at[pbase + l], gsend.at[l, dst], gp_sem.at[l])

    def swap_first(l):
        return remote(gsend.at[l], pbuf.at[l], gs_sem.at[0], gr_sem.at[NG + l], partner)

    def swap(l, i):
        src, dst = ((g_in, first(KI)), (g_out, pl.ds(KI, NO)))[i]
        return remote(src.at[pbase + l], pbuf.at[l, dst], gs_sem.at[0], gr_sem.at[l // LG], partner)

    my_rows, its_rows = pl.ds(base, LC), pl.ds(pbase, LC)
    loads = [local(m_in, mraw_in, ml_sem.at[0]), local(m_out, mraw_out, ml_sem.at[1]),
             local(r_in.at[my_rows], lraw.at[0, c], ol_sem.at[0]), local(c_out.at[my_rows], lraw.at[1, c], ol_sem.at[1]),
             local(c_in.at[my_rows], craw, ol_sem.at[2]), local(r_out.at[my_rows], oraw, ol_sem.at[3])]
    w_loads = [local(w_in, wn_in, wl_sem.at[0]), local(w_out, wn_out, wl_sem.at[1])]

    def lane_swap(m, core):
        return remote((r_in, c_out)[m].at[its_rows], lraw.at[m, core], os_sem.at[0], os_sem.at[1], partner)

    def start_loads(l, carry):
        own(l, 0).start()
        own(l, 1).start()
        return carry

    for l in range(LG):
        for i in range(2):
            others(l, i).start()
            own(l, i).start()
    lax.fori_loop(LG, LC, start_loads, 0)
    for copy in loads:
        copy.start()
    pl.semaphore_wait(barrier, len(peers))
    for k in range(1, RING):
        pl.semaphore_signal(ready, inc=1, device_id=at_y(y + k), device_id_type=MESH)
    for l in range(LG):
        local(gsend.at[l], gsend.at[l], gp_sem.at[l]).wait()
        swap_first(l).start()
    lane_swap(0, c).start()
    lane_swap(1, c).start()
    rvacc[...] = jnp.zeros_like(rvacc)
    lvacc[...] = jnp.zeros_like(lvacc)

    lane, lane8, row8 = lane_of((Q, LN)), lane_of((8, LN)), row_of((8, LN))
    m96, k96 = lane < B96, lane8 < B96
    head = row_of((Q, LN)) < HEAD
    only_x = (row8 >= 2 * LG) & (row8 < 3 * LG)

    def way(l):
        return 1 - 2 * (l % 2)

    def ahead(l):
        return (x + way(l) + RING) % RING

    def behind(l):
        return (x - way(l) + RING) % RING

    across = (x + 2) % RING

    def step1(l):
        return remote(pack.at[l, across], via.at[l], s_sem.at[0], via_sem.at[l], at_x(ahead(l)))

    def step2(l):
        return remote(pack.at[l, ahead(l)], rin.at[l, 0], s_sem.at[0], rin_sem.at[l // LG], at_x(ahead(l)))

    def step3(l):
        return remote(pack.at[l, behind(l)], rin.at[l, 1], s_sem.at[0], rin_sem.at[l // LG], at_x(behind(l)))

    def m_rows(core):
        return pl.ds(pl.multiple_of(core * B48, 16), B48)

    def moment_swap(l, core):
        return remote(msend.at[l], mt.at[l, m_rows(core)], ms_sem.at[0], mr_sem.at[l // LG], partner)

    def stage_a(l):
        def tile(t, q):
            return gbuf[l, block(q), tile_cols(t)] + pbuf[l, block(q), tile_cols(t)]

        def chunk(d, q):
            if d == 0:
                return tile(0, q)
            if d == 1:
                return roll(jnp.where(m96, tile(1, q), tile(0, q)), 32)
            if d == 2:
                return roll(jnp.where(lane < 64, tile(2, q), tile(1, q)), 64)
            return roll(tile(2, q), B96)

        def put(d):
            for i, val in enumerate(join_quarters([chunk(d, q) for q in range(4)], m96)):
                pack[l, d, block(i), :] = val

        if not isinstance(l, int):
            for d in range(RING):
                put(d)
            return

        for d in range(RING):
            pl.when(across == d)(lambda: put(d))
        step1(l).start()
        for d in range(RING):
            pl.when(across != d)(lambda: put(d))

    def stage_n(l):
        msend[l, :, first(KI)] = mraw_in[pbase + l].astype(F32)
        msend[l, :, pl.ds(MID, NO)] = mraw_out[pbase + l].astype(F32)
        moment_swap(l, c).start()
        mt[l, m_rows(c), first(KI)] = mraw_in[base + l].astype(F32)
        mt[l, m_rows(c), pl.ds(MID, NO)] = mraw_out[base + l].astype(F32)

    def stage_b(l):
        step1(l).wait_recv()
        to = ahead(l)
        pack[l, to] = pack[l, to] + via[l]
        step2(l).start()

    def stage_c(l):
        sq = []
        for i in range(3):
            grad = pack[l, x, block(i), :] + rin[l, 0, block(i), :] + rin[l, 1, block(i), :]
            fin[l, block(i), :] = grad
            sq.append(grad * grad + 1e-30)
        g, lg = l // LG, l % LG
        sums = [rowsum(pick(m96, val)) for val in sq]
        sums.append(rowsum(jnp.where(m96, 0.0, sq[0] + sq[1] + sq[2])))
        acc = rvacc[g, first(Q), :]
        for q in range(4):
            acc = jnp.where(lane == LG * q + lg, sums[q], acc)
        rvacc[g, first(Q), :] = acc
        top = colsum(pick(head, sq[2]))
        low = colsum(jnp.where(head, 0.0, sq[2]))
        cols = [colsum(sq[0]), colsum(sq[1])]
        wide = [jnp.broadcast_to(val, (8, LN)) for val in (cols[0], cols[1], top + low)]
        in_sum = pick(k96, cols[0] + cols[1] + top)
        out_sum = pick(k96, low + last_quarter(wide))
        both = jnp.where(row8 == lg, in_sum, lvacc[g])
        lvacc[g] = jnp.where(row8 == LG + lg, out_sum, both)

    def stage_m(l):
        val = mt[l].T
        third = jnp.concatenate([val[2 * Q:KI], val[MID:MID + B48]], axis=0)
        quarters = [val[:Q], val[Q:2 * Q], third, val[MID + B48:MID + NO]]
        for i, part in enumerate(join_quarters(quarters, m96)):
            mpack[l, block(i), :] = part

    boxes = {RV: (box_rv, x, RING), SX: (box_sx, x, RING), LT: (box_lt, tp, TP), ST: (box_st, tp, TP)}

    def post(kind, g, val):
        box, me, num = boxes[kind]
        box[g, me] = val

        def send(k, carry):
            device = at_x(me + k) if num == RING else {'tp': (me + k) % TP}
            remote(box.at[g, me], box.at[g, me], sts_sem.at[int(kind == SX)], str_sem.at[g, kind], device).start()
            return carry

        lax.fori_loop(1, num, send, 0)

    def collect(kind, g):
        box, me, num = boxes[kind]
        rest = box.at[g, first(num - 1)]
        remote(rest, rest, sts_sem.at[int(kind == SX)], str_sem.at[g, kind], partner).wait_recv()
        val = box[g, 0]
        for k in range(1, num):
            val = val + box[g, k]
        return val

    def sums_send(g):
        post(LT, g, lvacc[g])
        post(RV, g, rvacc[g].T[:8])

    beta = beta_ref[0]

    def old_vectors():
        for copy in loads[2:]:
            copy.wait()
        remote(lraw.at[0], lraw.at[0], os_sem.at[0], os_sem.at[1], partner).wait_recv()
        for m in range(2):
            for core in range(2):
                pads[m, core, :, first(B48)] = lraw[m, core]
        pads[2, 0, :, first(KI - LN)] = craw[:, pl.ds(LN, KI - LN)]
        pads[2, 1, :, first(NO)] = oraw[...]
        low, high, rest = craw[:, first(LN)], pads[2, 0], pads[2, 1]
        lanes = [jnp.where(lane8 < B48, pads[m, 0], roll(pads[m, 1], B48)) for m in range(2)]
        rows = [low, jnp.where(lane8 < LN - Q, roll(low, -Q), roll(high, -Q)),
                jnp.where(lane8 < HEAD, roll(high, -16), roll(rest, HEAD)), roll(rest, -B48)]
        for g in range(NG):
            part = slice(LG * g, LG * g + LG)
            lvold[g] = jnp.concatenate([val[part] for val in lanes + lanes], axis=0)
            rvold[g] = jnp.concatenate([val[part] for val in rows], axis=0)

    def vec_swap(g, half, i):
        ref = (lvnew, rvnew)[i]
        return remote(ref.at[half, g], ref.at[half, g], vs_sem.at[0], vr_sem.at[i], partner)

    def moments(g):
        lv_mean = collect(LT, g) / jnp.where(row8 < LG, KIN, NOUT)
        lv_new = beta * lvold[g] + (1.0 - beta) * lv_mean
        lvnew[c, g] = lv_new
        rv_new = beta * rvold[g] + (1.0 - beta) * (collect(RV, g) / NI)
        rvnew[c, g] = rv_new
        for i in range(2):
            vec_swap(g, c, i).start()
        scale_l = 1.0 / jnp.sqrt(jnp.where(k96, lv_new, 1.0))
        scale_r = 1.0 / jnp.sqrt(jnp.where(lane8 < Q, rv_new, 1.0))
        wide = jnp.concatenate([scale_r, jnp.ones((LN - 8, LN), F32)], axis=0).T
        tots = jnp.zeros((8, LN), F32)
        lane1 = lane_of((1, LN))
        for lg in range(LG):
            l = g * LG + lg
            rs = [jnp.broadcast_to(wide[:Q, LG * q + lg:LG * q + lg + 1], (Q, LN)) for q in range(4)]
            sc_in = scale_l[lg:lg + 1, :]
            sc_out = jnp.broadcast_to(scale_l[LG + lg:LG + lg + 1, :], (8, LN))
            parts = []
            for i in range(3):
                body = jnp.where(head, sc_in, sc_out[:1]) if i == 2 else sc_in
                lanes = jnp.where(m96, body, roll(sc_out, B96 - 32 * i)[:1])
                u0 = fin[l, block(i), :] * jnp.where(m96, rs[i], rs[3]) * lanes
                fin[l, block(i), :] = u0
                parts.append(u0 * u0)
            inner = pick(m96, parts[0] + parts[1] + pick(head, parts[2]))
            outer = jnp.where(m96, jnp.where(head, 0.0, parts[2]), parts[0] + parts[1] + parts[2])
            v_in = pick(lane1 < B96, lv_new[lg:lg + 1, :])
            v_out = pick((lane1 >= HEAD) & (lane1 < Q), rv_new[2 * LG + lg:2 * LG + lg + 1, :]) + pick(lane1 < Q, rv_new[3 * LG + lg:3 * LG + lg + 1, :])
            for k, val in enumerate((colsum(inner), colsum(outer), v_in, v_out)):
                tots = jnp.where(row8 == LG * k + lg, val, tots)
        post(ST, g, tots)

    def totals(g):
        val = rowsum(jnp.where(only_x, box_st[g, tp], collect(ST, g)))
        post(SX, g, colsum(pick(row8 == lane8, val)))

    def factors(g):
        val = jnp.where(lane_of((1, LN)) >= 3 * LG, box_sx[g, x], collect(SX, g))
        tot = rowsum(pick(row8 == lane8, val))
        isin = row_of((2 * LG, 1)) < LG
        mean_r = tot[2 * LG:] / jnp.where(isin, NI, NOUT)
        rms = jnp.sqrt(mean_r * tot[:2 * LG] / jnp.where(isin, NI * KIN, NOUT * KO))
        return jnp.sqrt(mean_r) / jnp.maximum(1.0, rms)

    def update(l, lg, fac):
        f_in, f_out = fac[lg:lg + 1, :], fac[LG + lg:LG + lg + 1, :]
        for i in range(3):
            upd = fin[l, block(i), :] * jnp.where((m96 & head) if i == 2 else m96, f_in, f_out)
            new = 0.9 * mpack[l, block(i), :] + 0.1 * upd
            mall[base + l, x, block(i), :] = new.astype(BF16).astype(F32)

    def arrived(l, k):
        return l if k == 0 else LC + NG if k == 1 and l >= LC - LG else LC + l // LG

    def gather(l, k):
        slot = x if k < 2 else behind(l)
        ref = mall.at[base + l, slot]
        return remote(ref, ref, ags_sem.at[0], agr_sem.at[arrived(l, k)], at_x(behind(l) if k == 1 else ahead(l)))

    def share(l, k, start):
        ref = mall.at[start + l, (behind(l), ahead(l), across, x)[k]]
        return remote(ref, ref, shs_sem.at[0], shr_sem.at[NG if k == 3 and l >= LC - LG else l // LG], partner)

    def send_pair(l):
        gather(l, 0).start()
        gather(l + 1, 0).start()

    def send_back(l):
        gather(l, 1).start()
        gather(l + 1, 1).start()
        share(l, 3, base).start()
        share(l + 1, 3, base).start()

    def forward_pair(l):
        for k in (l, l + 1):
            gather(k, 0).wait_recv()
            gather(k, 2).start()
            share(k, 0, base).start()

    def half(ref, h):
        return ref.at[(first(HALF), pl.ds(HALF, CH - HALF))[h]]

    def gather_half(l, h, slot):
        ref = half(mall.at[base + l, slot], h)
        return remote(ref, ref, ags_sem.at[0], agr_sem.at[l if h == 0 else LC + NG + 1 + l], at_x(ahead(l)))

    def send_first():
        for h in range(2):
            for l in range(LG):
                gather_half(l, h, x).start()

    def forward_first():
        for h in range(2):
            for l in range(LG):
                gather_half(l, h, behind(l)).wait_recv()
                ref = half(mall.at[base + l, behind(l)], h)
                remote(ref, ref, ags_sem.at[0], agr_sem.at[arrived(l, 2)], at_x(ahead(l))).start()
        share(0, 0, base).start()
        share(1, 0, base).start()

    def settle_pair(l):
        four = mall.at[base + l]
        remote(four, four, ags_sem.at[0], agr_sem.at[LC + l // LG], partner).wait_recv()
        for k in (l, l + 1):
            for i in (1, 2):
                share(k, i, base).start()

    def settle_last(k):
        l = LC - LG
        two = mall.at[base + l, first(LG)]
        remote(two, two, ags_sem.at[0], agr_sem.at[arrived(l, k)], partner).wait_recv()
        share(l, k, base).start()
        share(l + 1, k, base).start()

    rate = rate_ref[0]
    decay = rate * wd_ref[0]

    def unpack(at):
        for q in range(4):
            if q < 3:
                chunk = [mall[at, d, block(q), :] for d in range(RING)]
            else:
                chunk = [last_quarter([mall[at, d, block(i), :] for i in range(3)]) for d in range(RING)]
            r1, r2, r3 = roll(chunk[1], B96), roll(chunk[2], 64), roll(chunk[3], 32)
            mom = (jnp.where(m96, chunk[0], r1), jnp.where(lane < 64, r1, r2), jnp.where(lane < 32, r2, r3))
            spots = (((wn_in, 0, 0, Q),), ((wn_in, Q, 0, Q),), ((wn_in, 2 * Q, 0, HEAD), (wn_out, 0, HEAD, B48)), ((wn_out, B48, 0, Q),))[q]
            for t in range(3):
                for ref, dst, src, num in spots:
                    rows = pl.ds(dst, num)
                    w = ref[at, rows, tile_cols(t)]
                    ref[at, rows, tile_cols(t)] = w - rate * mom[t][src:src + num] - decay * w

    def turn_moment(at):
        parts = [mall[at, x, block(i), :] for i in range(3)]
        parts.append(last_quarter(parts))
        spots = ((0, 0, Q),), ((Q, 0, Q),), ((2 * Q, 0, HEAD), (MID, HEAD, B48)), ((MID + B48, 0, Q),)
        for val, places in zip(parts, spots):
            val = jnp.where(c == 0, val, roll(val, -B48))
            for dst, src, num in places:
                tall[pl.ds(dst, num), :] = val[src:src + num]
        turned = [tall[tile_cols(t), :].T[:B48] for t in range(3)]
        mn_in[at, :, first(LN)] = turned[0].astype(BF16)
        mn_in[at, :, pl.ds(LN, KI - LN)] = turned[1][:, :KI - LN].astype(BF16)
        mn_out[at] = turned[2][:, :NO].astype(BF16)

    def each(step, l, start):
        lax.fori_loop(start + l, start + l + LG, lambda at, carry: (step(at), carry)[1], 0)

    def unpack_pair(l, start):
        each(unpack, l, start)
        if l < LC - LG:
            each(turn_moment, l, start)

    def turn_last():
        l = LC - LG
        each(turn_moment, l, base)
        two = mall.at[base, first(LG)]
        remote(two, two, shs_sem.at[0], shr_sem.at[NG], partner).wait_recv()
        each(turn_moment, l, pbase)

    def take_pair(l):
        two = mall.at[pl.ds(pbase + l, LG)] if l < LC - LG else mall.at[pl.ds(pbase + l, LG), first(3)]
        remote(two, two, shs_sem.at[0], shr_sem.at[l // LG], partner).wait_recv()
        unpack_pair(l, pbase)

    def new_vectors():
        lane4 = lane_of((LG, LN))
        for half in range(2):
            for g in range(NG):
                rows = pl.ds(LC * half + LG * g, LG)
                both, val = lvnew[half, g], rvnew[half, g]
                both = jnp.where(c == 0, both, roll(both, -B48))
                rn_in[rows, :] = both[:LG, :B48]
                cn_out[rows, :] = both[LG:2 * LG, :B48]
                two = roll(val, Q)[LG:2 * LG]
                cn_in[rows, first(LN)] = jnp.where(lane4 < Q, val[:LG], two)
                cn_in[rows, pl.ds(LN, KI - LN)] = jnp.where(lane4 < 16, two, roll(val, 16)[2 * LG:3 * LG])[:, :KI - LN]
                rn_out[rows, :] = jnp.where(lane4 < B48, roll(val, -HEAD)[2 * LG:3 * LG], roll(val, B48)[3 * LG:])[:, :NO]

    def both(step, g):
        lax.fori_loop(LG * g, LG * g + LG, lambda l, carry: (step(l), carry)[1], 0)

    def swap_start(l):
        swap(l, 0).start()
        swap(l, 1).start()

    def pack_first():
        for l in range(LG):
            local(gbuf.at[l], gbuf.at[l], gl_sem.at[NG + l]).wait()
            swap_first(l).wait_recv()
            stage_a(l)
            if l == 0:
                both(swap_start, 1)
        both(lambda l: step3(l).start(), 0)

    def pack_pair(g):
        two = pl.ds(LG * g, LG)
        local(gbuf.at[two], gbuf.at[two], gl_sem.at[g]).wait()
        remote(pbuf.at[two], pbuf.at[two], gs_sem.at[0], gr_sem.at[g], partner).wait_recv()
        if g + 1 < NG:
            both(swap_start, g + 1)
        both(stage_a, g)
        both(lambda l: step1(l).start(), g)

    def direct_pair(g):
        both(lambda l: step3(l).start(), g)

    def cast_pair(g):
        if g == 0:
            loads[0].wait()
            loads[1].wait()
        both(stage_n, g)

    def relay_pair(g):
        both(stage_b, g)

    def sum_pair(g):
        two = rin.at[pl.ds(LG * g, LG)]
        remote(two, two, s_sem.at[0], rin_sem.at[g], partner).wait_recv()
        both(stage_c, g)
        sums_send(g)

    def moment_pair(g):
        two = msend.at[pl.ds(LG * g, LG)]
        remote(two, two, ms_sem.at[0], mr_sem.at[g], partner).wait_recv()
        both(stage_m, g)

    def update_pair(g):
        fac = factors(g)
        for lg in range(LG):
            update(LG * g + lg, lg, fac)

    pack_first()
    cast_pair(0)
    pack_pair(1)
    w_loads[0].start()
    w_loads[1].start()
    old_vectors()
    pl.semaphore_wait(ready, RING - 1)
    relay_pair(0)
    direct_pair(1)
    cast_pair(1)
    pack_pair(2)
    sum_pair(0)
    relay_pair(1)
    direct_pair(2)
    cast_pair(2)
    moment_pair(0)
    pack_pair(3)
    moments(0)
    sum_pair(1)
    relay_pair(2)
    cast_pair(3)
    moment_pair(1)
    totals(0)
    direct_pair(3)
    relay_pair(3)
    moments(1)
    sum_pair(2)
    moment_pair(2)
    update_pair(0)
    send_first()
    totals(1)
    send_back(0)
    sum_pair(3)
    moment_pair(3)
    moments(2)
    forward_first()
    update_pair(1)
    send_pair(2)
    moments(3)
    totals(2)
    send_back(2)
    forward_pair(2)
    settle_pair(0)
    totals(3)
    update_pair(2)
    send_pair(4)
    send_back(4)
    w_loads[0].wait()
    w_loads[1].wait()
    unpack_pair(0, base)
    take_pair(0)
    settle_pair(2)
    update_pair(3)
    send_pair(6)
    forward_pair(4)
    send_back(6)
    unpack_pair(2, base)
    take_pair(2)
    for i, ref in enumerate((lvnew, rvnew)):
        remote(ref.at[other], ref.at[other], vs_sem.at[0], vr_sem.at[i], partner).wait_recv()
    new_vectors()
    turn_last()
    forward_pair(6)
    settle_pair(4)
    unpack_pair(4, base)
    settle_last(1)
    take_pair(4)
    settle_last(2)
    unpack_pair(6, base)
    take_pair(6)
    for ref, sem in ((pbuf, gs_sem), (msend, ms_sem), (mall.at[first(6)], s_sem), (mall.at[first(6)], ags_sem), (mall.at[first(8)], shs_sem),
                     (lraw.at[0], os_sem), (mt.at[first(4), first(88)], sts_sem), (lvnew, vs_sem)):
        remote(ref, ref, sem.at[0], os_sem.at[1], partner).wait_send()
    last = box_sx.at[:, first(RING - 1)]
    remote(last, last, sts_sem.at[1], os_sem.at[1], partner).wait_send()


def update_call(scalars, arrays):
    hbm, smem = pl.BlockSpec(memory_space=pltpu.HBM), pl.BlockSpec(memory_space=pltpu.SMEM)
    dma, vmem = pltpu.SemaphoreType.DMA, pltpu.VMEM

    def lanes(*lead):
        return vmem(lead + (LN,), F32)

    scratch = [
        vmem((LC, KI + NO, D), F32), vmem((LC, KI + NO, D), F32), vmem((LG, KI + NO, D), F32), lanes(LC, RING, CH), lanes(LC, CH), lanes(LC, 2, CH), lanes(LC, CH),
        lanes(L, RING, CH), vmem((L, B48, KI), BF16), vmem((L, B48, NO), BF16), vmem((LC, B48, D), F32), vmem((LC, LN, D), F32),
        lanes(LC, CH), lanes(D), lanes(NG, LN), lanes(NG, 8),
        vmem((2, 2, LC, B48), F32), vmem((LC, KI), F32), vmem((LC, NO), F32), lanes(3, 2, LC),
        lanes(NG, 8), lanes(NG, 8), lanes(2, NG, 8), lanes(2, NG, 8),
        lanes(NG, RING, 8), lanes(NG, RING, 1), lanes(NG, TP, 8), lanes(NG, TP, 8),
        dma((NG + LG,)), dma((LG,)), dma((1,)), dma((NG + LG,)), dma((2,)), dma((1,)), dma((NG,)), dma((1,)), dma((LC,)), dma((NG,)),
        dma((1,)), dma((LC + NG + 1 + LG,)), dma((1,)), dma((NG + 1,)), dma((2,)), dma((NG, len(KINDS))), dma((1,)), dma((2,)), dma((4,)),
        dma((2,)), dma((2,)), pltpu.SemaphoreType.REGULAR,
    ]
    outs = [((L, KI, D), F32), ((L, NO, D), F32), ((L, B48, KI), BF16), ((L, B48, NO), BF16),
            ((L, B48), F32), ((L, KI), F32), ((L, NO), F32), ((L, B48), F32)]
    return pl.pallas_call(
        kernel,
        out_shape=[vmem(*out) for out in outs],
        in_specs=[smem] * len(scalars) + [hbm] * len(arrays),
        out_specs=[pl.BlockSpec(memory_space=vmem)] * len(outs),
        scratch_shapes=scratch,
        compiler_params=pltpu.CompilerParams(collective_id=0, has_side_effects=True, vmem_limit_bytes=36 * 2**20),
        name='adafactor',
    )(*[val.reshape(1) for val in scalars], *[pltpu.with_memory_space_constraint(val, pltpu.HBM) for val in arrays])


def store_kernel(*refs):
    num = len(refs) // 2
    copies = [pltpu.make_async_copy(src, dst, refs[-1].at[i]) for i, (src, dst) in enumerate(zip(refs[:num], refs[num:-1]))]
    for copy in copies:
        copy.start()
    for copy in copies:
        copy.wait()


def store_call(vals):
    anyspace = pl.BlockSpec(memory_space=pl.ANY)
    return pl.pallas_call(
        store_kernel,
        out_shape=[jax.ShapeDtypeStruct(val.shape, val.dtype) for val in vals],
        in_specs=[anyspace] * len(vals),
        out_specs=[anyspace] * len(vals),
        scratch_shapes=[pltpu.SemaphoreType.DMA((len(vals),))],
        compiler_params=pltpu.CompilerParams(vmem_limit_bytes=2**20),
        name='store',
    )(*[pltpu.with_memory_space_constraint(val, pltpu.VMEM) for val in vals])


def solution(mesh):
    def turn(val):
        return val.swapaxes(1, 2)

    def body(w_in, w_out, g_in, g_out, m_in, m_out, r_in, c_in, r_out, c_out, learn_rate, weight_decay, beta_two):
        out = store_call(update_call((learn_rate, weight_decay, beta_two),
                          (turn(w_in), w_out, turn(g_in[0]), g_out[0], m_in, turn(m_out), r_in, c_in, r_out, c_out)))
        return (turn(out[0]), out[1], out[2], turn(out[3])) + tuple(out[4:])

    cols, rows, own = P(None, None, 'tp'), P(None, 'tp', None), P(None, 'dp')
    outs = (cols, rows, P(None, 'dp', 'tp'), P(None, 'tp', 'dp'), own, P(None, 'tp'), P(None, 'tp'), own)
    in_specs = (cols, rows, P('dp', *cols), P('dp', *rows)) + outs[2:] + (P(), P(), P())
    return jax.shard_map(body, mesh=mesh, in_specs=in_specs, out_specs=outs, check_vma=False)
```

```python
import jax
import jax.numpy as jnp
from jax import lax
from jax.experimental import pallas as pl
from jax.experimental.pallas import tpu as pltpu
from jax.sharding import PartitionSpec as P

F32, BF16 = jnp.float32, jnp.bfloat16
MESH = pl.DeviceIdType.MESH
RING = 4
L, D = 16, 384
KI, NO = 168, 120
LC, LG, NG = 8, 2, 4
Q, LN, B48, B96 = 72, 128, 48, 96
CH, HEAD, MID, HALF = 3 * Q, KI - 2 * Q, 256, 104
NI, KIN, NOUT, KO = 384.0, 2688.0, 1920.0, 384.0
KINDS = RV, LT, SX, ST = range(4)
TP = RING * RING


def roll(val, shift):
    return pltpu.roll(val, shift % LN, 1)


def lane_of(shape):
    return lax.broadcasted_iota(jnp.int32, shape, 1)


def row_of(shape):
    return lax.broadcasted_iota(jnp.int32, shape, 0)


def colsum(val):
    return jnp.sum(val, axis=0, keepdims=True)


def rowsum(val):
    return jnp.sum(val, axis=1, keepdims=True)


def pick(cond, val):
    return jnp.where(cond, val, 0.0)


def first(num):
    return pl.ds(0, num)


def block(i):
    return pl.ds(Q * i, Q)


def tile_cols(t):
    return pl.ds(LN * t, LN)


def last_quarter(parts):
    lane = lane_of(parts[0].shape)
    tail = jnp.where(lane < 64, roll(parts[1], 64), roll(parts[2], B96))
    return jnp.where(lane < 32, roll(parts[0], 32), tail)


def join_quarters(quarters, keep):
    return [jnp.where(keep, quarters[i], roll(quarters[3], B96 - 32 * i)) for i in range(3)]


def kernel(rate_ref, wd_ref, beta_ref, w_in, w_out, g_in, g_out, m_in, m_out, r_in, c_in, r_out, c_out,
           wn_in, wn_out, mn_in, mn_out, rn_in, cn_in, rn_out, cn_out,
           gbuf, pbuf, gsend, pack, via, rin, fin, mall, mraw_in, mraw_out, msend, mt, mpack, tall,
           rvacc, lvacc, lraw, craw, oraw, pads, lvold, rvold, lvnew, rvnew, box_rv, box_sx, box_lt, box_st,
           gl_sem, gp_sem, gs_sem, gr_sem, ml_sem, ms_sem, mr_sem, s_sem, via_sem, rin_sem, ags_sem, agr_sem,
           shs_sem, shr_sem, sts_sem, str_sem, vs_sem, ol_sem, os_sem, wl_sem, ready):
    tp, dp = lax.axis_index('tp'), lax.axis_index('dp')
    z, y, x, c = tp // RING, tp % RING, dp // 2, dp % 2
    other = 1 - c
    base, pbase = c * LC, other * LC

    def at_x(xx):
        return {'dp': (xx % RING) * 2 + c}

    def at_y(yy):
        return {'tp': z * RING + yy % RING}

    def at_z(zz):
        return {'tp': (zz % RING) * RING + y}

    partner = {'dp': x * 2 + other}

    def local(src, dst, sem):
        return pltpu.make_async_copy(src, dst, sem)

    def remote(src, dst, send_sem, recv_sem, device):
        return pltpu.make_async_remote_copy(src_ref=src, dst_ref=dst, send_sem=send_sem, recv_sem=recv_sem,
                                            device_id=device, device_id_type=MESH)

    barrier = pltpu.get_barrier_semaphore()
    peers = [partner]
    for k in range(1, RING):
        peers += [at_x(x + k), at_y(y + k), at_z(z + k)]
    for peer in peers:
        pl.semaphore_signal(barrier, inc=1, device_id=peer, device_id_type=MESH)

    def own(l, i):
        src, dst = ((g_in, first(KI)), (g_out, pl.ds(KI, NO)))[i]
        return local(src.at[base + l], gbuf.at[l, dst], gl_sem.at[l if isinstance(l, int) else LG])

    def others(l, i):
        src, dst = ((g_in, first(KI)), (g_out, pl.ds(KI, NO)))[i]
        return local(src.at[pbase + l], gsend.at[l, dst], gp_sem.at[l])

    def swap_first(l):
        return remote(gsend.at[l], pbuf.at[l], gs_sem.at[0], gr_sem.at[NG + l], partner)

    def swap(l, i):
        src, dst = ((g_in, first(KI)), (g_out, pl.ds(KI, NO)))[i]
        return remote(src.at[pbase + l], pbuf.at[l, dst], gs_sem.at[0], gr_sem.at[l // LG], partner)

    my_rows, its_rows = pl.ds(base, LC), pl.ds(pbase, LC)
    loads = [local(m_in, mraw_in, ml_sem.at[0]), local(m_out, mraw_out, ml_sem.at[1]),
             local(r_in.at[my_rows], lraw.at[0, c], ol_sem.at[0]), local(c_out.at[my_rows], lraw.at[1, c], ol_sem.at[1]),
             local(c_in.at[my_rows], craw, ol_sem.at[2]), local(r_out.at[my_rows], oraw, ol_sem.at[3])]
    w_loads = [local(w_in, wn_in, wl_sem.at[0]), local(w_out, wn_out, wl_sem.at[1])]

    def lane_swap(m, core):
        return remote((r_in, c_out)[m].at[its_rows], lraw.at[m, core], os_sem.at[0], os_sem.at[1], partner)

    def start_loads(l, carry):
        own(l, 0).start()
        own(l, 1).start()
        return carry

    for l in range(LG):
        for i in range(2):
            others(l, i).start()
            own(l, i).start()
    lax.fori_loop(LG, LC, start_loads, 0)
    for copy in loads:
        copy.start()
    pl.semaphore_wait(barrier, len(peers))
    for k in range(1, RING):
        pl.semaphore_signal(ready, inc=1, device_id=at_y(y + k), device_id_type=MESH)
    for l in range(LG):
        local(gsend.at[l], gsend.at[l], gp_sem.at[l]).wait()
        swap_first(l).start()
    lane_swap(0, c).start()
    lane_swap(1, c).start()
    rvacc[...] = jnp.zeros_like(rvacc)
    lvacc[...] = jnp.zeros_like(lvacc)

    lane, lane8, row8 = lane_of((Q, LN)), lane_of((8, LN)), row_of((8, LN))
    m96, k96 = lane < B96, lane8 < B96
    head = row_of((Q, LN)) < HEAD
    only_x = (row8 >= 2 * LG) & (row8 < 3 * LG)

    def way(l):
        return 1 - 2 * (l % 2)

    def ahead(l):
        return (x + way(l) + RING) % RING

    def behind(l):
        return (x - way(l) + RING) % RING

    across = (x + 2) % RING

    def step1(l):
        return remote(pack.at[l, across], via.at[l], s_sem.at[0], via_sem.at[l // LG], at_x(ahead(l)))

    def step2(l):
        return remote(pack.at[l, ahead(l)], rin.at[l, 0], s_sem.at[0], rin_sem.at[l // LG], at_x(ahead(l)))

    def step3(l):
        return remote(pack.at[l, behind(l)], rin.at[l, 1], s_sem.at[0], rin_sem.at[l // LG], at_x(behind(l)))

    def m_rows(core):
        return pl.ds(pl.multiple_of(core * B48, 16), B48)

    def moment_swap(l, core):
        return remote(msend.at[l], mt.at[l, m_rows(core)], ms_sem.at[0], mr_sem.at[0], partner)

    def stage_a(l):
        def tile(t, q):
            return gbuf[l, block(q), tile_cols(t)] + pbuf[l, block(q), tile_cols(t)]

        def chunk(d, q):
            if d == 0:
                return tile(0, q)
            if d == 1:
                return roll(jnp.where(m96, tile(1, q), tile(0, q)), 32)
            if d == 2:
                return roll(jnp.where(lane < 64, tile(2, q), tile(1, q)), 64)
            return roll(tile(2, q), B96)

        def put(d):
            for i, val in enumerate(join_quarters([chunk(d, q) for q in range(4)], m96)):
                pack[l, d, block(i), :] = val

        if not isinstance(l, int):
            for d in range(RING):
                put(d)
            return

        for d in range(RING):
            pl.when(across == d)(lambda: put(d))
        step1(l).start()
        for d in range(RING):
            pl.when(across != d)(lambda: put(d))

    def stage_n(l):
        msend[l, :, first(KI)] = mraw_in[pbase + l].astype(F32)
        msend[l, :, pl.ds(MID, NO)] = mraw_out[pbase + l].astype(F32)
        moment_swap(l, c).start()
        mt[l, m_rows(c), first(KI)] = mraw_in[base + l].astype(F32)
        mt[l, m_rows(c), pl.ds(MID, NO)] = mraw_out[base + l].astype(F32)

    def stage_b(l):
        to = ahead(l)
        pack[l, to] = pack[l, to] + via[l]
        step2(l).start()

    def stage_c(l):
        sq = []
        for i in range(3):
            grad = pack[l, x, block(i), :] + rin[l, 0, block(i), :] + rin[l, 1, block(i), :]
            fin[l, block(i), :] = grad
            sq.append(grad * grad + 1e-30)
        g, lg = l // LG, l % LG
        sums = [rowsum(pick(m96, val)) for val in sq]
        sums.append(rowsum(jnp.where(m96, 0.0, sq[0] + sq[1] + sq[2])))
        acc = rvacc[g, first(Q), :]
        for q in range(4):
            acc = jnp.where(lane == LG * q + lg, sums[q], acc)
        rvacc[g, first(Q), :] = acc
        top = colsum(pick(head, sq[2]))
        low = colsum(jnp.where(head, 0.0, sq[2]))
        cols = [colsum(sq[0]), colsum(sq[1])]
        wide = [jnp.broadcast_to(val, (8, LN)) for val in (cols[0], cols[1], top + low)]
        in_sum = pick(k96, cols[0] + cols[1] + top)
        out_sum = pick(k96, low + last_quarter(wide))
        both = jnp.where(row8 == lg, in_sum, lvacc[g])
        lvacc[g] = jnp.where(row8 == LG + lg, out_sum, both)

    def stage_m(l):
        val = mt[l].T
        third = jnp.concatenate([val[2 * Q:KI], val[MID:MID + B48]], axis=0)
        quarters = [val[:Q], val[Q:2 * Q], third, val[MID + B48:MID + NO]]
        for i, part in enumerate(join_quarters(quarters, m96)):
            mpack[l, block(i), :] = part

    boxes = {RV: (box_rv, x, RING), SX: (box_sx, x, RING), LT: (box_lt, tp, TP), ST: (box_st, tp, TP)}

    def post(kind, g, val):
        box, me, num = boxes[kind]
        box[g, me] = val

        def send(k, carry):
            device = at_x(me + k) if num == RING else {'tp': (me + k) % TP}
            remote(box.at[g, me], box.at[g, me], sts_sem.at[int(kind == SX)], str_sem.at[g, max(kind - 1, 0)], device).start()
            return carry

        lax.fori_loop(1, num, send, 0)

    def collect(kind, g):
        box, me, num = boxes[kind]
        rest = mt.at[0, first(B48)] if kind == LT else box.at[g, first(num - 1)]
        if kind != RV:
            remote(rest, rest, sts_sem.at[int(kind == SX)], str_sem.at[g, max(kind - 1, 0)], partner).wait_recv()
        val = box[g, 0]
        for k in range(1, num):
            val = val + box[g, k]
        return val

    def sums_send(g):
        post(LT, g, lvacc[g])
        post(RV, g, rvacc[g].T[:8])

    beta = beta_ref[0]

    def old_vectors():
        for copy in loads[2:]:
            copy.wait()
        remote(lraw.at[0], lraw.at[0], os_sem.at[0], os_sem.at[1], partner).wait_recv()
        for m in range(2):
            for core in range(2):
                pads[m, core, :, first(B48)] = lraw[m, core]
        pads[2, 0, :, first(KI - LN)] = craw[:, pl.ds(LN, KI - LN)]
        pads[2, 1, :, first(NO)] = oraw[...]
        low, high, rest = craw[:, first(LN)], pads[2, 0], pads[2, 1]
        lanes = [jnp.where(lane8 < B48, pads[m, 0], roll(pads[m, 1], B48)) for m in range(2)]
        rows = [low, jnp.where(lane8 < LN - Q, roll(low, -Q), roll(high, -Q)),
                jnp.where(lane8 < HEAD, roll(high, -16), roll(rest, HEAD)), roll(rest, -B48)]
        for g in range(NG):
            part = slice(LG * g, LG * g + LG)
            lvold[g] = jnp.concatenate([val[part] for val in lanes + lanes], axis=0)
            rvold[g] = jnp.concatenate([val[part] for val in rows], axis=0)

    def vec_swap(g, half, i):
        ref = (lvnew, rvnew)[i]
        return remote(ref.at[half, g], ref.at[half, g], vs_sem.at[0], vs_sem.at[1], partner)

    def moments(g):
        lv_mean = collect(LT, g) / jnp.where(row8 < LG, KIN, NOUT)
        lv_new = beta * lvold[g] + (1.0 - beta) * lv_mean
        lvnew[c, g] = lv_new
        rv_new = beta * rvold[g] + (1.0 - beta) * (collect(RV, g) / NI)
        rvnew[c, g] = rv_new
        for i in range(2):
            vec_swap(g, c, i).start()
        scale_l = 1.0 / jnp.sqrt(jnp.where(k96, lv_new, 1.0))
        scale_r = 1.0 / jnp.sqrt(jnp.where(lane8 < Q, rv_new, 1.0))
        wide = jnp.concatenate([scale_r, jnp.ones((LN - 8, LN), F32)], axis=0).T
        tots = jnp.zeros((8, LN), F32)
        lane1 = lane_of((1, LN))
        for lg in range(LG):
            l = g * LG + lg
            rs = [jnp.broadcast_to(wide[:Q, LG * q + lg:LG * q + lg + 1], (Q, LN)) for q in range(4)]
            sc_in = scale_l[lg:lg + 1, :]
            sc_out = jnp.broadcast_to(scale_l[LG + lg:LG + lg + 1, :], (8, LN))
            parts = []
            for i in range(3):
                body = jnp.where(head, sc_in, sc_out[:1]) if i == 2 else sc_in
                lanes = jnp.where(m96, body, roll(sc_out, B96 - 32 * i)[:1])
                u0 = fin[l, block(i), :] * jnp.where(m96, rs[i], rs[3]) * lanes
                fin[l, block(i), :] = u0
                parts.append(u0 * u0)
            inner = pick(m96, parts[0] + parts[1] + pick(head, parts[2]))
            outer = jnp.where(m96, jnp.where(head, 0.0, parts[2]), parts[0] + parts[1] + parts[2])
            v_in = pick(lane1 < B96, lv_new[lg:lg + 1, :])
            v_out = pick((lane1 >= HEAD) & (lane1 < Q), rv_new[2 * LG + lg:2 * LG + lg + 1, :]) + pick(lane1 < Q, rv_new[3 * LG + lg:3 * LG + lg + 1, :])
            for k, val in enumerate((colsum(inner), colsum(outer), v_in, v_out)):
                tots = jnp.where(row8 == LG * k + lg, val, tots)
        post(ST, g, tots)

    def totals(g):
        val = rowsum(jnp.where(only_x, box_st[g, tp], collect(ST, g)))
        post(SX, g, colsum(pick(row8 == lane8, val)))

    def factors(g):
        val = jnp.where(lane_of((1, LN)) >= 3 * LG, box_sx[g, x], collect(SX, g))
        tot = rowsum(pick(row8 == lane8, val))
        isin = row_of((2 * LG, 1)) < LG
        mean_r = tot[2 * LG:] / jnp.where(isin, NI, NOUT)
        rms = jnp.sqrt(mean_r * tot[:2 * LG] / jnp.where(isin, NI * KIN, NOUT * KO))
        return jnp.sqrt(mean_r) / jnp.maximum(1.0, rms)

    def update(l, lg, fac):
        f_in, f_out = fac[lg:lg + 1, :], fac[LG + lg:LG + lg + 1, :]
        for i in range(3):
            upd = fin[l, block(i), :] * jnp.where((m96 & head) if i == 2 else m96, f_in, f_out)
            new = 0.9 * mpack[l, block(i), :] + 0.1 * upd
            mall[base + l, x, block(i), :] = new.astype(BF16).astype(F32)

    def arrived(l, k):
        return l // LG if k == 0 else 2 * NG if k == 1 and l >= LC - LG else NG + l // LG

    def gather(l, k):
        slot = x if k < 2 else behind(l)
        ref = mall.at[base + l, slot]
        return remote(ref, ref, ags_sem.at[0], agr_sem.at[arrived(l, k)], at_x(behind(l) if k == 1 else ahead(l)))

    def share(l, k, start):
        ref = mall.at[start + l, (behind(l), ahead(l), across, x)[k]]
        return remote(ref, ref, shs_sem.at[0], shr_sem.at[NG if k == 3 and l >= LC - LG else min(l // LG, NG - 1) if l < LC - 1 else NG + 1], partner)

    def send_pair(l):
        gather(l, 0).start()
        gather(l + 1, 0).start()

    def send_back(l):
        gather(l, 1).start()
        gather(l + 1, 1).start()
        share(l, 3, base).start()
        share(l + 1, 3, base).start()

    def forward_pair(l):
        two = mall.at[base + l, first(LG)]
        remote(two, two, ags_sem.at[0], agr_sem.at[arrived(l, 0)], partner).wait_recv()
        for k in (l, l + 1):
            gather(k, 2).start()
            share(k, 0, base).start()

    def half(ref, h, lead=0):
        rows = (first(HALF), pl.ds(HALF, CH - HALF))[h]
        return ref.at[:, rows] if lead else ref.at[rows]

    def gather_half(l, h, slot):
        ref = half(mall.at[base + l, slot], h)
        return remote(ref, ref, ags_sem.at[0], agr_sem.at[0 if h == 0 else 2 * NG + 1], at_x(ahead(l)))

    def send_first():
        for h in range(2):
            for l in range(LG):
                gather_half(l, h, x).start()

    def forward_first():
        for h in range(2):
            two = half(mall.at[base, first(LG)], h, 1)
            remote(two, two, ags_sem.at[0], agr_sem.at[0 if h == 0 else 2 * NG + 1], partner).wait_recv()
            for l in range(LG):
                ref = half(mall.at[base + l, behind(l)], h)
                remote(ref, ref, ags_sem.at[0], agr_sem.at[arrived(l, 2)], at_x(ahead(l))).start()
        share(0, 0, base).start()
        share(1, 0, base).start()

    def settle_pair(l):
        four = mall.at[base + l]
        remote(four, four, ags_sem.at[0], agr_sem.at[arrived(0, 1) + l // LG], partner).wait_recv()
        for k in (l, l + 1):
            for i in (1, 2):
                share(k, i, base).start()

    def settle_last(k):
        l = LC - LG
        two = mall.at[base + l, first(LG)]
        remote(two, two, ags_sem.at[0], agr_sem.at[arrived(l, k)], partner).wait_recv()
        share(l, k, base).start()
        share(l + 1, k, base).start()

    rate = rate_ref[0]
    decay = rate * wd_ref[0]

    def unpack(at):
        for q in range(4):
            if q < 3:
                chunk = [mall[at, d, block(q), :] for d in range(RING)]
            else:
                chunk = [last_quarter([mall[at, d, block(i), :] for i in range(3)]) for d in range(RING)]
            r1, r2, r3 = roll(chunk[1], B96), roll(chunk[2], 64), roll(chunk[3], 32)
            mom = (jnp.where(m96, chunk[0], r1), jnp.where(lane < 64, r1, r2), jnp.where(lane < 32, r2, r3))
            spots = (((wn_in, 0, 0, Q),), ((wn_in, Q, 0, Q),), ((wn_in, 2 * Q, 0, HEAD), (wn_out, 0, HEAD, B48)), ((wn_out, B48, 0, Q),))[q]
            for t in range(3):
                for ref, dst, src, num in spots:
                    rows = pl.ds(dst, num)
                    w = ref[at, rows, tile_cols(t)]
                    ref[at, rows, tile_cols(t)] = w - rate * mom[t][src:src + num] - decay * w

    def turn_moment(at):
        parts = [mall[at, x, block(i), :] for i in range(3)]
        parts.append(last_quarter(parts))
        spots = ((0, 0, Q),), ((Q, 0, Q),), ((2 * Q, 0, HEAD), (MID, HEAD, B48)), ((MID + B48, 0, Q),)
        for val, places in zip(parts, spots):
            val = jnp.where(c == 0, val, roll(val, -B48))
            for dst, src, num in places:
                tall[pl.ds(dst, num), :] = val[src:src + num]
        turned = [tall[tile_cols(t), :].T[:B48] for t in range(3)]
        mn_in[at, :, first(LN)] = turned[0].astype(BF16)
        mn_in[at, :, pl.ds(LN, KI - LN)] = turned[1][:, :KI - LN].astype(BF16)
        mn_out[at] = turned[2][:, :NO].astype(BF16)

    def each(step, l, start):
        lax.fori_loop(start + l, start + l + LG, lambda at, carry: (step(at), carry)[1], 0)

    def unpack_pair(l, start):
        each(unpack, l, start)
        if l < LC - LG:
            each(turn_moment, l, start)

    def turn_last():
        l = LC - LG
        each(turn_moment, l, base)
        two = mall.at[base, first(LG)]
        remote(two, two, shs_sem.at[0], shr_sem.at[NG], partner).wait_recv()
        each(turn_moment, l, pbase)

    def take_pair(l):
        two = mall.at[pl.ds(pbase + l, LG)]
        remote(two, two, shs_sem.at[0], shr_sem.at[l // LG], partner).wait_recv()
        unpack_pair(l, pbase)

    def take_last():
        for l in range(LC - LG, LC):
            three = mall.at[pbase + l, first(3)]
            remote(three, three, shs_sem.at[0], shr_sem.at[NG - 1 if l < LC - 1 else NG + 1], partner).wait_recv()
            lax.fori_loop(pbase + l, pbase + l + 1, lambda at, carry: (unpack(at), carry)[1], 0)

    def new_vectors():
        lane4 = lane_of((LG, LN))
        for half in range(2):
            for g in range(NG):
                rows = pl.ds(LC * half + LG * g, LG)
                both, val = lvnew[half, g], rvnew[half, g]
                both = jnp.where(c == 0, both, roll(both, -B48))
                rn_in[rows, :] = both[:LG, :B48]
                cn_out[rows, :] = both[LG:2 * LG, :B48]
                two = roll(val, Q)[LG:2 * LG]
                cn_in[rows, first(LN)] = jnp.where(lane4 < Q, val[:LG], two)
                cn_in[rows, pl.ds(LN, KI - LN)] = jnp.where(lane4 < 16, two, roll(val, 16)[2 * LG:3 * LG])[:, :KI - LN]
                rn_out[rows, :] = jnp.where(lane4 < B48, roll(val, -HEAD)[2 * LG:3 * LG], roll(val, B48)[3 * LG:])[:, :NO]

    def both(step, g):
        lax.fori_loop(LG * g, LG * g + LG, lambda l, carry: (step(l), carry)[1], 0)

    def swap_start(l):
        swap(l, 0).start()
        swap(l, 1).start()

    def pack_first():
        for l in range(LG):
            local(gbuf.at[l], gbuf.at[l], gl_sem.at[l]).wait()
            swap_first(l).wait_recv()
            stage_a(l)
            if l == 0:
                both(swap_start, 1)
        both(lambda l: step3(l).start(), 0)

    def pack_pair(g):
        two = pl.ds(LG * g, LG)
        if g == 1:
            rest = gbuf.at[pl.ds(LG, LC - LG)]
            local(rest, rest, gl_sem.at[LG]).wait()
        remote(pbuf.at[two], pbuf.at[two], gs_sem.at[0], gr_sem.at[g], partner).wait_recv()
        if g + 1 < NG:
            both(swap_start, g + 1)
        both(stage_a, g)
        both(lambda l: step1(l).start(), g)

    def direct_pair(g):
        both(lambda l: step3(l).start(), g)

    def cast_all():
        loads[0].wait()
        loads[1].wait()
        lax.fori_loop(0, LC, lambda l, carry: (stage_n(l), carry)[1], 0)

    def relay_pair(g):
        two = via.at[pl.ds(LG * g, LG)]
        remote(two, two, s_sem.at[0], via_sem.at[g], partner).wait_recv()
        both(stage_b, g)

    def sum_pair(g):
        two = rin.at[pl.ds(LG * g, LG)]
        remote(two, two, s_sem.at[0], rin_sem.at[g], partner).wait_recv()
        both(stage_c, g)
        sums_send(g)

    def moment_pair(g):
        if g == 0:
            remote(msend, msend, ms_sem.at[0], mr_sem.at[0], partner).wait_recv()
        both(stage_m, g)

    def update_pair(g):
        fac = factors(g)
        for lg in range(LG):
            update(LG * g + lg, lg, fac)

    pack_first()
    pack_pair(1)
    cast_all()
    w_loads[0].start()
    w_loads[1].start()
    old_vectors()
    pl.semaphore_wait(ready, RING - 1)
    relay_pair(0)
    direct_pair(1)
    pack_pair(2)
    sum_pair(0)
    relay_pair(1)
    direct_pair(2)
    moment_pair(0)
    pack_pair(3)
    moments(0)
    sum_pair(1)
    relay_pair(2)
    moment_pair(1)
    totals(0)
    direct_pair(3)
    relay_pair(3)
    moments(1)
    sum_pair(2)
    moment_pair(2)
    update_pair(0)
    send_first()
    totals(1)
    send_back(0)
    sum_pair(3)
    moment_pair(3)
    moments(2)
    forward_first()
    update_pair(1)
    send_pair(2)
    moments(3)
    totals(2)
    send_back(2)
    forward_pair(2)
    settle_pair(0)
    totals(3)
    update_pair(2)
    send_pair(4)
    send_back(4)
    w_loads[0].wait()
    w_loads[1].wait()
    unpack_pair(0, base)
    take_pair(0)
    settle_pair(2)
    update_pair(3)
    send_pair(6)
    forward_pair(4)
    send_back(6)
    unpack_pair(2, base)
    take_pair(2)
    remote(lvnew, lvnew, vs_sem.at[0], vs_sem.at[1], partner).wait_recv()
    new_vectors()
    turn_last()
    forward_pair(6)
    settle_pair(4)
    unpack_pair(4, base)
    settle_last(1)
    take_pair(4)
    settle_last(2)
    unpack_pair(6, base)
    take_last()
    for ref, sem in ((pbuf, gs_sem), (msend, ms_sem), (mall.at[first(6)], s_sem), (mall.at[first(6)], ags_sem), (mall.at[first(8)], shs_sem),
                     (lraw.at[0], os_sem), (mt.at[first(4), first(88)], sts_sem), (lvnew, vs_sem)):
        remote(ref, ref, sem.at[0], os_sem.at[1], partner).wait_send()
    last = box_sx.at[:, first(RING - 1)]
    remote(last, last, sts_sem.at[1], os_sem.at[1], partner).wait_send()


def update_call(scalars, arrays):
    hbm, smem = pl.BlockSpec(memory_space=pltpu.HBM), pl.BlockSpec(memory_space=pltpu.SMEM)
    dma, vmem = pltpu.SemaphoreType.DMA, pltpu.VMEM

    def lanes(*lead):
        return vmem(lead + (LN,), F32)

    scratch = [
        vmem((LC, KI + NO, D), F32), vmem((LC, KI + NO, D), F32), vmem((LG, KI + NO, D), F32), lanes(LC, RING, CH), lanes(LC, CH), lanes(LC, 2, CH), lanes(LC, CH),
        lanes(L, RING, CH), vmem((L, B48, KI), BF16), vmem((L, B48, NO), BF16), vmem((LC, B48, D), F32), vmem((LC, LN, D), F32),
        lanes(LC, CH), lanes(D), lanes(NG, LN), lanes(NG, 8),
        vmem((2, 2, LC, B48), F32), vmem((LC, KI), F32), vmem((LC, NO), F32), lanes(3, 2, LC),
        lanes(NG, 8), lanes(NG, 8), lanes(2, NG, 8), lanes(2, NG, 8),
        lanes(NG, RING, 8), lanes(NG, RING, 1), lanes(NG, TP, 8), lanes(NG, TP, 8),
        dma((LG + 1,)), dma((LG,)), dma((1,)), dma((NG + LG,)), dma((2,)), dma((1,)), dma((1,)), dma((1,)), dma((NG,)), dma((NG,)),
        dma((1,)), dma((2 * NG + 2,)), dma((1,)), dma((NG + 2,)), dma((2,)), dma((NG, 3)), dma((2,)), dma((4,)),
        dma((2,)), dma((2,)), pltpu.SemaphoreType.REGULAR,
    ]
    outs = [((L, KI, D), F32), ((L, NO, D), F32), ((L, B48, KI), BF16), ((L, B48, NO), BF16),
            ((L, B48), F32), ((L, KI), F32), ((L, NO), F32), ((L, B48), F32)]
    return pl.pallas_call(
        kernel,
        out_shape=[vmem(*out) for out in outs],
        in_specs=[smem] * len(scalars) + [hbm] * len(arrays),
        out_specs=[pl.BlockSpec(memory_space=vmem)] * len(outs),
        scratch_shapes=scratch,
        compiler_params=pltpu.CompilerParams(collective_id=0, has_side_effects=True, vmem_limit_bytes=36 * 2**20),
        name='adafactor',
    )(*[val.reshape(1) for val in scalars], *[pltpu.with_memory_space_constraint(val, pltpu.HBM) for val in arrays])


def store_kernel(*refs):
    num = len(refs) // 2
    copies = [pltpu.make_async_copy(src, dst, refs[-1].at[i]) for i, (src, dst) in enumerate(zip(refs[:num], refs[num:-1]))]
    for copy in copies:
        copy.start()
    for copy in copies:
        copy.wait()


def store_call(vals):
    anyspace = pl.BlockSpec(memory_space=pl.ANY)
    return pl.pallas_call(
        store_kernel,
        out_shape=[jax.ShapeDtypeStruct(val.shape, val.dtype) for val in vals],
        in_specs=[anyspace] * len(vals),
        out_specs=[anyspace] * len(vals),
        scratch_shapes=[pltpu.SemaphoreType.DMA((len(vals),))],
        compiler_params=pltpu.CompilerParams(vmem_limit_bytes=2**20),
        name='store',
    )(*[pltpu.with_memory_space_constraint(val, pltpu.VMEM) for val in vals])


def solution(mesh):
    def turn(val):
        return val.swapaxes(1, 2)

    def body(w_in, w_out, g_in, g_out, m_in, m_out, r_in, c_in, r_out, c_out, learn_rate, weight_decay, beta_two):
        out = store_call(update_call((learn_rate, weight_decay, beta_two),
                          (turn(w_in), w_out, turn(g_in[0]), g_out[0], m_in, turn(m_out), r_in, c_in, r_out, c_out)))
        return (turn(out[0]), out[1], out[2], turn(out[3])) + tuple(out[4:])

    cols, rows, own = P(None, None, 'tp'), P(None, 'tp', None), P(None, 'dp')
    outs = (cols, rows, P(None, 'dp', 'tp'), P(None, 'tp', 'dp'), own, P(None, 'tp'), P(None, 'tp'), own)
    in_specs = (cols, rows, P('dp', *cols), P('dp', *rows)) + outs[2:] + (P(), P(), P())
    return jax.shard_map(body, mesh=mesh, in_specs=in_specs, out_specs=outs, check_vma=False)
```

```python
import jax
import jax.numpy as jnp
from jax import lax
from jax.experimental import pallas as pl
from jax.experimental.pallas import tpu as pltpu
from jax.sharding import PartitionSpec as P

F32, BF16 = jnp.float32, jnp.bfloat16
MESH = pl.DeviceIdType.MESH
RING = 4
L, D = 16, 384
KI, NO = 168, 120
LC, LG, NG = 8, 2, 4
Q, LN, B48, B96 = 72, 128, 48, 96
CH, HEAD, MID, HALF = 3 * Q, KI - 2 * Q, 256, 104
NI, KIN, NOUT, KO = 384.0, 2688.0, 1920.0, 384.0
KINDS = RV, LT, SX, ST = range(4)
TP = RING * RING


def roll(val, shift):
    return pltpu.roll(val, shift % LN, 1)


def lane_of(shape):
    return lax.broadcasted_iota(jnp.int32, shape, 1)


def row_of(shape):
    return lax.broadcasted_iota(jnp.int32, shape, 0)


def colsum(val):
    return jnp.sum(val, axis=0, keepdims=True)


def rowsum(val):
    return jnp.sum(val, axis=1, keepdims=True)


def pick(cond, val):
    return jnp.where(cond, val, 0.0)


def first(num):
    return pl.ds(0, num)


def block(i):
    return pl.ds(Q * i, Q)


def tile_cols(t):
    return pl.ds(LN * t, LN)


def last_quarter(parts):
    lane = lane_of(parts[0].shape)
    tail = jnp.where(lane < 64, roll(parts[1], 64), roll(parts[2], B96))
    return jnp.where(lane < 32, roll(parts[0], 32), tail)


def join_quarters(quarters, keep):
    return [jnp.where(keep, quarters[i], roll(quarters[3], B96 - 32 * i)) for i in range(3)]


def kernel(rate_ref, wd_ref, beta_ref, w_in, w_out, g_in, g_out, m_in, m_out, r_in, c_in, r_out, c_out,
           wn_in, wn_out, mn_in, mn_out, rn_in, cn_in, rn_out, cn_out,
           gbuf, pbuf, gsend, pack, via, rin, fin, mall, mraw_in, mraw_out, msend, mt, mpack, tall,
           rvacc, lvacc, lraw, craw, oraw, pads, lvold, rvold, lvnew, rvnew, box_rv, box_sx, box_lt, box_st,
           gl_sem, gp_sem, gs_sem, gr_sem, ml_sem, ms_sem, mr_sem, s_sem, via_sem, rin_sem, ags_sem, agr_sem,
           shs_sem, shr_sem, sts_sem, str_sem, vs_sem, ol_sem, os_sem, wl_sem, ready):
    tp, dp = lax.axis_index('tp'), lax.axis_index('dp')
    z, y, x, c = tp // RING, tp % RING, dp // 2, dp % 2
    other = 1 - c
    base, pbase = c * LC, other * LC

    def at_x(xx):
        return {'dp': (xx % RING) * 2 + c}

    def at_y(yy):
        return {'tp': z * RING + yy % RING}

    def at_z(zz):
        return {'tp': (zz % RING) * RING + y}

    partner = {'dp': x * 2 + other}

    def local(src, dst, sem):
        return pltpu.make_async_copy(src, dst, sem)

    def remote(src, dst, send_sem, recv_sem, device):
        return pltpu.make_async_remote_copy(src_ref=src, dst_ref=dst, send_sem=send_sem, recv_sem=recv_sem,
                                            device_id=device, device_id_type=MESH)

    def greet(step):
        for peer in plane:
            pl.semaphore_signal(ready.at[step], inc=1, device_id=peer, device_id_type=MESH)

    def greeted(step):
        pl.semaphore_wait(ready.at[step], len(plane))

    barrier = pltpu.get_barrier_semaphore()
    plane = [at_y(y + 1), at_y(y + RING - 1), at_z(z + 1), at_z(z + RING - 1)]
    peers = [partner, at_x(x + 1), at_x(x + RING - 1)] + plane
    for peer in peers:
        pl.semaphore_signal(barrier, inc=1, device_id=peer, device_id_type=MESH)

    def own(l, i):
        src, dst = ((g_in, first(KI)), (g_out, pl.ds(KI, NO)))[i]
        return local(src.at[base + l], gbuf.at[l, dst], gl_sem.at[l if isinstance(l, int) else LG])

    def others(l, i):
        src, dst = ((g_in, first(KI)), (g_out, pl.ds(KI, NO)))[i]
        return local(src.at[pbase + l], gsend.at[l, dst], gp_sem.at[l])

    def swap_first(l):
        return remote(gsend.at[l], pbuf.at[l], gs_sem.at[0], gr_sem.at[NG + l], partner)

    def swap(l, i):
        src, dst = ((g_in, first(KI)), (g_out, pl.ds(KI, NO)))[i]
        return remote(src.at[pbase + l], pbuf.at[l, dst], gs_sem.at[0], gr_sem.at[l // LG], partner)

    my_rows, its_rows = pl.ds(base, LC), pl.ds(pbase, LC)
    loads = [local(m_in, mraw_in, ml_sem.at[0]), local(m_out, mraw_out, ml_sem.at[1]),
             local(r_in.at[my_rows], lraw.at[0, c], ol_sem.at[0]), local(c_out.at[my_rows], lraw.at[1, c], ol_sem.at[1]),
             local(c_in.at[my_rows], craw, ol_sem.at[2]), local(r_out.at[my_rows], oraw, ol_sem.at[3])]
    w_loads = [local(w_in, wn_in, wl_sem.at[0]), local(w_out, wn_out, wl_sem.at[1])]

    def lane_swap(m, core):
        return remote((r_in, c_out)[m].at[its_rows], lraw.at[m, core], os_sem.at[0], os_sem.at[1], partner)

    def start_loads(l, carry):
        own(l, 0).start()
        own(l, 1).start()
        return carry

    for l in range(LG):
        for i in range(2):
            others(l, i).start()
            own(l, i).start()
    lax.fori_loop(LG, LC, start_loads, 0)
    for copy in loads:
        copy.start()
    pl.semaphore_wait(barrier, len(peers))
    greet(0)
    for l in range(LG):
        local(gsend.at[l], gsend.at[l], gp_sem.at[l]).wait()
        swap_first(l).start()
    lane_swap(0, c).start()
    lane_swap(1, c).start()
    rvacc[...] = jnp.zeros_like(rvacc)
    lvacc[...] = jnp.zeros_like(lvacc)

    lane, lane8, row8 = lane_of((Q, LN)), lane_of((8, LN)), row_of((8, LN))
    m96, k96 = lane < B96, lane8 < B96
    head = row_of((Q, LN)) < HEAD
    only_x = (row8 >= 2 * LG) & (row8 < 3 * LG)

    def way(l):
        return 1 - 2 * (l % 2)

    def ahead(l):
        return (x + way(l) + RING) % RING

    def behind(l):
        return (x - way(l) + RING) % RING

    across = (x + 2) % RING

    def step1(l):
        return remote(pack.at[l, across], via.at[l], s_sem.at[0], via_sem.at[l // LG], at_x(ahead(l)))

    def step2(l):
        return remote(pack.at[l, ahead(l)], rin.at[l, 0], s_sem.at[0], rin_sem.at[l // LG], at_x(ahead(l)))

    def step3(l):
        return remote(pack.at[l, behind(l)], rin.at[l, 1], s_sem.at[0], rin_sem.at[l // LG], at_x(behind(l)))

    def m_rows(core):
        return pl.ds(pl.multiple_of(core * B48, 16), B48)

    def moment_swap(l, core):
        return remote(msend.at[l], mt.at[l, m_rows(core)], ms_sem.at[0], mr_sem.at[0], partner)

    def stage_a(l):
        def tile(t, q):
            return gbuf[l, block(q), tile_cols(t)] + pbuf[l, block(q), tile_cols(t)]

        def chunk(d, q):
            if d == 0:
                return tile(0, q)
            if d == 1:
                return roll(jnp.where(m96, tile(1, q), tile(0, q)), 32)
            if d == 2:
                return roll(jnp.where(lane < 64, tile(2, q), tile(1, q)), 64)
            return roll(tile(2, q), B96)

        def put(d):
            for i, val in enumerate(join_quarters([chunk(d, q) for q in range(4)], m96)):
                pack[l, d, block(i), :] = val

        if not isinstance(l, int):
            for d in range(RING):
                put(d)
            return

        for d in range(RING):
            pl.when(across == d)(lambda: put(d))
        step1(l).start()
        for d in range(RING):
            pl.when(across != d)(lambda: put(d))

    def stage_n(l):
        msend[l, :, first(KI)] = mraw_in[pbase + l].astype(F32)
        msend[l, :, pl.ds(MID, NO)] = mraw_out[pbase + l].astype(F32)
        moment_swap(l, c).start()
        mt[l, m_rows(c), first(KI)] = mraw_in[base + l].astype(F32)
        mt[l, m_rows(c), pl.ds(MID, NO)] = mraw_out[base + l].astype(F32)

    def stage_b(l):
        to = ahead(l)
        pack[l, to] = pack[l, to] + via[l]
        step2(l).start()

    def stage_c(l):
        sq = []
        for i in range(3):
            grad = pack[l, x, block(i), :] + rin[l, 0, block(i), :] + rin[l, 1, block(i), :]
            fin[l, block(i), :] = grad
            sq.append(grad * grad + 1e-30)
        g, lg = l // LG, l % LG
        sums = [rowsum(pick(m96, val)) for val in sq]
        sums.append(rowsum(jnp.where(m96, 0.0, sq[0] + sq[1] + sq[2])))
        acc = rvacc[g, first(Q), :]
        for q in range(4):
            acc = jnp.where(lane == LG * q + lg, sums[q], acc)
        rvacc[g, first(Q), :] = acc
        top = colsum(pick(head, sq[2]))
        low = colsum(jnp.where(head, 0.0, sq[2]))
        cols = [colsum(sq[0]), colsum(sq[1])]
        wide = [jnp.broadcast_to(val, (8, LN)) for val in (cols[0], cols[1], top + low)]
        in_sum = pick(k96, cols[0] + cols[1] + top)
        out_sum = pick(k96, low + last_quarter(wide))
        both = jnp.where(row8 == lg, in_sum, lvacc[g])
        lvacc[g] = jnp.where(row8 == LG + lg, out_sum, both)

    def stage_m(l):
        val = mt[l].T
        third = jnp.concatenate([val[2 * Q:KI], val[MID:MID + B48]], axis=0)
        quarters = [val[:Q], val[Q:2 * Q], third, val[MID + B48:MID + NO]]
        for i, part in enumerate(join_quarters(quarters, m96)):
            mpack[l, block(i), :] = part

    boxes = {RV: (box_rv, x, RING), SX: (box_sx, x, RING), LT: (box_lt, tp, TP), ST: (box_st, tp, TP)}

    def post(kind, g, val):
        box, me, num = boxes[kind]
        box[g, me] = val

        def send(k, carry):
            device = at_x(me + k) if num == RING else {'tp': (me + k) % TP}
            remote(box.at[g, me], box.at[g, me], sts_sem.at[int(kind == SX)], str_sem.at[g, max(kind - 1, 0)], device).start()
            return carry

        lax.fori_loop(1, num, send, 0)

    def collect(kind, g):
        box, me, num = boxes[kind]
        rest = mt.at[0, first(B48)] if kind == LT else box.at[g, first(num - 1)]
        if kind != RV:
            remote(rest, rest, sts_sem.at[int(kind == SX)], str_sem.at[g, max(kind - 1, 0)], partner).wait_recv()
        val = box[g, 0]
        for k in range(1, num):
            val = val + box[g, k]
        return val

    def sums_send(g):
        post(LT, g, lvacc[g])
        post(RV, g, rvacc[g].T[:8])

    beta = beta_ref[0]

    def old_vectors():
        for copy in loads[2:]:
            copy.wait()
        remote(lraw.at[0], lraw.at[0], os_sem.at[0], os_sem.at[1], partner).wait_recv()
        for m in range(2):
            for core in range(2):
                pads[m, core, :, first(B48)] = lraw[m, core]
        pads[2, 0, :, first(KI - LN)] = craw[:, pl.ds(LN, KI - LN)]
        pads[2, 1, :, first(NO)] = oraw[...]
        low, high, rest = craw[:, first(LN)], pads[2, 0], pads[2, 1]
        lanes = [jnp.where(lane8 < B48, pads[m, 0], roll(pads[m, 1], B48)) for m in range(2)]
        rows = [low, jnp.where(lane8 < LN - Q, roll(low, -Q), roll(high, -Q)),
                jnp.where(lane8 < HEAD, roll(high, -16), roll(rest, HEAD)), roll(rest, -B48)]
        for g in range(NG):
            part = slice(LG * g, LG * g + LG)
            lvold[g] = jnp.concatenate([val[part] for val in lanes + lanes], axis=0)
            rvold[g] = jnp.concatenate([val[part] for val in rows], axis=0)

    def vec_swap(g, half, i):
        ref = (lvnew, rvnew)[i]
        return remote(ref.at[half, g], ref.at[half, g], vs_sem.at[0], vs_sem.at[1], partner)

    def moments(g):
        lv_mean = collect(LT, g) / jnp.where(row8 < LG, KIN, NOUT)
        lv_new = beta * lvold[g] + (1.0 - beta) * lv_mean
        lvnew[c, g] = lv_new
        rv_new = beta * rvold[g] + (1.0 - beta) * (collect(RV, g) / NI)
        rvnew[c, g] = rv_new
        for i in range(2):
            vec_swap(g, c, i).start()
        scale_l = 1.0 / jnp.sqrt(jnp.where(k96, lv_new, 1.0))
        scale_r = 1.0 / jnp.sqrt(jnp.where(lane8 < Q, rv_new, 1.0))
        wide = jnp.concatenate([scale_r, jnp.ones((LN - 8, LN), F32)], axis=0).T
        tots = jnp.zeros((8, LN), F32)
        lane1 = lane_of((1, LN))
        for lg in range(LG):
            l = g * LG + lg
            rs = [jnp.broadcast_to(wide[:Q, LG * q + lg:LG * q + lg + 1], (Q, LN)) for q in range(4)]
            sc_in = scale_l[lg:lg + 1, :]
            sc_out = jnp.broadcast_to(scale_l[LG + lg:LG + lg + 1, :], (8, LN))
            parts = []
            for i in range(3):
                body = jnp.where(head, sc_in, sc_out[:1]) if i == 2 else sc_in
                lanes = jnp.where(m96, body, roll(sc_out, B96 - 32 * i)[:1])
                u0 = fin[l, block(i), :] * jnp.where(m96, rs[i], rs[3]) * lanes
                fin[l, block(i), :] = u0
                parts.append(u0 * u0)
            inner = pick(m96, parts[0] + parts[1] + pick(head, parts[2]))
            outer = jnp.where(m96, jnp.where(head, 0.0, parts[2]), parts[0] + parts[1] + parts[2])
            v_in = pick(lane1 < B96, lv_new[lg:lg + 1, :])
            v_out = pick((lane1 >= HEAD) & (lane1 < Q), rv_new[2 * LG + lg:2 * LG + lg + 1, :]) + pick(lane1 < Q, rv_new[3 * LG + lg:3 * LG + lg + 1, :])
            for k, val in enumerate((colsum(inner), colsum(outer), v_in, v_out)):
                tots = jnp.where(row8 == LG * k + lg, val, tots)
        post(ST, g, tots)

    def totals(g):
        val = rowsum(jnp.where(only_x, box_st[g, tp], collect(ST, g)))
        post(SX, g, colsum(pick(row8 == lane8, val)))

    def factors(g):
        val = jnp.where(lane_of((1, LN)) >= 3 * LG, box_sx[g, x], collect(SX, g))
        tot = rowsum(pick(row8 == lane8, val))
        isin = row_of((2 * LG, 1)) < LG
        mean_r = tot[2 * LG:] / jnp.where(isin, NI, NOUT)
        rms = jnp.sqrt(mean_r * tot[:2 * LG] / jnp.where(isin, NI * KIN, NOUT * KO))
        return jnp.sqrt(mean_r) / jnp.maximum(1.0, rms)

    def update(l, lg, fac):
        f_in, f_out = fac[lg:lg + 1, :], fac[LG + lg:LG + lg + 1, :]
        for i in range(3):
            upd = fin[l, block(i), :] * jnp.where((m96 & head) if i == 2 else m96, f_in, f_out)
            new = 0.9 * mpack[l, block(i), :] + 0.1 * upd
            mall[base + l, x, block(i), :] = new.astype(BF16).astype(F32)

    def arrived(l, k):
        return l // LG if k == 0 else 2 * NG if k == 1 and l >= LC - LG else NG + l // LG

    def gather(l, k):
        slot = x if k < 2 else behind(l)
        ref = mall.at[base + l, slot]
        return remote(ref, ref, ags_sem.at[0], agr_sem.at[arrived(l, k)], at_x(behind(l) if k == 1 else ahead(l)))

    def share(l, k, start):
        ref = mall.at[start + l, (behind(l), ahead(l), across, x)[k]]
        return remote(ref, ref, shs_sem.at[0], shr_sem.at[NG if k == 3 and l >= LC - LG else min(l // LG, NG - 1) if l < LC - 1 else NG + 1], partner)

    def send_pair(l):
        gather(l, 0).start()
        gather(l + 1, 0).start()

    def send_back(l):
        gather(l, 1).start()
        gather(l + 1, 1).start()
        share(l, 3, base).start()
        share(l + 1, 3, base).start()

    def forward_pair(l):
        two = mall.at[base + l, first(LG)]
        remote(two, two, ags_sem.at[0], agr_sem.at[arrived(l, 0)], partner).wait_recv()
        for k in (l, l + 1):
            gather(k, 2).start()
            share(k, 0, base).start()

    def half(ref, h, lead=0):
        rows = (first(HALF), pl.ds(HALF, CH - HALF))[h]
        return ref.at[:, rows] if lead else ref.at[rows]

    def gather_half(l, h, slot):
        ref = half(mall.at[base + l, slot], h)
        return remote(ref, ref, ags_sem.at[0], agr_sem.at[0 if h == 0 else 2 * NG + 1], at_x(ahead(l)))

    def send_first():
        for h in range(2):
            for l in range(LG):
                gather_half(l, h, x).start()

    def forward_first():
        for h in range(2):
            two = half(mall.at[base, first(LG)], h, 1)
            remote(two, two, ags_sem.at[0], agr_sem.at[0 if h == 0 else 2 * NG + 1], partner).wait_recv()
            for l in range(LG):
                ref = half(mall.at[base + l, behind(l)], h)
                remote(ref, ref, ags_sem.at[0], agr_sem.at[arrived(l, 2)], at_x(ahead(l))).start()
        share(0, 0, base).start()
        share(1, 0, base).start()

    def settle_pair(l):
        four = mall.at[base + l]
        remote(four, four, ags_sem.at[0], agr_sem.at[arrived(0, 1) + l // LG], partner).wait_recv()
        for k in (l, l + 1):
            for i in (1, 2):
                share(k, i, base).start()

    def settle_last(k):
        l = LC - LG
        two = mall.at[base + l, first(LG)]
        remote(two, two, ags_sem.at[0], agr_sem.at[arrived(l, k)], partner).wait_recv()
        share(l, k, base).start()
        share(l + 1, k, base).start()

    rate = rate_ref[0]
    decay = rate * wd_ref[0]

    def unpack(at):
        for q in range(4):
            if q < 3:
                chunk = [mall[at, d, block(q), :] for d in range(RING)]
            else:
                chunk = [last_quarter([mall[at, d, block(i), :] for i in range(3)]) for d in range(RING)]
            r1, r2, r3 = roll(chunk[1], B96), roll(chunk[2], 64), roll(chunk[3], 32)
            mom = (jnp.where(m96, chunk[0], r1), jnp.where(lane < 64, r1, r2), jnp.where(lane < 32, r2, r3))
            spots = (((wn_in, 0, 0, Q),), ((wn_in, Q, 0, Q),), ((wn_in, 2 * Q, 0, HEAD), (wn_out, 0, HEAD, B48)), ((wn_out, B48, 0, Q),))[q]
            for t in range(3):
                for ref, dst, src, num in spots:
                    rows = pl.ds(dst, num)
                    w = ref[at, rows, tile_cols(t)]
                    ref[at, rows, tile_cols(t)] = w - rate * mom[t][src:src + num] - decay * w

    def turn_moment(at):
        parts = [mall[at, x, block(i), :] for i in range(3)]
        parts.append(last_quarter(parts))
        spots = ((0, 0, Q),), ((Q, 0, Q),), ((2 * Q, 0, HEAD), (MID, HEAD, B48)), ((MID + B48, 0, Q),)
        for val, places in zip(parts, spots):
            val = jnp.where(c == 0, val, roll(val, -B48))
            for dst, src, num in places:
                tall[pl.ds(dst, num), :] = val[src:src + num]
        turned = [tall[tile_cols(t), :].T[:B48] for t in range(3)]
        mn_in[at, :, first(LN)] = turned[0].astype(BF16)
        mn_in[at, :, pl.ds(LN, KI - LN)] = turned[1][:, :KI - LN].astype(BF16)
        mn_out[at] = turned[2][:, :NO].astype(BF16)

    def each(step, l, start):
        lax.fori_loop(start + l, start + l + LG, lambda at, carry: (step(at), carry)[1], 0)

    def unpack_pair(l, start):
        each(unpack, l, start)
        if l < LC - LG:
            each(turn_moment, l, start)

    def turn_last():
        l = LC - LG
        each(turn_moment, l, base)
        two = mall.at[base, first(LG)]
        remote(two, two, shs_sem.at[0], shr_sem.at[NG], partner).wait_recv()
        each(turn_moment, l, pbase)

    def take_pair(l):
        two = mall.at[pl.ds(pbase + l, LG)]
        remote(two, two, shs_sem.at[0], shr_sem.at[l // LG], partner).wait_recv()
        unpack_pair(l, pbase)

    def take_last():
        for l in range(LC - LG, LC):
            three = mall.at[pbase + l, first(3)]
            remote(three, three, shs_sem.at[0], shr_sem.at[NG - 1 if l < LC - 1 else NG + 1], partner).wait_recv()
            lax.fori_loop(pbase + l, pbase + l + 1, lambda at, carry: (unpack(at), carry)[1], 0)

    def new_vectors():
        lane4 = lane_of((LG, LN))
        for half in range(2):
            for g in range(NG):
                rows = pl.ds(LC * half + LG * g, LG)
                both, val = lvnew[half, g], rvnew[half, g]
                both = jnp.where(c == 0, both, roll(both, -B48))
                rn_in[rows, :] = both[:LG, :B48]
                cn_out[rows, :] = both[LG:2 * LG, :B48]
                two = roll(val, Q)[LG:2 * LG]
                cn_in[rows, first(LN)] = jnp.where(lane4 < Q, val[:LG], two)
                cn_in[rows, pl.ds(LN, KI - LN)] = jnp.where(lane4 < 16, two, roll(val, 16)[2 * LG:3 * LG])[:, :KI - LN]
                rn_out[rows, :] = jnp.where(lane4 < B48, roll(val, -HEAD)[2 * LG:3 * LG], roll(val, B48)[3 * LG:])[:, :NO]

    def both(step, g):
        lax.fori_loop(LG * g, LG * g + LG, lambda l, carry: (step(l), carry)[1], 0)

    def swap_start(l):
        swap(l, 0).start()
        swap(l, 1).start()

    def pack_first():
        for l in range(LG):
            local(gbuf.at[l], gbuf.at[l], gl_sem.at[l]).wait()
            swap_first(l).wait_recv()
            stage_a(l)
            if l == 0:
                both(swap_start, 1)
        both(lambda l: step3(l).start(), 0)

    def pack_pair(g):
        two = pl.ds(LG * g, LG)
        if g == 1:
            rest = gbuf.at[pl.ds(LG, LC - LG)]
            local(rest, rest, gl_sem.at[LG]).wait()
        remote(pbuf.at[two], pbuf.at[two], gs_sem.at[0], gr_sem.at[g], partner).wait_recv()
        if g + 1 < NG:
            both(swap_start, g + 1)
        both(stage_a, g)
        both(lambda l: step1(l).start(), g)

    def direct_pair(g):
        both(lambda l: step3(l).start(), g)

    def cast_all():
        loads[0].wait()
        loads[1].wait()
        lax.fori_loop(0, LC, lambda l, carry: (stage_n(l), carry)[1], 0)

    def relay_pair(g):
        two = via.at[pl.ds(LG * g, LG)]
        remote(two, two, s_sem.at[0], via_sem.at[g], partner).wait_recv()
        both(stage_b, g)

    def sum_pair(g):
        two = rin.at[pl.ds(LG * g, LG)]
        remote(two, two, s_sem.at[0], rin_sem.at[g], partner).wait_recv()
        both(stage_c, g)
        sums_send(g)

    def moment_pair(g):
        if g == 0:
            remote(msend, msend, ms_sem.at[0], mr_sem.at[0], partner).wait_recv()
        both(stage_m, g)

    def update_pair(g):
        fac = factors(g)
        for lg in range(LG):
            update(LG * g + lg, lg, fac)

    pack_first()
    pack_pair(1)
    cast_all()
    w_loads[0].start()
    w_loads[1].start()
    old_vectors()
    greeted(0)
    greet(1)
    relay_pair(0)
    direct_pair(1)
    greeted(1)
    greet(2)
    pack_pair(2)
    greeted(2)
    sum_pair(0)
    relay_pair(1)
    direct_pair(2)
    moment_pair(0)
    pack_pair(3)
    moments(0)
    sum_pair(1)
    relay_pair(2)
    moment_pair(1)
    totals(0)
    direct_pair(3)
    relay_pair(3)
    moments(1)
    sum_pair(2)
    moment_pair(2)
    update_pair(0)
    send_first()
    totals(1)
    send_back(0)
    sum_pair(3)
    moment_pair(3)
    moments(2)
    forward_first()
    update_pair(1)
    send_pair(2)
    moments(3)
    totals(2)
    send_back(2)
    forward_pair(2)
    settle_pair(0)
    totals(3)
    update_pair(2)
    send_pair(4)
    send_back(4)
    w_loads[0].wait()
    w_loads[1].wait()
    unpack_pair(0, base)
    take_pair(0)
    settle_pair(2)
    update_pair(3)
    send_pair(6)
    forward_pair(4)
    send_back(6)
    unpack_pair(2, base)
    take_pair(2)
    remote(lvnew, lvnew, vs_sem.at[0], vs_sem.at[1], partner).wait_recv()
    new_vectors()
    turn_last()
    forward_pair(6)
    settle_pair(4)
    unpack_pair(4, base)
    settle_last(1)
    take_pair(4)
    settle_last(2)
    unpack_pair(6, base)
    take_last()
    for ref, sem in ((pbuf, gs_sem), (msend, ms_sem), (mall.at[first(6)], s_sem), (mall.at[first(6)], ags_sem), (mall.at[first(8)], shs_sem),
                     (lraw.at[0], os_sem), (mt.at[first(4), first(88)], sts_sem), (lvnew, vs_sem)):
        remote(ref, ref, sem.at[0], os_sem.at[1], partner).wait_send()
    last = box_sx.at[:, first(RING - 1)]
    remote(last, last, sts_sem.at[1], os_sem.at[1], partner).wait_send()


def update_call(scalars, arrays):
    hbm, smem = pl.BlockSpec(memory_space=pltpu.HBM), pl.BlockSpec(memory_space=pltpu.SMEM)
    dma, vmem = pltpu.SemaphoreType.DMA, pltpu.VMEM

    def lanes(*lead):
        return vmem(lead + (LN,), F32)

    scratch = [
        vmem((LC, KI + NO, D), F32), vmem((LC, KI + NO, D), F32), vmem((LG, KI + NO, D), F32), lanes(LC, RING, CH), lanes(LC, CH), lanes(LC, 2, CH), lanes(LC, CH),
        lanes(L, RING, CH), vmem((L, B48, KI), BF16), vmem((L, B48, NO), BF16), vmem((LC, B48, D), F32), vmem((LC, LN, D), F32),
        lanes(LC, CH), lanes(D), lanes(NG, LN), lanes(NG, 8),
        vmem((2, 2, LC, B48), F32), vmem((LC, KI), F32), vmem((LC, NO), F32), lanes(3, 2, LC),
        lanes(NG, 8), lanes(NG, 8), lanes(2, NG, 8), lanes(2, NG, 8),
        lanes(NG, RING, 8), lanes(NG, RING, 1), lanes(NG, TP, 8), lanes(NG, TP, 8),
        dma((LG + 1,)), dma((LG,)), dma((1,)), dma((NG + LG,)), dma((2,)), dma((1,)), dma((1,)), dma((1,)), dma((NG,)), dma((NG,)),
        dma((1,)), dma((2 * NG + 2,)), dma((1,)), dma((NG + 2,)), dma((2,)), dma((NG, 3)), dma((2,)), dma((4,)),
        dma((2,)), dma((2,)), pltpu.SemaphoreType.REGULAR((3,)),
    ]
    outs = [((L, KI, D), F32), ((L, NO, D), F32), ((L, B48, KI), BF16), ((L, B48, NO), BF16),
            ((L, B48), F32), ((L, KI), F32), ((L, NO), F32), ((L, B48), F32)]
    return pl.pallas_call(
        kernel,
        out_shape=[vmem(*out) for out in outs],
        in_specs=[smem] * len(scalars) + [hbm] * len(arrays),
        out_specs=[pl.BlockSpec(memory_space=vmem)] * len(outs),
        scratch_shapes=scratch,
        compiler_params=pltpu.CompilerParams(collective_id=0, has_side_effects=True, vmem_limit_bytes=36 * 2**20),
        name='adafactor',
    )(*[val.reshape(1) for val in scalars], *[pltpu.with_memory_space_constraint(val, pltpu.HBM) for val in arrays])


def store_kernel(*refs):
    num = len(refs) // 2
    copies = [pltpu.make_async_copy(src, dst, refs[-1].at[i]) for i, (src, dst) in enumerate(zip(refs[:num], refs[num:-1]))]
    for copy in copies:
        copy.start()
    for copy in copies:
        copy.wait()


def store_call(vals):
    anyspace = pl.BlockSpec(memory_space=pl.ANY)
    return pl.pallas_call(
        store_kernel,
        out_shape=[jax.ShapeDtypeStruct(val.shape, val.dtype) for val in vals],
        in_specs=[anyspace] * len(vals),
        out_specs=[anyspace] * len(vals),
        scratch_shapes=[pltpu.SemaphoreType.DMA((len(vals),))],
        compiler_params=pltpu.CompilerParams(vmem_limit_bytes=2**20),
        name='store',
    )(*[pltpu.with_memory_space_constraint(val, pltpu.VMEM) for val in vals])


def solution(mesh):
    def turn(val):
        return val.swapaxes(1, 2)

    def body(w_in, w_out, g_in, g_out, m_in, m_out, r_in, c_in, r_out, c_out, learn_rate, weight_decay, beta_two):
        out = store_call(update_call((learn_rate, weight_decay, beta_two),
                          (turn(w_in), w_out, turn(g_in[0]), g_out[0], m_in, turn(m_out), r_in, c_in, r_out, c_out)))
        return (turn(out[0]), out[1], out[2], turn(out[3])) + tuple(out[4:])

    cols, rows, own = P(None, None, 'tp'), P(None, 'tp', None), P(None, 'dp')
    outs = (cols, rows, P(None, 'dp', 'tp'), P(None, 'tp', 'dp'), own, P(None, 'tp'), P(None, 'tp'), own)
    in_specs = (cols, rows, P('dp', *cols), P('dp', *rows)) + outs[2:] + (P(), P(), P())
    return jax.shard_map(body, mesh=mesh, in_specs=in_specs, out_specs=outs, check_vma=False)
```

```python
import jax
import jax.numpy as jnp
from jax import lax
from jax.experimental import pallas as pl
from jax.experimental.pallas import tpu as pltpu
from jax.sharding import PartitionSpec as P

F32, BF16 = jnp.float32, jnp.bfloat16
MESH = pl.DeviceIdType.MESH
RING = 4
L, D = 16, 384
KI, NO = 168, 120
LC, LG, NG = 8, 2, 4
Q, LN, B48, B96 = 72, 128, 48, 96
CH, HEAD, MID, HALF = 3 * Q, KI - 2 * Q, 256, 104
NI, KIN, NOUT, KO = 384.0, 2688.0, 1920.0, 384.0
KINDS = RV, LT, SX, ST = range(4)
TP = RING * RING


def roll(val, shift):
    return pltpu.roll(val, shift % LN, 1)


def lane_of(shape):
    return lax.broadcasted_iota(jnp.int32, shape, 1)


def row_of(shape):
    return lax.broadcasted_iota(jnp.int32, shape, 0)


def colsum(val):
    return jnp.sum(val, axis=0, keepdims=True)


def rowsum(val):
    return jnp.sum(val, axis=1, keepdims=True)


def pick(cond, val):
    return jnp.where(cond, val, 0.0)


def first(num):
    return pl.ds(0, num)


def block(i):
    return pl.ds(Q * i, Q)


def tile_cols(t):
    return pl.ds(LN * t, LN)


def last_quarter(parts):
    lane = lane_of(parts[0].shape)
    tail = jnp.where(lane < 64, roll(parts[1], 64), roll(parts[2], B96))
    return jnp.where(lane < 32, roll(parts[0], 32), tail)


def join_quarters(quarters, keep):
    return [jnp.where(keep, quarters[i], roll(quarters[3], B96 - 32 * i)) for i in range(3)]


def kernel(rate_ref, wd_ref, beta_ref, w_in, w_out, g_in, g_out, m_in, m_out, r_in, c_in, r_out, c_out,
           wn_in, wn_out, mn_in, mn_out, rn_in, cn_in, rn_out, cn_out,
           gbuf, pbuf, gsend, pack, via, rin, fin, mall, mraw_in, mraw_out, msend, mt, mpack, tall,
           rvacc, lvacc, lraw, craw, oraw, pads, lvold, rvold, lvnew, rvnew, box_rv, box_sx, box_lt, box_st,
           gl_sem, gp_sem, gs_sem, gr_sem, ml_sem, ms_sem, mr_sem, s_sem, via_sem, rin_sem, ags_sem, agr_sem,
           shs_sem, shr_sem, sts_sem, str_sem, vs_sem, ol_sem, os_sem, wl_sem, ready):
    tp, dp = lax.axis_index('tp'), lax.axis_index('dp')
    z, y, x, c = tp // RING, tp % RING, dp // 2, dp % 2
    other = 1 - c
    base, pbase = c * LC, other * LC

    def at_x(xx):
        return {'dp': (xx % RING) * 2 + c}

    def at_y(yy):
        return {'tp': z * RING + yy % RING}

    def at_z(zz):
        return {'tp': (zz % RING) * RING + y}

    partner = {'dp': x * 2 + other}

    def local(src, dst, sem):
        return pltpu.make_async_copy(src, dst, sem)

    def remote(src, dst, send_sem, recv_sem, device):
        return pltpu.make_async_remote_copy(src_ref=src, dst_ref=dst, send_sem=send_sem, recv_sem=recv_sem,
                                            device_id=device, device_id_type=MESH)

    def greet(step):
        for peer in plane:
            pl.semaphore_signal(ready.at[step], inc=1, device_id=peer, device_id_type=MESH)

    def greeted(step):
        pl.semaphore_wait(ready.at[step], len(plane))

    barrier = pltpu.get_barrier_semaphore()
    plane = [at_y(y + 1), at_y(y + RING - 1), at_z(z + 1), at_z(z + RING - 1)]
    peers = [partner, at_x(x + 1), at_x(x + RING - 1)] + plane
    for peer in peers:
        pl.semaphore_signal(barrier, inc=1, device_id=peer, device_id_type=MESH)

    def own(l, i):
        src, dst = ((g_in, first(KI)), (g_out, pl.ds(KI, NO)))[i]
        return local(src.at[base + l], gbuf.at[l, dst], gl_sem.at[l if isinstance(l, int) else LG])

    def others(l, i):
        src, dst = ((g_in, first(KI)), (g_out, pl.ds(KI, NO)))[i]
        return local(src.at[pbase + l], gsend.at[l, dst], gp_sem.at[l])

    def swap_first(l):
        return remote(gsend.at[l], pbuf.at[l], gs_sem.at[0], gr_sem.at[NG + l], partner)

    def swap(l, i):
        src, dst = ((g_in, first(KI)), (g_out, pl.ds(KI, NO)))[i]
        return remote(src.at[pbase + l], pbuf.at[l, dst], gs_sem.at[0], gr_sem.at[l // LG], partner)

    my_rows, its_rows = pl.ds(base, LC), pl.ds(pbase, LC)
    loads = [local(m_in, mraw_in, ml_sem.at[0]), local(m_out, mraw_out, ml_sem.at[1]),
             local(r_in.at[my_rows], lraw.at[0, c], ol_sem.at[0]), local(c_out.at[my_rows], lraw.at[1, c], ol_sem.at[1]),
             local(c_in.at[my_rows], craw, ol_sem.at[2]), local(r_out.at[my_rows], oraw, ol_sem.at[3])]
    w_loads = [local(w_in, wn_in, wl_sem.at[0]), local(w_out, wn_out, wl_sem.at[1])]

    def lane_swap(m, core):
        return remote((r_in, c_out)[m].at[its_rows], lraw.at[m, core], os_sem.at[0], os_sem.at[1], partner)

    def start_loads(l, carry):
        own(l, 0).start()
        own(l, 1).start()
        return carry

    for l in range(LG):
        for i in range(2):
            others(l, i).start()
            own(l, i).start()
    lax.fori_loop(LG, LC, start_loads, 0)
    for copy in loads:
        copy.start()
    pl.semaphore_wait(barrier, len(peers))
    greet(0)
    for l in range(LG):
        local(gsend.at[l], gsend.at[l], gp_sem.at[l]).wait()
        swap_first(l).start()
    lane_swap(0, c).start()
    lane_swap(1, c).start()
    rvacc[...] = jnp.zeros_like(rvacc)
    lvacc[...] = jnp.zeros_like(lvacc)

    lane, lane8, row8 = lane_of((Q, LN)), lane_of((8, LN)), row_of((8, LN))
    m96, k96 = lane < B96, lane8 < B96
    head = row_of((Q, LN)) < HEAD
    only_x = (row8 >= 2 * LG) & (row8 < 3 * LG)

    def way(l):
        return 1 - 2 * (l % 2)

    def ahead(l):
        return (x + way(l) + RING) % RING

    def behind(l):
        return (x - way(l) + RING) % RING

    across = (x + 2) % RING

    def step1(l):
        return remote(pack.at[l, across], via.at[l], s_sem.at[0], via_sem.at[l // LG], at_x(ahead(l)))

    def step2(l):
        return remote(pack.at[l, ahead(l)], rin.at[l, 0], s_sem.at[0], rin_sem.at[l // LG], at_x(ahead(l)))

    def step3(l):
        return remote(pack.at[l, behind(l)], rin.at[l, 1], s_sem.at[0], rin_sem.at[l // LG], at_x(behind(l)))

    def m_rows(core):
        return pl.ds(pl.multiple_of(core * B48, 16), B48)

    def moment_swap(l, core):
        return remote(msend.at[l], mt.at[l, m_rows(core)], ms_sem.at[0], mr_sem.at[0], partner)

    def stage_a(l):
        def tile(t, q):
            return gbuf[l, block(q), tile_cols(t)] + pbuf[l, block(q), tile_cols(t)]

        def chunk(d, q):
            if d == 0:
                return tile(0, q)
            if d == 1:
                return roll(jnp.where(m96, tile(1, q), tile(0, q)), 32)
            if d == 2:
                return roll(jnp.where(lane < 64, tile(2, q), tile(1, q)), 64)
            return roll(tile(2, q), B96)

        def put(d):
            for i, val in enumerate(join_quarters([chunk(d, q) for q in range(4)], m96)):
                pack[l, d, block(i), :] = val

        if not isinstance(l, int):
            for d in range(RING):
                put(d)
            return

        for d in range(RING):
            pl.when(across == d)(lambda: put(d))
        step1(l).start()
        for d in range(RING):
            pl.when(across != d)(lambda: put(d))

    def stage_n(l):
        msend[l, :, first(KI)] = mraw_in[pbase + l].astype(F32)
        msend[l, :, pl.ds(MID, NO)] = mraw_out[pbase + l].astype(F32)
        moment_swap(l, c).start()
        mt[l, m_rows(c), first(KI)] = mraw_in[base + l].astype(F32)
        mt[l, m_rows(c), pl.ds(MID, NO)] = mraw_out[base + l].astype(F32)

    def stage_b(l):
        to = ahead(l)
        pack[l, to] = pack[l, to] + via[l]
        step2(l).start()

    def stage_c(l):
        sq = []
        for i in range(3):
            grad = pack[l, x, block(i), :] + rin[l, 0, block(i), :] + rin[l, 1, block(i), :]
            fin[l, block(i), :] = grad
            sq.append(grad * grad + 1e-30)
        g, lg = l // LG, l % LG
        sums = [rowsum(pick(m96, val)) for val in sq]
        sums.append(rowsum(jnp.where(m96, 0.0, sq[0] + sq[1] + sq[2])))
        acc = rvacc[g, first(Q), :]
        for q in range(4):
            acc = jnp.where(lane == LG * q + lg, sums[q], acc)
        rvacc[g, first(Q), :] = acc
        top = colsum(pick(head, sq[2]))
        low = colsum(jnp.where(head, 0.0, sq[2]))
        cols = [colsum(sq[0]), colsum(sq[1])]
        wide = [jnp.broadcast_to(val, (8, LN)) for val in (cols[0], cols[1], top + low)]
        in_sum = pick(k96, cols[0] + cols[1] + top)
        out_sum = pick(k96, low + last_quarter(wide))
        both = jnp.where(row8 == lg, in_sum, lvacc[g])
        lvacc[g] = jnp.where(row8 == LG + lg, out_sum, both)

    def stage_m(l):
        val = mt[l].T
        third = jnp.concatenate([val[2 * Q:KI], val[MID:MID + B48]], axis=0)
        quarters = [val[:Q], val[Q:2 * Q], third, val[MID + B48:MID + NO]]
        for i, part in enumerate(join_quarters(quarters, m96)):
            mpack[l, block(i), :] = part

    boxes = {RV: (box_rv, x, RING), SX: (box_sx, x, RING), LT: (box_lt, tp, TP), ST: (box_st, tp, TP)}

    def post(kind, g, val):
        box, me, num = boxes[kind]
        box[g, me] = val

        def send(k, carry):
            device = at_x(me + k) if num == RING else {'tp': (me + k) % TP}
            remote(box.at[g, me], box.at[g, me], sts_sem.at[int(kind == SX)], str_sem.at[g, max(kind - 1, 0)], device).start()
            return carry

        lax.fori_loop(1, num, send, 0)

    def collect(kind, g):
        box, me, num = boxes[kind]
        rest = mt.at[0, first(B48)] if kind == LT else box.at[g, first(num - 1)]
        if kind != RV:
            remote(rest, rest, sts_sem.at[int(kind == SX)], str_sem.at[g, max(kind - 1, 0)], partner).wait_recv()
        val = box[g, 0]
        for k in range(1, num):
            val = val + box[g, k]
        return val

    def sums_send(g):
        post(LT, g, lvacc[g])
        post(RV, g, rvacc[g].T[:8])

    beta = beta_ref[0]

    def old_vectors():
        for copy in loads[2:]:
            copy.wait()
        remote(lraw.at[0], lraw.at[0], os_sem.at[0], os_sem.at[1], partner).wait_recv()
        for m in range(2):
            for core in range(2):
                pads[m, core, :, first(B48)] = lraw[m, core]
        pads[2, 0, :, first(KI - LN)] = craw[:, pl.ds(LN, KI - LN)]
        pads[2, 1, :, first(NO)] = oraw[...]
        low, high, rest = craw[:, first(LN)], pads[2, 0], pads[2, 1]
        lanes = [jnp.where(lane8 < B48, pads[m, 0], roll(pads[m, 1], B48)) for m in range(2)]
        rows = [low, jnp.where(lane8 < LN - Q, roll(low, -Q), roll(high, -Q)),
                jnp.where(lane8 < HEAD, roll(high, -16), roll(rest, HEAD)), roll(rest, -B48)]
        for g in range(NG):
            part = slice(LG * g, LG * g + LG)
            lvold[g] = jnp.concatenate([val[part] for val in lanes + lanes], axis=0)
            rvold[g] = jnp.concatenate([val[part] for val in rows], axis=0)

    def vec_swap(g, half, i):
        ref = (lvnew, rvnew)[i]
        return remote(ref.at[half, g], ref.at[half, g], vs_sem.at[0], vs_sem.at[1], partner)

    def moments(g):
        lv_mean = collect(LT, g) / jnp.where(row8 < LG, KIN, NOUT)
        lv_new = beta * lvold[g] + (1.0 - beta) * lv_mean
        lvnew[c, g] = lv_new
        rv_new = beta * rvold[g] + (1.0 - beta) * (collect(RV, g) / NI)
        rvnew[c, g] = rv_new
        for i in range(2):
            vec_swap(g, c, i).start()
        scale_l = 1.0 / jnp.sqrt(jnp.where(k96, lv_new, 1.0))
        scale_r = 1.0 / jnp.sqrt(jnp.where(lane8 < Q, rv_new, 1.0))
        wide = jnp.concatenate([scale_r, jnp.ones((LN - 8, LN), F32)], axis=0).T
        tots = jnp.zeros((8, LN), F32)
        lane1 = lane_of((1, LN))
        for lg in range(LG):
            l = g * LG + lg
            rs = [jnp.broadcast_to(wide[:Q, LG * q + lg:LG * q + lg + 1], (Q, LN)) for q in range(4)]
            sc_in = scale_l[lg:lg + 1, :]
            sc_out = jnp.broadcast_to(scale_l[LG + lg:LG + lg + 1, :], (8, LN))
            parts = []
            for i in range(3):
                body = jnp.where(head, sc_in, sc_out[:1]) if i == 2 else sc_in
                lanes = jnp.where(m96, body, roll(sc_out, B96 - 32 * i)[:1])
                u0 = fin[l, block(i), :] * jnp.where(m96, rs[i], rs[3]) * lanes
                fin[l, block(i), :] = u0
                parts.append(u0 * u0)
            inner = pick(m96, parts[0] + parts[1] + pick(head, parts[2]))
            outer = jnp.where(m96, jnp.where(head, 0.0, parts[2]), parts[0] + parts[1] + parts[2])
            v_in = pick(lane1 < B96, lv_new[lg:lg + 1, :])
            v_out = pick((lane1 >= HEAD) & (lane1 < Q), rv_new[2 * LG + lg:2 * LG + lg + 1, :]) + pick(lane1 < Q, rv_new[3 * LG + lg:3 * LG + lg + 1, :])
            for k, val in enumerate((colsum(inner), colsum(outer), v_in, v_out)):
                tots = jnp.where(row8 == LG * k + lg, val, tots)
        post(ST, g, tots)

    def totals(g):
        val = rowsum(jnp.where(only_x, box_st[g, tp], collect(ST, g)))
        post(SX, g, colsum(pick(row8 == lane8, val)))

    def factors(g):
        val = jnp.where(lane_of((1, LN)) >= 3 * LG, box_sx[g, x], collect(SX, g))
        tot = rowsum(pick(row8 == lane8, val))
        isin = row_of((2 * LG, 1)) < LG
        mean_r = tot[2 * LG:] / jnp.where(isin, NI, NOUT)
        rms = jnp.sqrt(mean_r * tot[:2 * LG] / jnp.where(isin, NI * KIN, NOUT * KO))
        return jnp.sqrt(mean_r) / jnp.maximum(1.0, rms)

    def update(l, lg, fac):
        f_in, f_out = fac[lg:lg + 1, :], fac[LG + lg:LG + lg + 1, :]
        for i in range(3):
            upd = fin[l, block(i), :] * jnp.where((m96 & head) if i == 2 else m96, f_in, f_out)
            new = 0.9 * mpack[l, block(i), :] + 0.1 * upd
            mall[base + l, x, block(i), :] = new.astype(BF16).astype(F32)

    def arrived(l, k):
        return l // LG if k == 0 else 2 * NG if k == 1 and l >= LC - LG else NG + l // LG

    def gather(l, k):
        slot = x if k < 2 else behind(l)
        ref = mall.at[base + l, slot]
        return remote(ref, ref, ags_sem.at[0], agr_sem.at[arrived(l, k)], at_x(behind(l) if k == 1 else ahead(l)))

    def share(l, k, start):
        ref = mall.at[start + l, (behind(l), ahead(l), across, x)[k]]
        return remote(ref, ref, shs_sem.at[0], shr_sem.at[NG if k == 3 and l >= LC - LG else min(l // LG, NG - 1) if l < LC - 1 else NG + 1], partner)

    def send_pair(l):
        gather(l, 0).start()
        gather(l + 1, 0).start()

    def send_back(l):
        gather(l, 1).start()
        gather(l + 1, 1).start()
        share(l, 3, base).start()
        share(l + 1, 3, base).start()

    def forward_pair(l):
        two = mall.at[base + l, first(LG)]
        remote(two, two, ags_sem.at[0], agr_sem.at[arrived(l, 0)], partner).wait_recv()
        for k in (l, l + 1):
            gather(k, 2).start()
            share(k, 0, base).start()

    def half(ref, h, lead=0):
        rows = (first(HALF), pl.ds(HALF, CH - HALF))[h]
        return ref.at[:, rows] if lead else ref.at[rows]

    def gather_half(l, h, slot):
        ref = half(mall.at[base + l, slot], h)
        return remote(ref, ref, ags_sem.at[0], agr_sem.at[0 if h == 0 else 2 * NG + 1], at_x(ahead(l)))

    def send_first():
        for h in range(2):
            for l in range(LG):
                gather_half(l, h, x).start()

    def forward_first():
        for h in range(2):
            two = half(mall.at[base, first(LG)], h, 1)
            remote(two, two, ags_sem.at[0], agr_sem.at[0 if h == 0 else 2 * NG + 1], partner).wait_recv()
            for l in range(LG):
                ref = half(mall.at[base + l, behind(l)], h)
                remote(ref, ref, ags_sem.at[0], agr_sem.at[arrived(l, 2)], at_x(ahead(l))).start()
        share(0, 0, base).start()
        share(1, 0, base).start()

    def settle_pair(l):
        four = mall.at[base + l]
        remote(four, four, ags_sem.at[0], agr_sem.at[arrived(0, 1) + l // LG], partner).wait_recv()
        for k in (l, l + 1):
            for i in (1, 2):
                share(k, i, base).start()

    def settle_last(k):
        l = LC - LG
        two = mall.at[base + l, first(LG)]
        remote(two, two, ags_sem.at[0], agr_sem.at[arrived(l, k)], partner).wait_recv()
        share(l, k, base).start()
        share(l + 1, k, base).start()

    rate = rate_ref[0]
    decay = rate * wd_ref[0]

    def unpack(at):
        for q in range(4):
            if q < 3:
                chunk = [mall[at, d, block(q), :] for d in range(RING)]
            else:
                chunk = [last_quarter([mall[at, d, block(i), :] for i in range(3)]) for d in range(RING)]
            r1, r2, r3 = roll(chunk[1], B96), roll(chunk[2], 64), roll(chunk[3], 32)
            mom = (jnp.where(m96, chunk[0], r1), jnp.where(lane < 64, r1, r2), jnp.where(lane < 32, r2, r3))
            spots = (((wn_in, 0, 0, Q),), ((wn_in, Q, 0, Q),), ((wn_in, 2 * Q, 0, HEAD), (wn_out, 0, HEAD, B48)), ((wn_out, B48, 0, Q),))[q]
            for t in range(3):
                for ref, dst, src, num in spots:
                    rows = pl.ds(dst, num)
                    w = ref[at, rows, tile_cols(t)]
                    ref[at, rows, tile_cols(t)] = w - rate * mom[t][src:src + num] - decay * w

    def turn_moment(at):
        parts = [mall[at, x, block(i), :] for i in range(3)]
        parts.append(last_quarter(parts))
        spots = ((0, 0, Q),), ((Q, 0, Q),), ((2 * Q, 0, HEAD), (MID, HEAD, B48)), ((MID + B48, 0, Q),)
        for val, places in zip(parts, spots):
            val = jnp.where(c == 0, val, roll(val, -B48))
            for dst, src, num in places:
                tall[pl.ds(dst, num), :] = val[src:src + num]
        turned = [tall[tile_cols(t), :].T[:B48] for t in range(3)]
        mn_in[at, :, first(LN)] = turned[0].astype(BF16)
        mn_in[at, :, pl.ds(LN, KI - LN)] = turned[1][:, :KI - LN].astype(BF16)
        mn_out[at] = turned[2][:, :NO].astype(BF16)

    def each(step, l, start):
        lax.fori_loop(start + l, start + l + LG, lambda at, carry: (step(at), carry)[1], 0)

    def unpack_pair(l, start):
        each(unpack, l, start)
        if l < LC - LG:
            each(turn_moment, l, start)

    def turn_last():
        l = LC - LG
        each(turn_moment, l, base)
        two = mall.at[base, first(LG)]
        remote(two, two, shs_sem.at[0], shr_sem.at[NG], partner).wait_recv()
        each(turn_moment, l, pbase)

    def take_pair(l):
        two = mall.at[pl.ds(pbase + l, LG)]
        remote(two, two, shs_sem.at[0], shr_sem.at[l // LG], partner).wait_recv()
        unpack_pair(l, pbase)

    def take_last():
        for l in range(LC - LG, LC):
            three = mall.at[pbase + l, first(3)]
            remote(three, three, shs_sem.at[0], shr_sem.at[NG - 1 if l < LC - 1 else NG + 1], partner).wait_recv()
            lax.fori_loop(pbase + l, pbase + l + 1, lambda at, carry: (unpack(at), carry)[1], 0)

    def new_vectors():
        lane4 = lane_of((LG, LN))
        for half in range(2):
            for g in range(NG):
                rows = pl.ds(LC * half + LG * g, LG)
                both, val = lvnew[half, g], rvnew[half, g]
                both = jnp.where(c == 0, both, roll(both, -B48))
                rn_in[rows, :] = both[:LG, :B48]
                cn_out[rows, :] = both[LG:2 * LG, :B48]
                two = roll(val, Q)[LG:2 * LG]
                cn_in[rows, first(LN)] = jnp.where(lane4 < Q, val[:LG], two)
                cn_in[rows, pl.ds(LN, KI - LN)] = jnp.where(lane4 < 16, two, roll(val, 16)[2 * LG:3 * LG])[:, :KI - LN]
                rn_out[rows, :] = jnp.where(lane4 < B48, roll(val, -HEAD)[2 * LG:3 * LG], roll(val, B48)[3 * LG:])[:, :NO]

    def both(step, g):
        lax.fori_loop(LG * g, LG * g + LG, lambda l, carry: (step(l), carry)[1], 0)

    def swap_start(l):
        swap(l, 0).start()
        swap(l, 1).start()

    def pack_first():
        for l in range(LG):
            local(gbuf.at[l], gbuf.at[l], gl_sem.at[l]).wait()
            swap_first(l).wait_recv()
            stage_a(l)
            if l == 0:
                both(swap_start, 1)
        both(lambda l: step3(l).start(), 0)

    def pack_pair(g):
        two = pl.ds(LG * g, LG)
        if g == 1:
            rest = gbuf.at[pl.ds(LG, LC - LG)]
            local(rest, rest, gl_sem.at[LG]).wait()
        remote(pbuf.at[two], pbuf.at[two], gs_sem.at[0], gr_sem.at[g], partner).wait_recv()
        if g + 1 < NG:
            both(swap_start, g + 1)
        both(stage_a, g)
        both(lambda l: step1(l).start(), g)

    def direct_pair(g):
        both(lambda l: step3(l).start(), g)

    def cast_all():
        loads[0].wait()
        loads[1].wait()
        lax.fori_loop(0, LC, lambda l, carry: (stage_n(l), carry)[1], 0)

    def relay_pair(g):
        two = via.at[pl.ds(LG * g, LG)]
        remote(two, two, s_sem.at[0], via_sem.at[g], partner).wait_recv()
        both(stage_b, g)

    def sum_pair(g):
        two = rin.at[pl.ds(LG * g, LG)]
        remote(two, two, s_sem.at[0], rin_sem.at[g], partner).wait_recv()
        both(stage_c, g)
        sums_send(g)

    def moment_pair(g):
        if g == 0:
            remote(msend, msend, ms_sem.at[0], mr_sem.at[0], partner).wait_recv()
        both(stage_m, g)

    def update_pair(g):
        fac = factors(g)
        for lg in range(LG):
            update(LG * g + lg, lg, fac)

    pack_first()
    pack_pair(1)
    cast_all()
    w_loads[0].start()
    w_loads[1].start()
    old_vectors()
    greeted(0)
    greet(1)
    relay_pair(0)
    direct_pair(1)
    greeted(1)
    greet(2)
    pack_pair(2)
    greeted(2)
    sum_pair(0)
    relay_pair(1)
    direct_pair(2)
    moment_pair(0)
    pack_pair(3)
    moments(0)
    sum_pair(1)
    relay_pair(2)
    moment_pair(1)
    totals(0)
    direct_pair(3)
    relay_pair(3)
    moments(1)
    sum_pair(2)
    moment_pair(2)
    update_pair(0)
    send_first()
    totals(1)
    send_back(0)
    sum_pair(3)
    moment_pair(3)
    moments(2)
    forward_first()
    update_pair(1)
    send_pair(2)
    moments(3)
    totals(2)
    send_back(2)
    forward_pair(2)
    settle_pair(0)
    totals(3)
    update_pair(2)
    send_pair(4)
    send_back(4)
    w_loads[0].wait()
    w_loads[1].wait()
    unpack_pair(0, base)
    take_pair(0)
    settle_pair(2)
    update_pair(3)
    send_pair(6)
    forward_pair(4)
    send_back(6)
    unpack_pair(2, base)
    take_pair(2)
    remote(lvnew, lvnew, vs_sem.at[0], vs_sem.at[1], partner).wait_recv()
    new_vectors()
    turn_last()
    forward_pair(6)
    settle_pair(4)
    unpack_pair(4, base)
    settle_last(1)
    take_pair(4)
    settle_last(2)
    unpack_pair(6, base)
    take_last()
    for ref, sem in ((pbuf, gs_sem), (msend, ms_sem), (mall.at[first(6)], s_sem), (mall.at[first(6)], ags_sem), (mall.at[first(8)], shs_sem),
                     (lraw.at[0], os_sem), (mt.at[first(4), first(88)], sts_sem), (lvnew, vs_sem)):
        remote(ref, ref, sem.at[0], os_sem.at[1], partner).wait_send()
    last = box_sx.at[:, first(RING - 1)]
    remote(last, last, sts_sem.at[1], os_sem.at[1], partner).wait_send()


def update_call(scalars, arrays):
    hbm, smem = pl.BlockSpec(memory_space=pltpu.HBM), pl.BlockSpec(memory_space=pltpu.SMEM)
    dma, vmem = pltpu.SemaphoreType.DMA, pltpu.VMEM

    def lanes(*lead):
        return vmem(lead + (LN,), F32)

    scratch = [
        vmem((LC, KI + NO, D), F32), vmem((LC, KI + NO, D), F32), vmem((LG, KI + NO, D), F32), lanes(LC, RING, CH), lanes(LC, CH), lanes(LC, 2, CH), lanes(LC, CH),
        lanes(L, RING, CH), vmem((L, B48, KI), BF16), vmem((L, B48, NO), BF16), vmem((LC, B48, D), F32), vmem((LC, LN, D), F32),
        lanes(LC, CH), lanes(D), lanes(NG, LN), lanes(NG, 8),
        vmem((2, 2, LC, B48), F32), vmem((LC, KI), F32), vmem((LC, NO), F32), lanes(3, 2, LC),
        lanes(NG, 8), lanes(NG, 8), lanes(2, NG, 8), lanes(2, NG, 8),
        lanes(NG, RING, 8), lanes(NG, RING, 1), lanes(NG, TP, 8), lanes(NG, TP, 8),
        dma((LG + 1,)), dma((LG,)), dma((1,)), dma((NG + LG,)), dma((2,)), dma((1,)), dma((1,)), dma((1,)), dma((NG,)), dma((NG,)),
        dma((1,)), dma((2 * NG + 2,)), dma((1,)), dma((NG + 2,)), dma((2,)), dma((NG, 3)), dma((2,)), dma((4,)),
        dma((2,)), dma((2,)), pltpu.SemaphoreType.REGULAR((3,)),
    ]
    outs = [((L, KI, D), F32), ((L, NO, D), F32), ((L, B48, KI), BF16), ((L, B48, NO), BF16),
            ((L, B48), F32), ((L, KI), F32), ((L, NO), F32), ((L, B48), F32)]
    return pl.pallas_call(
        kernel,
        out_shape=[vmem(*out) for out in outs],
        in_specs=[smem] * len(scalars) + [hbm] * len(arrays),
        out_specs=[pl.BlockSpec(memory_space=vmem)] * len(outs),
        scratch_shapes=scratch,
        compiler_params=pltpu.CompilerParams(collective_id=0, has_side_effects=True, vmem_limit_bytes=36 * 2**20),
        name='adafactor',
    )(*[val.reshape(1) for val in scalars], *[pltpu.with_memory_space_constraint(val, pltpu.HBM) for val in arrays])


def store_kernel(*refs):
    num = len(refs) // 2
    pairs = list(zip(refs[:num], refs[num:-1]))
    for i, (src, dst) in enumerate(pairs):
        step = LG * 2 if i < 2 else L
        for l in range(0, L, step):
            part = pl.ds(l, step)
            pltpu.make_async_copy(src.at[part], dst.at[part], refs[-1].at[i]).start(priority=(l // step) % 2)
    for i, (src, dst) in enumerate(pairs):
        pltpu.make_async_copy(src, dst, refs[-1].at[i]).wait()


def store_call(vals):
    anyspace = pl.BlockSpec(memory_space=pl.ANY)
    return pl.pallas_call(
        store_kernel,
        out_shape=[jax.ShapeDtypeStruct(val.shape, val.dtype) for val in vals],
        in_specs=[anyspace] * len(vals),
        out_specs=[anyspace] * len(vals),
        scratch_shapes=[pltpu.SemaphoreType.DMA((len(vals),))],
        compiler_params=pltpu.CompilerParams(vmem_limit_bytes=2**20),
        name='store',
    )(*[pltpu.with_memory_space_constraint(val, pltpu.VMEM) for val in vals])


def solution(mesh):
    def turn(val):
        return val.swapaxes(1, 2)

    def body(w_in, w_out, g_in, g_out, m_in, m_out, r_in, c_in, r_out, c_out, learn_rate, weight_decay, beta_two):
        out = store_call(update_call((learn_rate, weight_decay, beta_two),
                          (turn(w_in), w_out, turn(g_in[0]), g_out[0], m_in, turn(m_out), r_in, c_in, r_out, c_out)))
        return (turn(out[0]), out[1], out[2], turn(out[3])) + tuple(out[4:])

    cols, rows, own = P(None, None, 'tp'), P(None, 'tp', None), P(None, 'dp')
    outs = (cols, rows, P(None, 'dp', 'tp'), P(None, 'tp', 'dp'), own, P(None, 'tp'), P(None, 'tp'), own)
    in_specs = (cols, rows, P('dp', *cols), P('dp', *rows)) + outs[2:] + (P(), P(), P())
    return jax.shard_map(body, mesh=mesh, in_specs=in_specs, out_specs=outs, check_vma=False)
```
